128 devices in a mesh: obl: 16 (over y, z), scn: 8 (over x, core).
Axes of the slice: x: 4, y: 4, z: 4, core: 2. Of those that a mesh axis runs over, the one named last changes fastest.
Arguments:
- factors: bfloat16 [32768, 128], P('scn'), may hold values from -6 to 6
- idiosyncratic: bfloat16 [32768, 32768], P('obl', 'scn'), may hold values from -6 to 6
- loadings: bfloat16 [32768, 128], P('obl'), may hold values from -0.375 to 0.375
- rating: int32 [32768], P('obl'), may hold values from 0 to 15
- barrier: float32 [16], replicated, may hold values from 1 to 3
- loss_given: float32 [32768], P('obl'), may hold values from 0.2 to 0.9
- sector: int32 [32768], P('obl'), may hold values from 0 to 15, as said below
- allowed: int32 [256, 16], replicated, may hold values from 0 to 1, as said below
- holdings: float32 [32768, 256], P('obl'), may hold values from 0.1 to 10
Outputs:
- positions: float32 [32768, 256], P('obl')
- shortfall: float32 [2, 256], replicated
The draws below stay inside these ranges and needn't reach their ends.
Inputs may be any that keep to these rules, and one draw needn't show every extreme that they name: Each sector holds exactly 2048 obligors. `allowed`: every mandate allows at least one sector.
All inputs are finite; a program needn't handle non-finite values.
Results may differ from the reference program's by a relative error of at most 0.0003.
Values may be sent and summed in bfloat16 or wider, within the bound.
No kernel may reach another device: no remote copies, remote signals or barrier semaphores. Data moves between devices by JAX's collectives and lax.ppermute only.
A program may use at most 128 MiB of HBM per device.

```python
import math
import jax
import jax.numpy as jnp
from jax import lax

FACTORS = 128
MANDATES = 256
RATINGS = 16
SECTORS = 16
STEPS = 2
OBL_DEV = 2048
OBLIGORS = 32768
SCENARIOS = 32768


def draw_sector(key, part):
    shuffled = jax.random.permutation(key, OBLIGORS)
    return (shuffled % SECTORS).astype(jnp.int32)


def draw_allowed(key, part):
    random_bits = jax.random.randint(jax.random.fold_in(key, 11), (MANDATES, SECTORS), 0, 2)
    chosen = jax.random.randint(jax.random.fold_in(key, 12), (MANDATES,), 0, SECTORS)
    forced = jnp.arange(SECTORS)[None, :] == chosen[:, None]
    return jnp.where(forced, 1, random_bits).astype(jnp.int32)


def touch_ends(result, key, smallest, top_value):
    longest = result.shape.index(max(result.shape))
    spots = []
    for shift in (0, 1):
        where = [jax.random.randint(jax.random.fold_in(key, axis), (), 0, length) for axis, length in enumerate(result.shape)]
        where[longest] = (where[longest] + shift) % result.shape[longest]
        spots.append(tuple(where))
    return result.at[spots[0]].set(smallest).at[spots[1]].set(top_value)


def block_levels(key, extent, shards, low, high):
    def one(dim, blocks):
        draws = jax.random.uniform(jax.random.fold_in(jax.random.fold_in(key, 6), dim), (blocks,), jnp.float32, low / len(shards), high / len(shards))
        return jnp.repeat(jnp.exp(draws), extent[dim] // blocks).reshape((-1,) + (1,) * (len(extent) - dim - 1))

    loudness = one(*shards[0])
    for cut in shards[1:]:
        loudness = loudness * one(*cut)
    return loudness


def scatter_about(key, dims, scale, bound, split=(), kind=jnp.bfloat16):
    values = jax.random.normal(key, dims, jnp.float32) * scale
    if len(split) > 0:
        values = block_levels(key, dims, split, -0.22, 0.18) * values
    return jnp.clip(values, min=-bound, max=bound).astype(kind)


def setup_inputs(seed: int = 0) -> dict:
    streams_of = jax.random.split(jax.random.key(seed), 10)
    factors = scatter_about(streams_of[0], (SCENARIOS, FACTORS), 1.0, 6.0, ((0, 8),))
    idiosyncratic = scatter_about(streams_of[1], (OBLIGORS, SCENARIOS), 1.0, 6.0, ((0, 16), (1, 8)))
    loadings = scatter_about(streams_of[2], (OBLIGORS, FACTORS), (2 * FACTORS) ** -0.5, 0.375, ((0, 16),))
    rating = touch_ends(jax.random.randint(streams_of[3], (OBLIGORS,), 0, RATINGS), jax.random.fold_in(streams_of[3], 1), 0, RATINGS - 1).astype(jnp.int32)
    barrier = jnp.clip(jax.random.uniform(streams_of[4], (RATINGS,), jnp.float32, 1.0, 3.0), 1.0, 3.0)
    loss_given = jnp.clip(0.2 + 0.7 * jax.random.uniform(streams_of[5], (OBLIGORS,), jnp.float32) ** block_levels(streams_of[5], (OBLIGORS,), ((0, 16),), -0.2, 0.2), 0.2, 0.9)
    sector = draw_sector(jax.random.fold_in(streams_of[9], 71), 0)
    allowed = draw_allowed(jax.random.fold_in(streams_of[9], 71), 0)
    holdings = jnp.clip(jnp.exp(math.log(10.0) - 4.6051702 * jax.random.uniform(streams_of[8], (OBLIGORS, MANDATES), jnp.float32) ** block_levels(streams_of[8], (OBLIGORS, MANDATES), ((0, 16),), -0.2, 0.2)), 0.1, 10.0)
    return {"factors": factors, "idiosyncratic": idiosyncratic, "loadings": loadings, "rating": rating, "barrier": barrier, "loss_given": loss_given, "sector": sector, "allowed": allowed, "holdings": holdings}


IDIO_SCALE = 0.8
SHARP = 2.0
LEVEL = 0.99
QUANTILE = 2.326
SMOOTH = 0.5
EPSILON = 1e-06
STEP_RATE = 8.0

def default_block(load_rows, idio_rows, barrier_rows, factors):
    systematic = lax.dot_general(load_rows, factors, (((1,), (1,)), ((), ())), preferred_element_type=jnp.float32)
    latent = systematic + IDIO_SCALE * idio_rows.astype(jnp.float32)
    return jax.nn.sigmoid((latent - barrier_rows[:, None]) * SHARP).astype(jnp.bfloat16)

def reference(factors, idiosyncratic, loadings, rating, barrier, loss_given, sector, allowed, holdings):
    eligible = jnp.transpose(allowed)[sector].astype(jnp.float32)
    barrier_rows = barrier[rating]
    blocks = OBLIGORS // OBL_DEV
    load_blocks = loadings.reshape(blocks, OBL_DEV, FACTORS)
    idio_blocks = idiosyncratic.reshape(blocks, OBL_DEV, SCENARIOS)
    bar_blocks = barrier_rows.reshape(blocks, OBL_DEV)
    weighted = eligible * holdings
    positions = OBLIGORS * weighted / lax.optimization_barrier(jnp.sum(weighted, 0))
    tail_scale = 1.0 / ((1.0 - LEVEL) * SCENARIOS)
    results = []
    for iteration in range(STEPS):
        exposure = (loss_given[:, None] * positions / OBLIGORS).astype(jnp.bfloat16)
        expo_blocks = exposure.reshape(blocks, OBL_DEV, MANDATES)

        def accumulate(carry, pieces):
            default_prob = default_block(pieces[0], pieces[1], pieces[2], factors)
            term = lax.dot_general(default_prob, pieces[3], (((0,), (0,)), ((), ())), preferred_element_type=jnp.float32)
            return (carry + term, None)
        losses, unused = lax.scan(accumulate, jnp.zeros((SCENARIOS, MANDATES), jnp.float32), (load_blocks, idio_blocks, bar_blocks, expo_blocks))
        center = lax.optimization_barrier(jnp.sum(losses, 0)) / SCENARIOS
        deviate = losses - center
        spread = lax.optimization_barrier(jnp.sum(deviate * deviate, 0)) / SCENARIOS
        deviation = jnp.sqrt(spread + EPSILON)
        thresh = center + QUANTILE * deviation
        smooth_width = SMOOTH * deviation
        scaled = (losses - thresh) / smooth_width
        tail_weight = (jax.nn.sigmoid(scaled) * tail_scale).astype(jnp.bfloat16)
        tail_sum = lax.optimization_barrier(jnp.sum(jax.nn.softplus(scaled), 0))
        results.append(thresh + smooth_width * (tail_sum * tail_scale))

        def project(pieces):
            default_prob = default_block(pieces[0], pieces[1], pieces[2], factors)
            return jnp.dot(default_prob, tail_weight, preferred_element_type=jnp.float32)
        gradient = lax.map(project, (load_blocks, idio_blocks, bar_blocks)).reshape(OBLIGORS, MANDATES)
        gradient = loss_given[:, None] * eligible * gradient
        unnorm = positions * jnp.exp(-STEP_RATE * gradient)
        positions = OBLIGORS * unnorm / lax.optimization_barrier(jnp.sum(unnorm, 0))
    return (positions, jnp.stack(results))
```

```python
import functools

import jax
import jax.numpy as jnp
from jax import lax
from jax.experimental import pallas as pl
from jax.experimental.pallas import tpu as pltpu
from jax.sharding import Mesh
from jax.sharding import PartitionSpec as P

STEPS = 2
OBL = ("y", "z")
SCN = ("x", "c")
IDIO_SCALE = 0.8
LEVEL = 0.99
QUANTILE = 2.326
SMOOTH = 0.5
EPSILON = 1e-06
STEP_RATE = 8.0
HEAD = 16
SPAN = 127.0
INTERPRET = False

f32 = jnp.float32
bf16 = jnp.bfloat16


def call(kernel, grid, in_specs, out_specs, out_shape, scratch=(), prefetch=0, flops=0, nbytes=0, name=None):
    spec = pltpu.PrefetchScalarGridSpec(
        num_scalar_prefetch=prefetch, grid=grid, in_specs=in_specs, out_specs=out_specs, scratch_shapes=list(scratch)
    )
    return pl.pallas_call(
        kernel,
        grid_spec=spec,
        out_shape=out_shape,
        compiler_params=pltpu.CompilerParams(vmem_limit_bytes=56 * 1024 * 1024),
        cost_estimate=pl.CostEstimate(flops=int(flops), bytes_accessed=int(nbytes), transcendentals=0),
        interpret=INTERPRET,
        name=name,
    )


def split3(value):
    a = value.astype(bf16)
    rest = value - a.astype(f32)
    b = rest.astype(bf16)
    c = (rest - b.astype(f32)).astype(bf16)
    return [a.astype(f32), b.astype(f32), c.astype(f32)]


def join3(head, at):
    return head[at : at + 1] + head[at + 1 : at + 2] + head[at + 2 : at + 3]


def encode(values, extra):
    low = jnp.min(values, axis=0, keepdims=True)
    high = jnp.max(values, axis=0, keepdims=True)
    span = jnp.maximum(jnp.maximum(high - low, jnp.abs(low) * (1.0 / 64.0)), 1e-30)
    base = low.astype(bf16).astype(f32)
    span = (span * 1.02).astype(bf16).astype(f32)
    code = jnp.exp((values - base) * (SPAN / span) - 0.5 * SPAN).astype(bf16)
    rows = [base, span]
    for row in extra:
        rows += split3(row)
    rows.append(jnp.zeros((HEAD - len(rows), values.shape[1]), f32))
    return code, jnp.concatenate(rows, axis=0).astype(bf16)


def decode(code, head):
    base, span = head[0:1], head[1:2]
    return (base + 0.5 * span) + jnp.log(code.astype(f32)) * (span * (1.0 / SPAN))


def setup_kernel(hold_ref, lgd_ref, sector_ref, allowed_ref, weighted_ref, elig_ref, expot_ref, tot_ref):
    hot = (sector_ref[...] == lax.broadcasted_iota(jnp.int32, (1, allowed_ref.shape[0]), 1)).astype(bf16)
    elig = jnp.dot(hot, allowed_ref[...], preferred_element_type=f32)
    weighted = elig * hold_ref[...]
    weighted_ref[...] = weighted
    elig_ref[...] = elig.astype(bf16)
    expot_ref[...] = jnp.transpose(weighted * lgd_ref[...]).astype(bf16)

    @pl.when(pl.program_id(0) == 0)
    def _():
        tot_ref[...] = jnp.zeros_like(tot_ref)

    tot_ref[0:1] += jnp.sum(weighted, axis=0, keepdims=True)


def first_losses_kernel(load_ref, fac_ref, idio_ref, expot_ref, tot_ref, p_ref, pay_ref, acc_ref):
    rows = fac_ref.shape[0]
    block = min(256, load_ref.shape[0])
    acc_ref[...] = jnp.zeros_like(acc_ref)
    for i in range(load_ref.shape[0] // block):
        sl = slice(i * block, (i + 1) * block)
        systematic = lax.dot_general(
            load_ref[sl], fac_ref[...], (((1,), (1,)), ((), ())), preferred_element_type=f32
        )
        prob = (0.5 * jnp.tanh(systematic + IDIO_SCALE * idio_ref[sl].astype(f32)) + 0.5).astype(bf16)
        p_ref[sl] = prob
        acc_ref[...] += jnp.dot(expot_ref[:, sl], prob, preferred_element_type=f32)
    code, head = encode(jnp.transpose(acc_ref[...]), [tot_ref[0:1]])
    pay_ref[0, 0:rows] = code
    pay_ref[0, rows : rows + HEAD] = head


def losses_kernel(p_ref, expot_ref, tot_ref, pay_ref):
    rows = p_ref.shape[1]
    losses = jnp.dot(expot_ref[...], p_ref[...], preferred_element_type=f32)
    code, head = encode(jnp.transpose(losses), [tot_ref[0:1]])
    pay_ref[0, 0:rows] = code
    pay_ref[0, rows : rows + HEAD] = head


def chunk_kernel(pay_ref, out_ref, acc_ref, tot_ref):
    step = pl.program_id(0)
    rows = acc_ref.shape[0]

    @pl.when(step == 0)
    def _():
        acc_ref[...] = jnp.zeros_like(acc_ref)
        tot_ref[...] = jnp.zeros_like(tot_ref)

    total = jnp.zeros_like(acc_ref)
    norm = jnp.zeros((1, acc_ref.shape[1]), f32)
    for k in range(pay_ref.shape[0]):
        head = pay_ref[k, rows : rows + HEAD].astype(f32)
        total += decode(pay_ref[k, 0:rows], head)
        norm += join3(head, 2)
    acc_ref[...] += total
    tot_ref[0:1] += norm

    @pl.when(step == pl.num_programs(0) - 1)
    def _():
        losses = acc_ref[...] / tot_ref[0:1]
        mean = jnp.sum(losses, axis=0, keepdims=True) * (1.0 / rows)
        off = losses - mean
        second = jnp.sum(off * off, axis=0, keepdims=True)
        code, head = encode(losses, [mean, second])
        for k in range(out_ref.shape[0]):
            out_ref[k, 0:rows] = code
            out_ref[k, rows : rows + HEAD] = head


def tail_kernel(tail_scale, pay_ref, stat_ref, weight_ref, soft_ref):
    rows = weight_ref.shape[0]
    head = pay_ref[0, rows : rows + HEAD].astype(f32)
    losses = decode(pay_ref[0, 0:rows], head)
    scaled = (losses - stat_ref[0:1]) * stat_ref[1:2]
    weight_ref[...] = (tail_scale / (1.0 + jnp.exp(-scaled))).astype(bf16)
    soft = jnp.maximum(scaled, 0.0) + jnp.log(1.0 + jnp.exp(-jnp.abs(scaled)))

    @pl.when(pl.program_id(0) == 0)
    def _():
        soft_ref[...] = jnp.zeros_like(soft_ref)

    soft_ref[0:1] += jnp.sum(soft, axis=0, keepdims=True)


def gradient_kernel(half_ref, p_ref, weight_ref, out_ref):
    out_ref[...] = jnp.dot(p_ref[...], weight_ref[...], preferred_element_type=f32)


def pair_kernel(own_ref, other_ref, soft_ref, soft_other_ref, pay_ref):
    rows = own_ref.shape[0]
    code, head = encode(own_ref[...] + other_ref[...], [soft_ref[0:1] + soft_other_ref[0:1]])
    pay_ref[0, 0:rows] = code
    pay_ref[0, rows : rows + HEAD] = head


def whole_kernel(pay_ref, out_ref, soft_ref):
    rows = pay_ref.shape[1] - HEAD
    total = jnp.zeros((rows, pay_ref.shape[2]), f32)
    soft = jnp.zeros((1, pay_ref.shape[2]), f32)
    for k in range(pay_ref.shape[0]):
        head = pay_ref[k, rows : rows + HEAD].astype(f32)
        total += decode(pay_ref[k, 0:rows], head)
        soft += join3(head, 2)
    soft_ref[...] = jnp.broadcast_to(soft, soft_ref.shape)
    code, head = encode(total, [])
    for k in range(out_ref.shape[0]):
        out_ref[k, 0:rows] = code
        out_ref[k, rows : rows + HEAD] = head


def update_kernel(core_ref, own_ref, other_ref, prev_ref, lgd_ref, elig_ref, unnorm_ref, expot_ref, tot_ref):
    rows = prev_ref.shape[0]
    step = pl.program_id(0)
    mine = (step // (pl.num_programs(0) // 2)) == core_ref[0]
    pay = jnp.where(mine, own_ref[0], other_ref[0])
    gradient = decode(pay[0:rows], pay[rows : rows + HEAD].astype(f32))
    gradient = lgd_ref[...] * elig_ref[...].astype(f32) * gradient
    unnorm = prev_ref[...] * jnp.exp(-STEP_RATE * gradient)
    unnorm_ref[...] = unnorm
    expot_ref[...] = jnp.transpose(unnorm * lgd_ref[...]).astype(bf16)

    @pl.when(step == 0)
    def _():
        tot_ref[...] = jnp.zeros_like(tot_ref)

    tot_ref[0:1] += jnp.sum(unnorm, axis=0, keepdims=True)


def scale_kernel(unnorm_ref, tot_ref, out_ref):
    out_ref[...] = unnorm_ref[...] * tot_ref[0:1]


def whole(shape):
    return pl.BlockSpec(shape, lambda *_: (0,) * len(shape))


def rounded(value):
    return lax.reduce_precision(value, 8, 7)


def on_device(factors, idiosyncratic, loadings, rating, barrier, loss_given, sector, allowed, holdings):
    sds = jax.ShapeDtypeStruct
    n_obl, n_x, n_c = lax.axis_size(OBL), lax.axis_size("x"), lax.axis_size("c")
    obl_dev, scn_dev = idiosyncratic.shape
    mandates = holdings.shape[1]
    obligors = obl_dev * n_obl
    scenarios = scn_dev * n_x * n_c
    tail_scale = 1.0 / ((1.0 - LEVEL) * scenarios)
    rs, ro = scn_dev // n_obl, obl_dev // (n_x * n_c)
    ps, po = rs + HEAD, ro + HEAD
    half = obl_dev // n_c
    core = lax.axis_index("c").astype(jnp.int32).reshape(1)
    lgd = loss_given[:, None]
    row8 = sds((8, mandates), f32)

    hot = rating[:, None] == jnp.arange(barrier.shape[0])[None, :]
    bar = jnp.sum(jnp.where(hot, barrier[None, :], 0.0), axis=1)
    bar_a = rounded(bar)
    bar_b = rounded(bar - bar_a)
    bar_c = bar - bar_a - bar_b
    parts = -jnp.stack([bar_a, bar_b, bar_c], axis=1)
    fdim = factors.shape[1]
    load_aug = jnp.concatenate([loadings, jnp.pad(parts, ((0, 0), (0, 125))).astype(bf16)], axis=1)
    ones = (jnp.arange(128) < 3).astype(bf16)
    fac_aug = jnp.concatenate([factors, jnp.broadcast_to(ones, (scn_dev, 128))], axis=1)

    blk = pl.BlockSpec((ro, mandates), lambda i, *_: (i, 0))
    col = pl.BlockSpec((ro, 1), lambda i, *_: (i, 0))
    colt = pl.BlockSpec((mandates, ro), lambda i, *_: (0, i))
    n_ro = obl_dev // ro
    prev, elig, expot, tot = call(
        setup_kernel,
        (n_ro,),
        [blk, col, col, whole((allowed.shape[1], mandates))],
        [blk, blk, colt, whole((8, mandates))],
        [sds((obl_dev, mandates), f32), sds((obl_dev, mandates), bf16), sds((mandates, obl_dev), bf16), row8],
        nbytes=obl_dev * mandates * 12,
        name="setup",
    )(holdings, lgd, sector[:, None], allowed.T.astype(bf16))

    results = []
    prob = None
    for iteration in range(STEPS):
        pay_shape = sds((n_obl, ps, mandates), bf16)
        pay_spec = pl.BlockSpec((1, ps, mandates), lambda i, *_: (i, 0, 0))
        if iteration == 0:
            prob, pay = call(
                first_losses_kernel,
                (n_obl,),
                [
                    whole((obl_dev, fdim + 128)),
                    pl.BlockSpec((rs, fdim + 128), lambda i: (i, 0)),
                    pl.BlockSpec((obl_dev, rs), lambda i: (0, i)),
                    whole((mandates, obl_dev)),
                    whole((8, mandates)),
                ],
                [pl.BlockSpec((obl_dev, rs), lambda i: (0, i)), pay_spec],
                [sds((obl_dev, scn_dev), bf16), pay_shape],
                scratch=[pltpu.VMEM((mandates, rs), f32)],
                flops=4 * obl_dev * scn_dev * mandates,
                nbytes=obl_dev * scn_dev * 4,
                name="first_losses",
            )(load_aug, fac_aug, idiosyncratic, expot, tot)
        else:
            pay = call(
                losses_kernel,
                (n_obl,),
                [
                    pl.BlockSpec((obl_dev, rs), lambda i: (0, i)),
                    whole((mandates, obl_dev)),
                    whole((8, mandates)),
                ],
                pay_spec,
                pay_shape,
                flops=2 * obl_dev * scn_dev * mandates,
                nbytes=obl_dev * scn_dev * 2,
                name="losses",
            )(prob, expot, tot)
        pay = lax.all_to_all(pay, OBL, 0, 0, tiled=True)
        group = max(1, n_obl // 4)
        pay = call(
            chunk_kernel,
            (n_obl // group,),
            [pl.BlockSpec((group, ps, mandates), lambda i: (i, 0, 0))],
            whole((n_obl, ps, mandates)),
            pay_shape,
            scratch=[pltpu.VMEM((rs, mandates), f32), pltpu.VMEM((8, mandates), f32)],
            nbytes=n_obl * ps * mandates * 4,
            name="chunk",
        )(pay)
        pay = lax.all_to_all(pay, OBL, 0, 0, tiled=True)

        heads = pay[:, rs : rs + 8].astype(f32)
        means = heads[:, 2] + heads[:, 3] + heads[:, 4]
        seconds = heads[:, 5] + heads[:, 6] + heads[:, 7]
        mean = jnp.sum(means, 0) / n_obl
        second = jnp.sum(seconds, 0) + rs * jnp.sum(jnp.square(means - mean), 0)
        both = jnp.broadcast_to(jnp.stack([mean, second])[None], (n_x * n_c, 2, mandates))
        both = lax.all_to_all(both, SCN, 0, 0, tiled=True)
        means, seconds = both[:, 0], both[:, 1]
        center = jnp.sum(means, 0) / (n_x * n_c)
        spread = (jnp.sum(seconds, 0) + scn_dev * jnp.sum(jnp.square(means - center), 0)) / scenarios
        deviation = jnp.sqrt(spread + EPSILON)
        thresh = center + QUANTILE * deviation
        width = SMOOTH * deviation
        stat = jnp.concatenate([jnp.stack([thresh, 1.0 / width]), jnp.zeros((6, mandates), f32)])

        weight, soft = call(
            functools.partial(tail_kernel, tail_scale),
            (n_obl,),
            [pay_spec, whole((8, mandates))],
            [pl.BlockSpec((rs, mandates), lambda i: (i, 0)), whole((8, mandates))],
            [sds((scn_dev, mandates), bf16), row8],
            nbytes=scn_dev * mandates * 4,
            name="tail",
        )(pay, stat)
        gblock = min(256, half)
        n_half = half // gblock

        def gradient_of(which):
            return call(
                gradient_kernel,
                (n_half,),
                [
                    pl.BlockSpec((gblock, scn_dev), lambda i, h: (h[0] * n_half + i, 0)),
                    whole((scn_dev, mandates)),
                ],
                pl.BlockSpec((gblock, mandates), lambda i, h: (i, 0)),
                sds((half, mandates), f32),
                prefetch=1,
                flops=2 * half * scn_dev * mandates,
                nbytes=half * scn_dev * 2,
                name="gradient",
            )(which, prob, weight)

        swap = [(0, 1), (1, 0)]
        sent = lax.ppermute(gradient_of(1 - core), "c", swap)
        soft_other = lax.ppermute(soft, "c", swap)
        kept = gradient_of(core)
        gpay_shape = sds((n_x, po, mandates), bf16)
        gpay_spec = pl.BlockSpec((1, po, mandates), lambda i, *_: (i, 0, 0))
        pay = call(
            pair_kernel,
            (n_x,),
            [blk, blk, whole((8, mandates)), whole((8, mandates))],
            gpay_spec,
            gpay_shape,
            nbytes=half * mandates * 10,
            name="pair",
        )(kept, sent, soft, soft_other)
        pay = lax.all_to_all(pay, "x", 0, 0, tiled=True)
        pay, soft = call(
            whole_kernel,
            (1,),
            [whole((n_x, po, mandates))],
            [whole((n_x, po, mandates)), whole((8, mandates))],
            [gpay_shape, row8],
            nbytes=half * mandates * 4,
            name="whole",
        )(pay)
        results.append(thresh + width * (soft[0] * tail_scale))
        pay = lax.all_to_all(pay, "x", 0, 0, tiled=True)
        other = lax.ppermute(pay, "c", swap)
        gspec = pl.BlockSpec((1, po, mandates), lambda i, *_: (i % n_x, 0, 0))
        prev, expot, tot = call(
            update_kernel,
            (n_ro,),
            [gspec, gspec, blk, col, blk],
            [blk, colt, whole((8, mandates))],
            [sds((obl_dev, mandates), f32), sds((mandates, obl_dev), bf16), row8],
            prefetch=1,
            nbytes=obl_dev * mandates * 14,
            name="update",
        )(core, pay, other, prev, lgd, elig)

    totals = lax.all_to_all(jnp.broadcast_to(tot[None], (n_obl, 8, mandates)), OBL, 0, 0, tiled=True)
    factor = obligors / jnp.sum(totals, axis=0)
    positions = call(
        scale_kernel,
        (max(1, obl_dev // 512),),
        [pl.BlockSpec((min(512, obl_dev), mandates), lambda i: (i, 0)), whole((8, mandates))],
        pl.BlockSpec((min(512, obl_dev), mandates), lambda i: (i, 0)),
        sds((obl_dev, mandates), f32),
        nbytes=obl_dev * mandates * 8,
        name="scale",
    )(prev, factor)
    return (positions, jnp.stack(results))


def solution(mesh):
    n_obl, n_scn = mesh.shape["obl"], mesh.shape["scn"]
    side = 1
    while side * side < n_obl:
        side *= 2
    fine = Mesh(mesh.devices.reshape(side, n_obl // side, n_scn // 2, 2), ("y", "z", "x", "c"))
    in_specs = (P(SCN, None), P(OBL, SCN), P(OBL, None), P(OBL), P(), P(OBL), P(OBL), P(), P(OBL, None))
    return jax.shard_map(on_device, mesh=fine, in_specs=in_specs, out_specs=(P(OBL, None), P()), check_vma=False)
```

```python
import functools

import jax
import jax.numpy as jnp
from jax import lax
from jax.experimental import pallas as pl
from jax.experimental.pallas import tpu as pltpu
from jax.sharding import Mesh
from jax.sharding import PartitionSpec as P

STEPS = 2
OBL = ("y", "z")
SCN = ("x", "c")
IDIO_SCALE = 0.8
LEVEL = 0.99
QUANTILE = 2.326
SMOOTH = 0.5
EPSILON = 1e-06
STEP_RATE = 8.0
HEAD = 16
SPAN = 127.0
INTERPRET = False

f32 = jnp.float32
bf16 = jnp.bfloat16


def call(kernel, grid, in_specs, out_specs, out_shape, scratch=(), prefetch=0, flops=0, nbytes=0, name=None):
    spec = pltpu.PrefetchScalarGridSpec(
        num_scalar_prefetch=prefetch, grid=grid, in_specs=in_specs, out_specs=out_specs, scratch_shapes=list(scratch)
    )
    return pl.pallas_call(
        kernel,
        grid_spec=spec,
        out_shape=out_shape,
        compiler_params=pltpu.CompilerParams(vmem_limit_bytes=24 * 1024 * 1024),
        cost_estimate=pl.CostEstimate(flops=int(flops), bytes_accessed=int(nbytes), transcendentals=0),
        interpret=INTERPRET,
        name=name,
    )


def split3(value):
    a = value.astype(bf16)
    rest = value - a.astype(f32)
    b = rest.astype(bf16)
    c = (rest - b.astype(f32)).astype(bf16)
    return [a.astype(f32), b.astype(f32), c.astype(f32)]


def join3(head, at):
    return head[at : at + 1] + head[at + 1 : at + 2] + head[at + 2 : at + 3]


def encode(values, extra):
    low = jnp.min(values, axis=0, keepdims=True)
    high = jnp.max(values, axis=0, keepdims=True)
    span = jnp.maximum(jnp.maximum(high - low, jnp.abs(low) * (1.0 / 64.0)), 1e-30)
    base = low.astype(bf16).astype(f32)
    span = (span * 1.02).astype(bf16).astype(f32)
    code = jnp.exp((values - base) * (SPAN / span) - 0.5 * SPAN).astype(bf16)
    rows = [base, span]
    for row in extra:
        rows += split3(row)
    rows.append(jnp.zeros((HEAD - len(rows), values.shape[1]), f32))
    return code, jnp.concatenate(rows, axis=0).astype(bf16)


def decode(code, head):
    base, span = head[0:1], head[1:2]
    return (base + 0.5 * span) + jnp.log(code.astype(f32)) * (span * (1.0 / SPAN))


def setup_kernel(hold_ref, lgd_ref, sector_ref, rating_ref, allowed_ref, load_ref, weighted_ref, lge_ref, aug_ref, expot_ref, tot_ref):
    rows = sector_ref.shape[1]
    sectors = allowed_ref.shape[1]
    here = pl.ds(pl.multiple_of(pl.program_id(0) * rows, rows), rows)
    allowed = allowed_ref[...].astype(f32)
    hot = (lax.broadcasted_iota(jnp.int32, (sectors, rows), 0) == sector_ref[...]).astype(f32)
    lgd = lgd_ref[...]
    parts = jnp.concatenate([hot * part for part in split3(lgd)], axis=0)
    dims = (((0,), (1,)), ((), ()))
    elig = lax.dot_general(hot.astype(bf16), allowed.astype(bf16), dims, preferred_element_type=f32)
    thrice = jnp.concatenate([allowed] * 3, axis=1)
    lge = lax.dot_general(parts.astype(bf16), thrice.astype(bf16), dims, preferred_element_type=f32)
    hold = hold_ref[...]
    weighted = elig * hold
    weighted_ref[here] = weighted
    lge_ref[here] = lge
    expot_ref[:, here] = jnp.transpose(lge * hold).astype(bf16)
    lane = lax.broadcasted_iota(jnp.int32, (128, rows), 0)
    rated = ((lane % 16 == rating_ref[...]) & (lane < 48)).astype(f32)
    aug_ref[here] = jnp.concatenate([load_ref[...], jnp.transpose(rated).astype(bf16)], axis=1)

    @pl.when(pl.program_id(0) == 0)
    def _():
        tot_ref[...] = jnp.zeros_like(tot_ref)

    tot_ref[0:1] += jnp.sum(weighted, axis=0, keepdims=True)


def put_chunks(losses, tot_ref, pay_ref):
    rows = pay_ref.shape[1] - HEAD
    for k in range(pay_ref.shape[0]):
        code, head = encode(jnp.transpose(losses[:, k * rows : (k + 1) * rows]), [tot_ref[0:1]])
        pay_ref[k, 0:rows] = code
        pay_ref[k, rows : rows + HEAD] = head


def first_losses_kernel(load_ref, fac_ref, bar_ref, idio_ref, expot_ref, tot_ref, p_ref, pay_ref):
    wide = fac_ref.shape[0]
    cols = pl.ds(pl.multiple_of(pl.program_id(0) * wide, wide), wide)
    block = min(256, load_ref.shape[0])
    fac = jnp.concatenate([fac_ref[...], jnp.broadcast_to(bar_ref[...], (wide, 128))], axis=1)
    for i in range(load_ref.shape[0] // block):
        sl = slice(i * block, (i + 1) * block)
        latent = lax.dot_general(load_ref[sl], fac, (((1,), (1,)), ((), ())), preferred_element_type=f32)
        prob = 0.5 * jnp.tanh(latent + IDIO_SCALE * idio_ref[sl].astype(f32)) + 0.5
        p_ref[sl, cols] = prob.astype(bf16)
    put_chunks(jnp.dot(expot_ref[...], p_ref[:, cols], preferred_element_type=f32), tot_ref, pay_ref)


def losses_kernel(p_ref, expot_ref, tot_ref, pay_ref):
    wide = pay_ref.shape[0] * (pay_ref.shape[1] - HEAD)
    cols = pl.ds(pl.multiple_of(pl.program_id(0) * wide, wide), wide)
    put_chunks(jnp.dot(expot_ref[...], p_ref[:, cols], preferred_element_type=f32), tot_ref, pay_ref)


def chunk_kernel(pay_ref, out_ref, acc_ref, tot_ref):
    step = pl.program_id(0)
    rows = acc_ref.shape[0]

    @pl.when(step == 0)
    def _():
        acc_ref[...] = jnp.zeros_like(acc_ref)
        tot_ref[...] = jnp.zeros_like(tot_ref)

    total = jnp.zeros_like(acc_ref)
    norm = jnp.zeros((1, acc_ref.shape[1]), f32)
    for k in range(pay_ref.shape[0]):
        head = pay_ref[k, rows : rows + HEAD].astype(f32)
        total += decode(pay_ref[k, 0:rows], head)
        norm += join3(head, 2)
    acc_ref[...] += total
    tot_ref[0:1] += norm

    @pl.when(step == pl.num_programs(0) - 1)
    def _():
        losses = acc_ref[...] / tot_ref[0:1]
        mean = jnp.sum(losses, axis=0, keepdims=True) * (1.0 / rows)
        off = losses - mean
        second = jnp.sum(off * off, axis=0, keepdims=True)
        code, head = encode(losses, [mean, second])
        for k in range(out_ref.shape[0]):
            out_ref[k, 0:rows] = code
            out_ref[k, rows : rows + HEAD] = head


def tail_kernel(tail_scale, pay_ref, stat_ref, weight_ref, soft_ref):
    count, rows = pay_ref.shape[0], pay_ref.shape[1] - HEAD
    step = pl.program_id(0)

    @pl.when(step == 0)
    def _():
        soft_ref[...] = jnp.zeros_like(soft_ref)

    for k in range(count):
        head = pay_ref[k, rows : rows + HEAD].astype(f32)
        losses = decode(pay_ref[k, 0:rows], head)
        scaled = (losses - stat_ref[0:1]) * stat_ref[1:2]
        small = jnp.exp(-jnp.abs(scaled))
        grown = 1.0 + small
        sigmoid = jnp.where(scaled >= 0.0, tail_scale, tail_scale * small) / grown
        at = pl.multiple_of((step * count + k) * rows, rows)
        weight_ref[pl.ds(at, rows)] = sigmoid.astype(bf16)
        up = jnp.maximum(scaled, 0.0).reshape(rows // 8, 8, -1).sum(axis=0)
        tile = grown.reshape(rows // 8, 8, -1)
        for _ in range(5):
            if tile.shape[0] % 2 == 0:
                tile = tile[: tile.shape[0] // 2] * tile[tile.shape[0] // 2 :]
        soft_ref[...] += up + jnp.log(tile).sum(axis=0)


def gradient_kernel(half_ref, p_ref, weight_ref, out_ref):
    rows = out_ref.shape[0]
    at = (half_ref[0] * pl.num_programs(0) + pl.program_id(0)) * rows
    out_ref[...] = jnp.dot(
        p_ref[pl.ds(pl.multiple_of(at, rows), rows)], weight_ref[...], preferred_element_type=f32
    )


def pair_kernel(own_ref, other_ref, soft_ref, soft_other_ref, pay_ref):
    rows = own_ref.shape[0]
    code, head = encode(own_ref[...] + other_ref[...], [jnp.sum(soft_ref[...] + soft_other_ref[...], axis=0, keepdims=True)])
    pay_ref[0, 0:rows] = code
    pay_ref[0, rows : rows + HEAD] = head


def whole_kernel(pay_ref, out_ref, soft_ref):
    rows = pay_ref.shape[1] - HEAD
    total = jnp.zeros((rows, pay_ref.shape[2]), f32)
    soft = jnp.zeros((1, pay_ref.shape[2]), f32)
    for k in range(pay_ref.shape[0]):
        head = pay_ref[k, rows : rows + HEAD].astype(f32)
        total += decode(pay_ref[k, 0:rows], head)
        soft += join3(head, 2)
    soft_ref[...] = jnp.broadcast_to(soft, soft_ref.shape)
    code, head = encode(total, [])
    for k in range(out_ref.shape[0]):
        out_ref[k, 0:rows] = code
        out_ref[k, rows : rows + HEAD] = head


def update_kernel(core_ref, own_ref, other_ref, prev_ref, lge_ref, unnorm_ref, expot_ref, tot_ref):
    rows = own_ref.shape[1] - HEAD
    step = pl.program_id(0)
    here = pl.ds(pl.multiple_of(step * rows, rows), rows)
    mine = (step // (pl.num_programs(0) // 2)) == core_ref[0]
    pay = jnp.where(mine, own_ref[0], other_ref[0])
    gradient = decode(pay[0:rows], pay[rows : rows + HEAD].astype(f32))
    lge = lge_ref[here]
    unnorm = prev_ref[here] * jnp.exp(lge * (-STEP_RATE * gradient))
    unnorm_ref[here] = unnorm
    expot_ref[:, here] = jnp.transpose(unnorm * lge).astype(bf16)

    @pl.when(step == 0)
    def _():
        tot_ref[...] = jnp.zeros_like(tot_ref)

    tot_ref[0:1] += jnp.sum(unnorm, axis=0, keepdims=True)


def last_update_kernel(core_ref, own_ref, other_ref, prev_ref, lge_ref, unnorm_ref, tot_ref):
    rows = own_ref.shape[1] - HEAD
    step = pl.program_id(0)
    here = pl.ds(pl.multiple_of(step * rows, rows), rows)
    mine = (step // (pl.num_programs(0) // 2)) == core_ref[0]
    pay = jnp.where(mine, own_ref[0], other_ref[0])
    gradient = decode(pay[0:rows], pay[rows : rows + HEAD].astype(f32))
    unnorm = prev_ref[here] * jnp.exp(lge_ref[here] * (-STEP_RATE * gradient))
    unnorm_ref[here] = unnorm

    @pl.when(step == 0)
    def _():
        tot_ref[...] = jnp.zeros_like(tot_ref)

    tot_ref[0:1] += jnp.sum(unnorm, axis=0, keepdims=True)


def scale_kernel(unnorm_ref, tot_ref, out_ref):
    rows = out_ref.shape[0]
    here = pl.ds(pl.multiple_of(pl.program_id(0) * rows, rows), rows)
    out_ref[...] = unnorm_ref[here] * tot_ref[0:1]


VMEM = pl.BlockSpec(memory_space=pltpu.VMEM)


def near(array):
    return array if INTERPRET else pltpu.with_memory_space_constraint(array, pltpu.VMEM)


def near_shape(shape, dtype):
    return jax.ShapeDtypeStruct(shape, dtype) if INTERPRET else pltpu.VMEM(shape, dtype)


def whole(shape):
    return pl.BlockSpec(shape, lambda *_: (0,) * len(shape))


def rounded(value):
    return lax.reduce_precision(value, 8, 7)


def on_device(factors, idiosyncratic, loadings, rating, barrier, loss_given, sector, allowed, holdings):
    sds = jax.ShapeDtypeStruct
    n_obl, n_x, n_c = lax.axis_size(OBL), lax.axis_size("x"), lax.axis_size("c")
    obl_dev, scn_dev = idiosyncratic.shape
    mandates = holdings.shape[1]
    obligors = obl_dev * n_obl
    scenarios = scn_dev * n_x * n_c
    tail_scale = 1.0 / ((1.0 - LEVEL) * scenarios)
    rs, ro = scn_dev // n_obl, obl_dev // (n_x * n_c)
    ps, po = rs + HEAD, ro + HEAD
    half = obl_dev // n_c
    core = lax.axis_index("c").astype(jnp.int32).reshape(1)
    row8 = sds((8, mandates), f32)
    ratings = barrier.shape[0]
    bar_a = rounded(barrier)
    bar_b = rounded(barrier - bar_a)
    bar_c = barrier - bar_a - bar_b
    bars = -jnp.concatenate([bar_a, bar_b, bar_c])
    bars = jnp.pad(bars, (0, 128 - 3 * ratings)).astype(bf16)[None, :]
    fdim = factors.shape[1]

    blk = pl.BlockSpec((ro, mandates), lambda i, *_: (i, 0))
    line = pl.BlockSpec((1, ro), lambda i, *_: (0, i))
    n_ro = obl_dev // ro
    prev, lge, aug, expot, tot = call(
        setup_kernel,
        (n_ro,),
        [blk, line, line, line, whole(allowed.shape), pl.BlockSpec((ro, fdim), lambda i: (i, 0))],
        [VMEM, VMEM, VMEM, VMEM, whole((8, mandates))],
        [
            near_shape((obl_dev, mandates), f32),
            near_shape((obl_dev, mandates), f32),
            near_shape((obl_dev, fdim + 128), bf16),
            near_shape((mandates, obl_dev), bf16),
            row8,
        ],
        nbytes=obl_dev * mandates * 12,
        name="setup",
    )(holdings, loss_given[None, :], sector[None, :], rating[None, :], allowed, loadings)
    lge = near(lge)

    results = []
    prob = None
    for iteration in range(STEPS):
        pay_shape = sds((n_obl, ps, mandates), bf16)
        pay_spec = pl.BlockSpec((1, ps, mandates), lambda i, *_: (i, 0, 0))
        pair_spec = pl.BlockSpec((2, ps, mandates), lambda i, *_: (i, 0, 0))
        if iteration == 0:
            prob, pay = call(
                first_losses_kernel,
                (n_obl // 2,),
                [
                    VMEM,
                    pl.BlockSpec((2 * rs, fdim), lambda i: (i, 0)),
                    whole((1, 128)),
                    pl.BlockSpec((obl_dev, 2 * rs), lambda i: (0, i)),
                    VMEM,
                    whole((8, mandates)),
                ],
                [VMEM, pair_spec],
                [near_shape((obl_dev, scn_dev), bf16), pay_shape],
                flops=4 * obl_dev * scn_dev * mandates,
                nbytes=obl_dev * scn_dev * 4,
                name="first_losses",
            )(near(aug), factors, bars, idiosyncratic, near(expot), tot)
            prob = near(prob)
        else:
            pay = call(
                losses_kernel,
                (n_obl // 2,),
                [VMEM, VMEM, whole((8, mandates))],
                pair_spec,
                pay_shape,
                flops=2 * obl_dev * scn_dev * mandates,
                nbytes=obl_dev * scn_dev * 2,
                name="losses",
            )(prob, near(expot), tot)
        pay = lax.all_to_all(pay, OBL, 0, 0, tiled=True)
        group = max(1, n_obl // 4)
        pay = call(
            chunk_kernel,
            (n_obl // group,),
            [pl.BlockSpec((group, ps, mandates), lambda i: (i, 0, 0))],
            whole((n_obl, ps, mandates)),
            pay_shape,
            scratch=[pltpu.VMEM((rs, mandates), f32), pltpu.VMEM((8, mandates), f32)],
            nbytes=n_obl * ps * mandates * 4,
            name="chunk",
        )(pay)
        pay = lax.all_to_all(pay, OBL, 0, 0, tiled=True)

        heads = pay[:, rs : rs + 8].astype(f32)
        means = heads[:, 2] + heads[:, 3] + heads[:, 4]
        seconds = heads[:, 5] + heads[:, 6] + heads[:, 7]
        mean = jnp.sum(means, 0) / n_obl
        second = jnp.sum(seconds, 0) + rs * jnp.sum(jnp.square(means - mean), 0)
        both = jnp.broadcast_to(jnp.stack([mean, second])[None], (n_x * n_c, 2, mandates))
        both = lax.all_to_all(both, SCN, 0, 0, tiled=True)
        means, seconds = both[:, 0], both[:, 1]
        center = jnp.sum(means, 0) / (n_x * n_c)
        spread = (jnp.sum(seconds, 0) + scn_dev * jnp.sum(jnp.square(means - center), 0)) / scenarios
        deviation = jnp.sqrt(spread + EPSILON)
        thresh = center + QUANTILE * deviation
        width = SMOOTH * deviation
        stat = jnp.concatenate([jnp.stack([thresh, 1.0 / width]), jnp.zeros((6, mandates), f32)])

        weight, soft = call(
            functools.partial(tail_kernel, tail_scale),
            (n_obl // 4,),
            [pl.BlockSpec((4, ps, mandates), lambda i: (i, 0, 0)), whole((8, mandates))],
            [VMEM, whole((8, mandates))],
            [near_shape((scn_dev, mandates), bf16), row8],
            nbytes=scn_dev * mandates * 4,
            name="tail",
        )(pay, stat)
        weight = near(weight)
        gblock = min(512, half)

        def gradient_of(which):
            return call(
                gradient_kernel,
                (half // gblock,),
                [VMEM, VMEM],
                pl.BlockSpec((gblock, mandates), lambda i, h: (i, 0)),
                sds((half, mandates), f32),
                prefetch=1,
                flops=2 * half * scn_dev * mandates,
                nbytes=half * scn_dev * 2,
                name="gradient",
            )(which, prob, weight)

        swap = [(0, 1), (1, 0)]
        sent = lax.ppermute(gradient_of(1 - core), "c", swap)
        soft_other = lax.ppermute(soft, "c", swap)
        kept = gradient_of(core)
        gpay_shape = sds((n_x, po, mandates), bf16)
        gpay_spec = pl.BlockSpec((1, po, mandates), lambda i, *_: (i, 0, 0))
        pay = call(
            pair_kernel,
            (n_x,),
            [blk, blk, whole((8, mandates)), whole((8, mandates))],
            gpay_spec,
            gpay_shape,
            nbytes=half * mandates * 10,
            name="pair",
        )(kept, sent, soft, soft_other)
        pay = lax.all_to_all(pay, "x", 0, 0, tiled=True)
        pay, soft = call(
            whole_kernel,
            (1,),
            [whole((n_x, po, mandates))],
            [whole((n_x, po, mandates)), whole((8, mandates))],
            [gpay_shape, row8],
            nbytes=half * mandates * 4,
            name="whole",
        )(pay)
        results.append(thresh + width * (soft[0] * tail_scale))
        pay = lax.all_to_all(pay, "x", 0, 0, tiled=True)
        other = lax.ppermute(pay, "c", swap)
        gspec = pl.BlockSpec((1, po, mandates), lambda i, *_: (i % n_x, 0, 0))
        last = iteration == STEPS - 1
        outs = call(
            last_update_kernel if last else update_kernel,
            (n_ro,),
            [gspec, gspec, VMEM, VMEM],
            [VMEM] + [VMEM] * (not last) + [whole((8, mandates))],
            [near_shape((obl_dev, mandates), f32)]
            + [near_shape((mandates, obl_dev), bf16)] * (not last)
            + [row8],
            prefetch=1,
            nbytes=obl_dev * mandates * 14,
            name="update",
        )(core, pay, other, near(prev), lge)
        prev, expot, tot = outs[0], outs[-2], outs[-1]

    totals = lax.all_to_all(jnp.broadcast_to(tot[None], (n_obl, 8, mandates)), OBL, 0, 0, tiled=True)
    factor = obligors / jnp.sum(totals, axis=0)
    positions = call(
        scale_kernel,
        (max(1, obl_dev // 512),),
        [VMEM, whole((8, mandates))],
        pl.BlockSpec((min(512, obl_dev), mandates), lambda i: (i, 0)),
        sds((obl_dev, mandates), f32),
        nbytes=obl_dev * mandates * 8,
        name="scale",
    )(near(prev), factor)
    return (positions, jnp.stack(results))


def solution(mesh):
    n_obl, n_scn = mesh.shape["obl"], mesh.shape["scn"]
    side = 1
    while side * side < n_obl:
        side *= 2
    fine = Mesh(mesh.devices.reshape(side, n_obl // side, n_scn // 2, 2), ("y", "z", "x", "c"))
    in_specs = (P(SCN, None), P(OBL, SCN), P(OBL, None), P(OBL), P(), P(OBL), P(OBL), P(), P(OBL, None))
    return jax.shard_map(on_device, mesh=fine, in_specs=in_specs, out_specs=(P(OBL, None), P()), check_vma=False)
```

```python
import functools

import jax
import jax.numpy as jnp
from jax import lax
from jax.experimental import pallas as pl
from jax.experimental.pallas import tpu as pltpu
from jax.sharding import Mesh
from jax.sharding import PartitionSpec as P

STEPS = 2
OBL = ("y", "z")
SCN = ("x", "c")
IDIO_SCALE = 0.8
LEVEL = 0.99
QUANTILE = 2.326
SMOOTH = 0.5
EPSILON = 1e-06
STEP_RATE = 8.0
HEAD = 8
SPAN = 127.0
INTERPRET = False

f32 = jnp.float32
bf16 = jnp.bfloat16


def call(kernel, grid, in_specs, out_specs, out_shape, scratch=(), prefetch=0, flops=0, nbytes=0, name=None):
    spec = pltpu.PrefetchScalarGridSpec(
        num_scalar_prefetch=prefetch, grid=grid, in_specs=in_specs, out_specs=out_specs, scratch_shapes=list(scratch)
    )
    return pl.pallas_call(
        kernel,
        grid_spec=spec,
        out_shape=out_shape,
        compiler_params=pltpu.CompilerParams(vmem_limit_bytes=24 * 1024 * 1024),
        cost_estimate=pl.CostEstimate(flops=int(flops), bytes_accessed=int(nbytes), transcendentals=0),
        interpret=INTERPRET,
        name=name,
    )


def split3(value):
    a = value.astype(bf16)
    rest = value - a.astype(f32)
    b = rest.astype(bf16)
    c = (rest - b.astype(f32)).astype(bf16)
    return [a.astype(f32), b.astype(f32), c.astype(f32)]


def join3(head, at):
    return head[at : at + 1] + head[at + 1 : at + 2] + head[at + 2 : at + 3]


def encode(values, extra):
    low = jnp.min(values, axis=0, keepdims=True)
    high = jnp.max(values, axis=0, keepdims=True)
    span = jnp.maximum(jnp.maximum(high - low, jnp.abs(low) * (1.0 / 64.0)), 1e-30)
    base = low.astype(bf16).astype(f32)
    span = (span * 1.02).astype(bf16).astype(f32)
    code = jnp.exp((values - base) * (SPAN / span) - 0.5 * SPAN).astype(bf16)
    rows = [base, span]
    for row in extra:
        rows += split3(row)
    if len(rows) < HEAD:
        rows.append(jnp.zeros((HEAD - len(rows), values.shape[1]), f32))
    return code, jnp.concatenate(rows, axis=0).astype(bf16)


def decode(code, head):
    base, span = head[0:1], head[1:2]
    return (base + 0.5 * span) + jnp.log(code.astype(f32)) * (span * (1.0 / SPAN))


def setup_kernel(hold_ref, lgd_ref, sector_ref, rating_ref, allowed_ref, load_ref, weighted_ref, lge_ref, aug_ref, expot_ref, tot_ref):
    rows = sector_ref.shape[1]
    sectors = allowed_ref.shape[0]
    here = pl.ds(pl.multiple_of(pl.program_id(0) * rows, rows), rows)
    allowed = allowed_ref[...].astype(f32)
    hot = (lax.broadcasted_iota(jnp.int32, (sectors, rows), 0) == sector_ref[...]).astype(f32)
    lgd = lgd_ref[...]
    parts = jnp.concatenate([hot * part for part in split3(lgd)], axis=0)
    dims = (((0,), (0,)), ((), ()))
    elig = lax.dot_general(hot.astype(bf16), allowed.astype(bf16), dims, preferred_element_type=f32)
    thrice = jnp.concatenate([allowed] * 3, axis=0)
    lge = lax.dot_general(parts.astype(bf16), thrice.astype(bf16), dims, preferred_element_type=f32)
    hold = hold_ref[...]
    weighted = elig * hold
    weighted_ref[here] = weighted
    lge_ref[here] = lge
    expot_ref[:, here] = jnp.transpose(lge * hold).astype(bf16)
    lane = lax.broadcasted_iota(jnp.int32, (128, rows), 0)
    rated = ((lane % 16 == rating_ref[...]) & (lane < 48)).astype(f32)
    aug_ref[here] = jnp.concatenate([load_ref[...], jnp.transpose(rated).astype(bf16)], axis=1)

    @pl.when(pl.program_id(0) == 0)
    def _():
        tot_ref[...] = jnp.zeros_like(tot_ref)

    tot_ref[0:1] += jnp.sum(weighted, axis=0, keepdims=True)


def put_chunks(losses, tot_ref, pay_ref):
    rows = pay_ref.shape[1] - HEAD
    for k in range(pay_ref.shape[0]):
        code, head = encode(jnp.transpose(losses[:, k * rows : (k + 1) * rows]), [tot_ref[0:1]])
        pay_ref[k, 0:rows] = code
        pay_ref[k, rows : rows + HEAD] = head


def first_losses_kernel(load_ref, fac_ref, bar_ref, idio_ref, expot_ref, tot_ref, p_ref, pay_ref):
    wide = fac_ref.shape[0]
    cols = pl.ds(pl.multiple_of(pl.program_id(0) * wide, wide), wide)
    block = min(256, load_ref.shape[0])
    fac = jnp.concatenate([fac_ref[...], jnp.broadcast_to(bar_ref[...], (wide, 128))], axis=1)
    for i in range(load_ref.shape[0] // block):
        sl = slice(i * block, (i + 1) * block)
        latent = lax.dot_general(load_ref[sl], fac, (((1,), (1,)), ((), ())), preferred_element_type=f32)
        prob = 0.5 * jnp.tanh(latent + IDIO_SCALE * idio_ref[sl].astype(f32)) + 0.5
        p_ref[sl, cols] = prob.astype(bf16)
    put_chunks(jnp.dot(expot_ref[...], p_ref[:, cols], preferred_element_type=f32), tot_ref, pay_ref)


def losses_kernel(p_ref, expot_ref, tot_ref, pay_ref):
    wide = pay_ref.shape[0] * (pay_ref.shape[1] - HEAD)
    cols = pl.ds(pl.multiple_of(pl.program_id(0) * wide, wide), wide)
    put_chunks(jnp.dot(expot_ref[...], p_ref[:, cols], preferred_element_type=f32), tot_ref, pay_ref)


def chunk_kernel(pay_ref, out_ref, acc_ref, tot_ref):
    step = pl.program_id(0)
    rows = acc_ref.shape[0]

    @pl.when(step == 0)
    def _():
        acc_ref[...] = jnp.zeros_like(acc_ref)
        tot_ref[...] = jnp.zeros_like(tot_ref)

    total = jnp.zeros_like(acc_ref)
    norm = jnp.zeros((1, acc_ref.shape[1]), f32)
    for k in range(pay_ref.shape[0]):
        head = pay_ref[k, rows : rows + HEAD].astype(f32)
        total += decode(pay_ref[k, 0:rows], head)
        norm += join3(head, 2)
    acc_ref[...] += total
    tot_ref[0:1] += norm

    @pl.when(step == pl.num_programs(0) - 1)
    def _():
        losses = acc_ref[...] / tot_ref[0:1]
        mean = jnp.sum(losses, axis=0, keepdims=True) * (1.0 / rows)
        off = losses - mean
        second = jnp.sum(off * off, axis=0, keepdims=True)
        code, head = encode(losses, [mean, second])
        for k in range(out_ref.shape[0]):
            out_ref[k, 0:rows] = code
            out_ref[k, rows : rows + HEAD] = head


def stats_kernel(rows, head_ref, out_ref):
    count = head_ref.shape[0]
    heads = [head_ref[k].astype(f32) for k in range(count)]
    means = [join3(head, 2) for head in heads]
    mean = sum(means) * (1.0 / count)
    second = sum(join3(head, 5) for head in heads)
    second += rows * sum(jnp.square(each - mean) for each in means)
    both = jnp.concatenate([mean, second], axis=0)
    for k in range(out_ref.shape[0]):
        out_ref[k] = both


def tail_kernel(tail_scale, scenarios, pay_ref, both_ref, weight_ref, soft_ref, stat_ref):
    count, rows = pay_ref.shape[0], pay_ref.shape[1] - HEAD
    step = pl.program_id(0)
    groups = both_ref.shape[0]
    means = [both_ref[k, 0:1] for k in range(groups)]
    center = sum(means) * (1.0 / groups)
    spread = sum(both_ref[k, 1:2] for k in range(groups)) * (1.0 / scenarios)
    spread += sum(jnp.square(each - center) for each in means) * (1.0 / groups)
    deviation = jnp.sqrt(spread + EPSILON)
    thresh = center + QUANTILE * deviation
    width = SMOOTH * deviation
    narrow = 1.0 / width

    @pl.when(step == 0)
    def _():
        soft_ref[...] = jnp.zeros_like(soft_ref)
        stat_ref[0:1] = thresh
        stat_ref[1:2] = width

    for k in range(count):
        head = pay_ref[k, rows : rows + HEAD].astype(f32)
        losses = decode(pay_ref[k, 0:rows], head)
        scaled = (losses - thresh) * narrow
        small = jnp.exp(-jnp.abs(scaled))
        grown = 1.0 + small
        sigmoid = jnp.where(scaled >= 0.0, tail_scale, tail_scale * small) / grown
        at = pl.multiple_of((step * count + k) * rows, rows)
        weight_ref[pl.ds(at, rows)] = sigmoid.astype(bf16)
        up = jnp.maximum(scaled, 0.0).reshape(rows // 8, 8, -1).sum(axis=0)
        tile = grown.reshape(rows // 8, 8, -1)
        for _ in range(5):
            if tile.shape[0] % 2 == 0:
                tile = tile[: tile.shape[0] // 2] * tile[tile.shape[0] // 2 :]
        soft_ref[...] += up + jnp.log(tile).sum(axis=0)


def gradient_kernel(own, p_ref, weight_ref, out_ref):
    rows = out_ref.shape[0]
    core = lax.axis_index("c")
    half = core if own else 1 - core
    at = (half * pl.num_programs(0) + pl.program_id(0)) * rows
    out_ref[...] = jnp.dot(
        p_ref[pl.ds(pl.multiple_of(at, rows), rows)], weight_ref[...], preferred_element_type=f32
    )


def pair_kernel(own_ref, other_ref, soft_ref, soft_other_ref, *pay_refs):
    count = len(pay_refs)
    rows = pay_refs[0].shape[0] - HEAD
    soft = jnp.sum(soft_ref[...] + soft_other_ref[...], axis=0, keepdims=True)
    for k, pay_ref in enumerate(pay_refs):
        at = pl.multiple_of(lax.rem(lax.axis_index("x") + k, count) * rows, rows)
        code, head = encode(own_ref[pl.ds(at, rows)] + other_ref[pl.ds(at, rows)], [soft])
        pay_ref[0:rows] = code
        pay_ref[rows : rows + HEAD] = head


def whole_kernel(tail_scale, stat_ref, *refs):
    pay_refs, out_ref, short_ref = refs[:-2], refs[-2], refs[-1]
    rows = out_ref.shape[0] - HEAD
    total = jnp.zeros((rows, out_ref.shape[1]), f32)
    soft = jnp.zeros((1, out_ref.shape[1]), f32)
    for pay_ref in pay_refs:
        head = pay_ref[rows : rows + HEAD].astype(f32)
        total += decode(pay_ref[0:rows], head)
        soft += join3(head, 2)
    code, head = encode(total, [])
    out_ref[0:rows] = code
    out_ref[rows : rows + HEAD] = head
    short_ref[...] = jnp.broadcast_to(stat_ref[0:1] + stat_ref[1:2] * (soft * tail_scale), short_ref.shape)


def update_kernel(count, last, *refs):
    own_refs, other_refs = refs[:count], refs[count : 2 * count]
    prev_ref, lge_ref, unnorm_ref = refs[2 * count : 2 * count + 3]
    rows = own_refs[0].shape[0] - HEAD
    core = lax.axis_index("c")
    total = jnp.zeros((1, prev_ref.shape[1]), f32)
    for half, pay_refs in ((core, own_refs), (1 - core, other_refs)):
        for k, pay_ref in enumerate(pay_refs):
            at = (half * count + lax.rem(lax.axis_index("x") + (count - k), count)) * rows
            here = pl.ds(pl.multiple_of(at, rows), rows)
            gradient = decode(pay_ref[0:rows], pay_ref[rows : rows + HEAD].astype(f32))
            lge = lge_ref[here]
            unnorm = prev_ref[here] * jnp.exp(lge * (-STEP_RATE * gradient))
            unnorm_ref[here] = unnorm
            total += jnp.sum(unnorm, axis=0, keepdims=True)
            if not last:
                refs[-2][:, here] = jnp.transpose(unnorm * lge).astype(bf16)
    refs[-1][...] = jnp.broadcast_to(total, refs[-1].shape)


def scale_kernel(obligors, unnorm_ref, totals_ref, out_ref):
    rows = out_ref.shape[0]
    here = pl.ds(pl.multiple_of(pl.program_id(0) * rows, rows), rows)
    total = sum(totals_ref[k, 0:1] for k in range(totals_ref.shape[0]))
    out_ref[...] = unnorm_ref[here] * (obligors / total)


VMEM = pl.BlockSpec(memory_space=pltpu.VMEM)


def near(array):
    return array if INTERPRET else pltpu.with_memory_space_constraint(array, pltpu.VMEM)


def far(array):
    return array if INTERPRET else pltpu.with_memory_space_constraint(array, pltpu.HBM)


def near_shape(shape, dtype):
    return jax.ShapeDtypeStruct(shape, dtype) if INTERPRET else pltpu.VMEM(shape, dtype)


def whole(shape):
    return pl.BlockSpec(shape, lambda *_: (0,) * len(shape))


def rounded(value):
    return lax.reduce_precision(value, 8, 7)


def on_device(factors, idiosyncratic, loadings, rating, barrier, loss_given, sector, allowed, holdings):
    sds = jax.ShapeDtypeStruct
    n_obl, n_x, n_c = lax.axis_size(OBL), lax.axis_size("x"), lax.axis_size("c")
    obl_dev, scn_dev = idiosyncratic.shape
    mandates = holdings.shape[1]
    obligors = obl_dev * n_obl
    scenarios = scn_dev * n_x * n_c
    tail_scale = 1.0 / ((1.0 - LEVEL) * scenarios)
    rs, ro = scn_dev // n_obl, obl_dev // (n_x * n_c)
    ps, po = rs + HEAD, ro + HEAD
    half = obl_dev // n_c
    row8 = sds((8, mandates), f32)
    ratings = barrier.shape[0]
    bar_a = rounded(barrier)
    bar_b = rounded(barrier - bar_a)
    bar_c = barrier - bar_a - bar_b
    bars = -jnp.concatenate([bar_a, bar_b, bar_c])
    bars = jnp.pad(bars, (0, 128 - 3 * ratings)).astype(bf16)[None, :]
    fdim = factors.shape[1]

    blk = pl.BlockSpec((ro, mandates), lambda i, *_: (i, 0))
    line = pl.BlockSpec((1, ro), lambda i, *_: (0, i))
    n_ro = obl_dev // ro
    prev, lge, aug, expot, tot = call(
        setup_kernel,
        (n_ro,),
        [blk, line, line, line, whole(allowed.shape[::-1]), pl.BlockSpec((ro, fdim), lambda i: (i, 0))],
        [VMEM, VMEM, VMEM, VMEM, whole((8, mandates))],
        [
            near_shape((obl_dev, mandates), f32),
            near_shape((obl_dev, mandates), f32),
            near_shape((obl_dev, fdim + 128), bf16),
            near_shape((mandates, obl_dev), bf16),
            row8,
        ],
        nbytes=obl_dev * mandates * 12,
        name="setup",
    )(far(holdings), loss_given[None, :], sector[None, :], rating[None, :], allowed.T, far(loadings))
    lge = near(lge)

    results = []
    prob = None
    for iteration in range(STEPS):
        pay_shape = sds((n_obl, ps, mandates), bf16)
        pay_spec = pl.BlockSpec((1, ps, mandates), lambda i, *_: (i, 0, 0))
        pair_spec = pl.BlockSpec((2, ps, mandates), lambda i, *_: (i, 0, 0))
        if iteration == 0:
            prob, pay = call(
                first_losses_kernel,
                (n_obl // 2,),
                [
                    VMEM,
                    pl.BlockSpec((2 * rs, fdim), lambda i: (i, 0)),
                    whole((1, 128)),
                    pl.BlockSpec((obl_dev, 2 * rs), lambda i: (0, i)),
                    VMEM,
                    whole((8, mandates)),
                ],
                [VMEM, pair_spec],
                [near_shape((obl_dev, scn_dev), bf16), pay_shape],
                flops=4 * obl_dev * scn_dev * mandates,
                nbytes=obl_dev * scn_dev * 4,
                name="first_losses",
            )(near(aug), factors, bars, idiosyncratic, near(expot), tot)
            prob = near(prob)
        else:
            pay = call(
                losses_kernel,
                (n_obl // 2,),
                [VMEM, VMEM, whole((8, mandates))],
                pair_spec,
                pay_shape,
                flops=2 * obl_dev * scn_dev * mandates,
                nbytes=obl_dev * scn_dev * 2,
                name="losses",
            )(prob, near(expot), tot)
        pay = lax.all_to_all(pay, OBL, 0, 0, tiled=True)
        group = max(1, n_obl // 4)
        pay = call(
            chunk_kernel,
            (n_obl // group,),
            [pl.BlockSpec((group, ps, mandates), lambda i: (i, 0, 0))],
            whole((n_obl, ps, mandates)),
            pay_shape,
            scratch=[pltpu.VMEM((rs, mandates), f32), pltpu.VMEM((8, mandates), f32)],
            nbytes=n_obl * ps * mandates * 4,
            name="chunk",
        )(pay)
        pay = lax.all_to_all(pay, OBL, 0, 0, tiled=True)

        n_scn = n_x * n_c
        both = call(
            functools.partial(stats_kernel, rs),
            (1,),
            [pl.BlockSpec((n_obl, HEAD, mandates), lambda i: (0, rs // HEAD, 0))],
            whole((n_scn, 2, mandates)),
            sds((n_scn, 2, mandates), f32),
            name="stats",
        )(pay)
        both = lax.all_to_all(both, SCN, 0, 0, tiled=True)
        weight, soft, stat = call(
            functools.partial(tail_kernel, tail_scale, scenarios),
            (n_obl // 4,),
            [pl.BlockSpec((4, ps, mandates), lambda i: (i, 0, 0)), whole((n_scn, 2, mandates))],
            [VMEM, whole((8, mandates)), whole((8, mandates))],
            [near_shape((scn_dev, mandates), bf16), row8, row8],
            nbytes=scn_dev * mandates * 4,
            name="tail",
        )(pay, both)
        weight = near(weight)
        gblock = min(512, half)

        def gradient_of(own):
            return call(
                functools.partial(gradient_kernel, own),
                (half // gblock,),
                [VMEM, VMEM],
                pl.BlockSpec((gblock, mandates), lambda i: (i, 0)),
                sds((half, mandates), f32),
                flops=2 * half * scn_dev * mandates,
                nbytes=half * scn_dev * 2,
                name="gradient",
            )(prob, weight)

        swap = [(0, 1), (1, 0)]
        sent = lax.ppermute(gradient_of(False), "c", swap)
        soft_other = lax.ppermute(soft, "c", swap)
        kept = gradient_of(True)
        gshape = sds((po, mandates), bf16)
        hops = {k: [(i, (i + k) % n_x) for i in range(n_x)] for k in range(1, n_x)}
        order = sorted(hops, key=lambda k: -min(k, n_x - k))
        slots = call(
            pair_kernel,
            (1,),
            [VMEM, VMEM, whole((8, mandates)), whole((8, mandates))],
            [VMEM] * n_x,
            [gshape] * n_x,
            nbytes=half * mandates * 10,
            name="pair",
        )(kept, sent, soft, soft_other)
        slots = list(slots)
        for k in order:
            slots[k] = lax.ppermute(slots[k], "x", hops[k])
        pay, short = call(
            functools.partial(whole_kernel, tail_scale),
            (1,),
            [whole((8, mandates))] + [VMEM] * n_x,
            [VMEM, whole((8, mandates))],
            [gshape, row8],
            nbytes=half * mandates * 4,
            name="whole",
        )(stat, *slots)
        results.append(short[0])
        slots = [pay] * n_x
        for k in order:
            slots[k] = lax.ppermute(pay, "x", hops[k])
        others = [lax.ppermute(slot, "c", swap) for slot in slots]
        last = iteration == STEPS - 1
        tot_shape = (n_obl if last else 1, 8, mandates)
        outs = call(
            functools.partial(update_kernel, n_x, last),
            (1,),
            [VMEM] * (2 * n_x + 2),
            [VMEM] + [VMEM] * (not last) + [VMEM],
            [near_shape((obl_dev, mandates), f32)]
            + [near_shape((mandates, obl_dev), bf16)] * (not last)
            + [sds(tot_shape, f32)],
            nbytes=obl_dev * mandates * 14,
            name="update",
        )(*slots, *others, near(prev), lge)
        prev, expot, tot = outs[0], outs[-2], outs[-1]
        if not last:
            tot = tot[0]

    totals = lax.all_to_all(tot, OBL, 0, 0, tiled=True)
    positions = call(
        functools.partial(scale_kernel, obligors),
        (max(1, obl_dev // 512),),
        [VMEM, whole((n_obl, 8, mandates))],
        pl.BlockSpec((min(512, obl_dev), mandates), lambda i: (i, 0)),
        sds((obl_dev, mandates), f32),
        nbytes=obl_dev * mandates * 8,
        name="scale",
    )(near(prev), totals)
    return (positions, jnp.stack(results))


def solution(mesh):
    n_obl, n_scn = mesh.shape["obl"], mesh.shape["scn"]
    side = 1
    while side * side < n_obl:
        side *= 2
    fine = Mesh(mesh.devices.reshape(side, n_obl // side, n_scn // 2, 2), ("y", "z", "x", "c"))
    in_specs = (P(SCN, None), P(OBL, SCN), P(OBL, None), P(OBL), P(), P(OBL), P(OBL), P(), P(OBL, None))
    return jax.shard_map(on_device, mesh=fine, in_specs=in_specs, out_specs=(P(OBL, None), P()), check_vma=False)
```

```python
import functools

import jax
import jax.numpy as jnp
from jax import lax
from jax.experimental import pallas as pl
from jax.experimental.pallas import tpu as pltpu
from jax.sharding import Mesh
from jax.sharding import PartitionSpec as P

STEPS = 2
OBL = ("y", "z")
SCN = ("x", "c")
IDIO_SCALE = 0.8
LEVEL = 0.99
QUANTILE = 2.326
SMOOTH = 0.5
EPSILON = 1e-06
STEP_RATE = 8.0
HEAD = 8
SPAN = 127.0
INTERPRET = False

f32 = jnp.float32
bf16 = jnp.bfloat16


def call(kernel, grid, in_specs, out_specs, out_shape, scratch=(), prefetch=0, flops=0, nbytes=0, name=None):
    spec = pltpu.PrefetchScalarGridSpec(
        num_scalar_prefetch=prefetch, grid=grid, in_specs=in_specs, out_specs=out_specs, scratch_shapes=list(scratch)
    )
    return pl.pallas_call(
        kernel,
        grid_spec=spec,
        out_shape=out_shape,
        compiler_params=pltpu.CompilerParams(vmem_limit_bytes=24 * 1024 * 1024),
        cost_estimate=pl.CostEstimate(flops=int(flops), bytes_accessed=int(nbytes), transcendentals=0),
        interpret=INTERPRET,
        name=name,
    )


def split3(value):
    a = value.astype(bf16)
    rest = value - a.astype(f32)
    b = rest.astype(bf16)
    c = (rest - b.astype(f32)).astype(bf16)
    return [a.astype(f32), b.astype(f32), c.astype(f32)]


def join3(head, at):
    return head[at : at + 1] + head[at + 1 : at + 2] + head[at + 2 : at + 3]


def encode(values, extra):
    low = jnp.min(values, axis=0, keepdims=True)
    high = jnp.max(values, axis=0, keepdims=True)
    span = jnp.maximum(jnp.maximum(high - low, jnp.abs(low) * (1.0 / 64.0)), 1e-30)
    base = low.astype(bf16).astype(f32)
    span = (span * 1.02).astype(bf16).astype(f32)
    code = jnp.exp((values - base) * (SPAN / span) - 0.5 * SPAN).astype(bf16)
    rows = [base, span]
    for row in extra:
        rows += split3(row)
    if len(rows) < HEAD:
        rows.append(jnp.zeros((HEAD - len(rows), values.shape[1]), f32))
    return code, jnp.concatenate(rows, axis=0).astype(bf16)


def decode(code, head):
    base, span = head[0:1], head[1:2]
    return (base + 0.5 * span) + jnp.log(code.astype(f32)) * (span * (1.0 / SPAN))


def edge_of(total, reach):
    span = jnp.maximum(2.02 * reach, 1e-30).astype(bf16).astype(f32)
    rows = [span] + split3(total)
    rows.append(jnp.zeros((128 - len(rows), total.shape[1]), f32))
    return jnp.transpose(jnp.concatenate(rows, axis=0)).astype(bf16)


def put_codes(doubled, edge_ref, pay_ref, at):
    parts, rows = pay_ref.shape[:2]
    span = edge_ref[:, 0:1].astype(f32)
    code = jnp.exp(doubled * (SPAN / span) - 0.5 * SPAN).astype(bf16)
    pay_ref[:, :, at] = code.reshape(parts, rows, -1)

    @pl.when(pl.program_id(0) == 0)
    def _():
        pay_ref[:, :, pay_ref.shape[2] - 128 :] = edge_ref[...].reshape(parts, rows, 128)


def setup_kernel(hold_ref, lgd_ref, sector_ref, rating_ref, allowed_ref, load_ref, weighted_ref, lge_ref, aug_ref, expot_ref, edge_ref, sums_ref):
    rows = sector_ref.shape[1]
    sectors = allowed_ref.shape[0]
    here = pl.ds(pl.multiple_of(pl.program_id(0) * rows, rows), rows)
    allowed = allowed_ref[...].astype(f32)
    hot = (lax.broadcasted_iota(jnp.int32, (sectors, rows), 0) == sector_ref[...]).astype(f32)
    lgd = lgd_ref[...]
    parts = jnp.concatenate([hot * part for part in split3(lgd)], axis=0)
    dims = (((0,), (0,)), ((), ()))
    elig = lax.dot_general(hot.astype(bf16), allowed.astype(bf16), dims, preferred_element_type=f32)
    thrice = jnp.concatenate([allowed] * 3, axis=0)
    lge = lax.dot_general(parts.astype(bf16), thrice.astype(bf16), dims, preferred_element_type=f32)
    hold = hold_ref[...]
    weighted = elig * hold
    weighted_ref[here] = weighted
    lge_ref[here] = lge
    expo = (lge * hold).astype(bf16).astype(f32)
    expot_ref[:, here] = jnp.transpose(expo).astype(bf16)
    lane = lax.broadcasted_iota(jnp.int32, (128, rows), 0)
    rated = ((lane % 16 == rating_ref[...]) & (lane < 48)).astype(f32)
    aug_ref[here] = jnp.concatenate([load_ref[...], jnp.transpose(rated).astype(bf16)], axis=1)

    @pl.when(pl.program_id(0) == 0)
    def _():
        sums_ref[...] = jnp.zeros_like(sums_ref)

    sums_ref[0:1] += jnp.sum(weighted, axis=0, keepdims=True)
    sums_ref[1:2] += jnp.sum(expo, axis=0, keepdims=True)

    @pl.when(pl.program_id(0) == pl.num_programs(0) - 1)
    def _():
        edge_ref[...] = edge_of(sums_ref[0:1], sums_ref[1:2])


def first_losses_kernel(load_ref, fac_ref, bar_ref, idio_ref, expot_ref, edge_ref, p_ref, pay_ref):
    wide = fac_ref.shape[0]
    cols = pl.ds(pl.multiple_of(pl.program_id(0) * wide, wide), wide)
    block = min(256, load_ref.shape[0])
    fac = jnp.concatenate([fac_ref[...], jnp.broadcast_to(bar_ref[...], (wide, 128))], axis=1)
    for i in range(load_ref.shape[0] // block):
        sl = slice(i * block, (i + 1) * block)
        latent = lax.dot_general(load_ref[sl], fac, (((1,), (1,)), ((), ())), preferred_element_type=f32)
        p_ref[sl, cols] = (jnp.tanh(latent + IDIO_SCALE * idio_ref[sl].astype(f32)) + 1.0).astype(bf16)
    put_codes(jnp.dot(expot_ref[...], p_ref[:, cols], preferred_element_type=f32), edge_ref, pay_ref, cols)


def losses_kernel(wide, p_ref, expot_ref, edge_ref, pay_ref):
    cols = pl.ds(pl.multiple_of(pl.program_id(0) * wide, wide), wide)
    put_codes(jnp.dot(expot_ref[...], p_ref[:, cols], preferred_element_type=f32), edge_ref, pay_ref, cols)


def sum_kernel(pay_ref, losses_ref, both_ref):
    count = pay_ref.shape[0]
    wide = losses_ref.shape[1]
    edges = [pay_ref[k, :, wide:].astype(f32) for k in range(count)]
    spans = [edge[:, 0:1] for edge in edges]
    offset = 0.5 * sum(spans)
    scale = 0.5 / sum(edge[:, 1:2] + edge[:, 2:3] + edge[:, 3:4] for edge in edges)
    factors = [span * (1.0 / SPAN) for span in spans]
    piece = min(1024, wide)
    total = 0.0
    for at in range(0, wide, piece):
        part = sum(jnp.log(pay_ref[k, :, at : at + piece].astype(f32)) * factors[k] for k in range(count))
        part = (part + offset) * scale
        losses_ref[:, at : at + piece] = part
        total += jnp.sum(part, axis=1, keepdims=True)
    mean = total * (1.0 / wide)
    second = jnp.sum(jnp.square(losses_ref[...] - mean), axis=1, keepdims=True)
    lane = lax.broadcasted_iota(jnp.int32, both_ref.shape[1:], 1)
    both = jnp.where(lane == 0, mean, jnp.where(lane == 1, second, 0.0))
    for k in range(both_ref.shape[0]):
        both_ref[k] = both


def tail_kernel(tail_scale, scenarios, losses_ref, both_ref, pay_ref):
    groups = both_ref.shape[0]
    wide = losses_ref.shape[1]
    means = [both_ref[k, :, 0:1] for k in range(groups)]
    center = sum(means) * (1.0 / groups)
    spread = sum(both_ref[k, :, 1:2] for k in range(groups)) * (1.0 / scenarios)
    spread += sum(jnp.square(each - center) for each in means) * (1.0 / groups)
    deviation = jnp.sqrt(spread + EPSILON)
    thresh = center + QUANTILE * deviation
    width = SMOOTH * deviation
    narrow = 1.0 / width
    piece = min(1024, wide)
    soft = 0.0
    for at in range(0, wide, piece):
        scaled = (losses_ref[:, at : at + piece] - thresh) * narrow
        small = jnp.exp(-jnp.abs(scaled))
        grown = 1.0 + small
        half = 0.5 * tail_scale
        weight = (jnp.where(scaled >= 0.0, half, half * small) / grown).astype(bf16)
        soft += jnp.sum(jnp.maximum(scaled, 0.0) + jnp.log(grown), axis=1, keepdims=True)
        for k in range(pay_ref.shape[0]):
            pay_ref[k, :, at : at + piece] = weight
    lane = lax.broadcasted_iota(jnp.int32, (pay_ref.shape[1], 128), 1)
    edge = jnp.zeros(lane.shape, f32)
    for at, part in enumerate(split3(soft) + split3(thresh) + split3(width)):
        edge = jnp.where(lane == at, part, edge)
    for k in range(pay_ref.shape[0]):
        pay_ref[k, :, wide:] = edge.astype(bf16)


def heads_kernel(edge_ref, soft_ref, stat_ref):
    rows = jnp.transpose(edge_ref[...].reshape(-1, 128).astype(f32))
    soft_ref[...] = jnp.broadcast_to(join3(rows, 0), soft_ref.shape)
    stat_ref[...] = jnp.zeros_like(stat_ref)
    stat_ref[0:1] = join3(rows, 3)
    stat_ref[1:2] = join3(rows, 6)


def gradient_kernel(own, p_ref, weight_ref, out_ref):
    rows = out_ref.shape[0]
    core = lax.axis_index("c")
    half = core if own else 1 - core
    at = (half * pl.num_programs(0) + pl.program_id(0)) * rows
    weight = weight_ref[:, :, 0 : p_ref.shape[1]].reshape(out_ref.shape[1], -1)
    out_ref[...] = lax.dot_general(
        p_ref[pl.ds(pl.multiple_of(at, rows), rows)],
        weight,
        (((1,), (1,)), ((), ())),
        preferred_element_type=f32,
    )


def pair_kernel(own_ref, other_ref, soft_ref, soft_other_ref, *pay_refs):
    count = len(pay_refs)
    rows = pay_refs[0].shape[0] - HEAD
    soft = soft_ref[0:1] + soft_other_ref[0:1]
    for k, pay_ref in enumerate(pay_refs):
        at = pl.multiple_of(lax.rem(lax.axis_index("x") + k, count) * rows, rows)
        code, head = encode(own_ref[pl.ds(at, rows)] + other_ref[pl.ds(at, rows)], [soft])
        pay_ref[0:rows] = code
        pay_ref[rows : rows + HEAD] = head


def whole_kernel(tail_scale, stat_ref, *refs):
    pay_refs, out_ref, short_ref = refs[:-2], refs[-2], refs[-1]
    rows = out_ref.shape[0] - HEAD
    total = jnp.zeros((rows, out_ref.shape[1]), f32)
    soft = jnp.zeros((1, out_ref.shape[1]), f32)
    for pay_ref in pay_refs:
        head = pay_ref[rows : rows + HEAD].astype(f32)
        total += decode(pay_ref[0:rows], head)
        soft += join3(head, 2)
    code, head = encode(total, [])
    out_ref[0:rows] = code
    out_ref[rows : rows + HEAD] = head
    short_ref[...] = jnp.broadcast_to(stat_ref[0:1] + stat_ref[1:2] * (soft * tail_scale), short_ref.shape)


def update_kernel(count, last, *refs):
    own_refs, other_refs = refs[:count], refs[count : 2 * count]
    prev_ref, lge_ref, unnorm_ref = refs[2 * count : 2 * count + 3]
    rows = own_refs[0].shape[0] - HEAD
    core = lax.axis_index("c")
    total = jnp.zeros((1, prev_ref.shape[1]), f32)
    reach = jnp.zeros((1, prev_ref.shape[1]), f32)
    for half, pay_refs in ((core, own_refs), (1 - core, other_refs)):
        for k, pay_ref in enumerate(pay_refs):
            at = (half * count + lax.rem(lax.axis_index("x") + (count - k), count)) * rows
            here = pl.ds(pl.multiple_of(at, rows), rows)
            gradient = decode(pay_ref[0:rows], pay_ref[rows : rows + HEAD].astype(f32))
            lge = lge_ref[here]
            unnorm = prev_ref[here] * jnp.exp(lge * (-STEP_RATE * gradient))
            unnorm_ref[here] = unnorm
            total += jnp.sum(unnorm, axis=0, keepdims=True)
            if not last:
                expo = (unnorm * lge).astype(bf16).astype(f32)
                refs[-2][:, here] = jnp.transpose(expo).astype(bf16)
                reach += jnp.sum(expo, axis=0, keepdims=True)
    if last:
        refs[-1][...] = jnp.broadcast_to(total[None], refs[-1].shape)
    else:
        refs[-1][...] = edge_of(total, reach)


def scale_kernel(obligors, unnorm_ref, totals_ref, out_ref):
    rows = out_ref.shape[0]
    here = pl.ds(pl.multiple_of(pl.program_id(0) * rows, rows), rows)
    total = sum(totals_ref[k] for k in range(totals_ref.shape[0]))
    out_ref[...] = unnorm_ref[here] * (obligors / total)


VMEM = pl.BlockSpec(memory_space=pltpu.VMEM)


def near(array):
    return array if INTERPRET else pltpu.with_memory_space_constraint(array, pltpu.VMEM)


def far(array):
    return array if INTERPRET else pltpu.with_memory_space_constraint(array, pltpu.HBM)


def near_shape(shape, dtype):
    return jax.ShapeDtypeStruct(shape, dtype) if INTERPRET else pltpu.VMEM(shape, dtype)


def whole(shape):
    return pl.BlockSpec(shape, lambda *_: (0,) * len(shape))


def rounded(value):
    return lax.reduce_precision(value, 8, 7)


def on_device(factors, idiosyncratic, loadings, rating, barrier, loss_given, sector, allowed, holdings):
    sds = jax.ShapeDtypeStruct
    n_obl, n_x, n_c = lax.axis_size(OBL), lax.axis_size("x"), lax.axis_size("c")
    obl_dev, scn_dev = idiosyncratic.shape
    mandates = holdings.shape[1]
    obligors = obl_dev * n_obl
    scenarios = scn_dev * n_x * n_c
    tail_scale = 1.0 / ((1.0 - LEVEL) * scenarios)
    ro = obl_dev // (n_x * n_c)
    po = ro + HEAD
    mr = mandates // n_obl
    half = obl_dev // n_c
    row8 = sds((8, mandates), f32)
    ratings = barrier.shape[0]
    bar_a = rounded(barrier)
    bar_b = rounded(barrier - bar_a)
    bar_c = barrier - bar_a - bar_b
    bars = -jnp.concatenate([bar_a, bar_b, bar_c])
    bars = jnp.pad(bars, (0, 128 - 3 * ratings)).astype(bf16)[None, :]
    fdim = factors.shape[1]

    sb = min(512, obl_dev)
    line = pl.BlockSpec((1, sb), lambda i: (0, i))
    prev, lge, aug, expot, edge = call(
        setup_kernel,
        (obl_dev // sb,),
        [
            pl.BlockSpec((sb, mandates), lambda i: (i, 0)),
            line,
            line,
            line,
            whole(allowed.shape[::-1]),
            pl.BlockSpec((sb, fdim), lambda i: (i, 0)),
        ],
        [VMEM] * 5,
        [
            near_shape((obl_dev, mandates), f32),
            near_shape((obl_dev, mandates), f32),
            near_shape((obl_dev, fdim + 128), bf16),
            near_shape((mandates, obl_dev), bf16),
            near_shape((mandates, 128), bf16),
        ],
        scratch=[pltpu.VMEM((8, mandates), f32)],
        nbytes=obl_dev * mandates * 12,
        name="setup",
    )(far(holdings), far(loss_given[None, :]), far(sector[None, :]), far(rating[None, :]), allowed.T, far(loadings))
    lge = near(lge)

    results = []
    prob = None
    for iteration in range(STEPS):
        pay_shape = sds((n_obl, mr, scn_dev + 128), bf16)
        wide = min(512, scn_dev)
        if iteration == 0:
            prob, pay = call(
                first_losses_kernel,
                (scn_dev // wide,),
                [
                    VMEM,
                    pl.BlockSpec((wide, fdim), lambda i: (i, 0)),
                    whole((1, 128)),
                    pl.BlockSpec((obl_dev, wide), lambda i: (0, i)),
                    VMEM,
                    VMEM,
                ],
                [VMEM, VMEM],
                [near_shape((obl_dev, scn_dev), bf16), pay_shape],
                flops=4 * obl_dev * scn_dev * mandates,
                nbytes=obl_dev * scn_dev * 4,
                name="first_losses",
            )(near(aug), factors, bars, idiosyncratic, near(expot), near(edge))
            prob = near(prob)
        else:
            pay = call(
                functools.partial(losses_kernel, wide),
                (scn_dev // wide,),
                [VMEM, VMEM, VMEM],
                VMEM,
                pay_shape,
                flops=2 * obl_dev * scn_dev * mandates,
                nbytes=obl_dev * scn_dev * 2,
                name="losses",
            )(prob, near(expot), near(edge))
        pay = lax.all_to_all(pay, OBL, 0, 0, tiled=True)
        n_scn = n_x * n_c
        losses, both = call(
            sum_kernel,
            (1,),
            [VMEM],
            [VMEM, VMEM],
            [near_shape((mr, scn_dev), f32), sds((n_scn, mr, 128), f32)],
            nbytes=mandates * scn_dev * 2,
            name="sum",
        )(pay)
        both = lax.all_to_all(both, SCN, 0, 0, tiled=True)
        weight = call(
            functools.partial(tail_kernel, tail_scale, scenarios),
            (1,),
            [VMEM, VMEM],
            VMEM,
            pay_shape,
            nbytes=mandates * scn_dev * 2,
            name="tail",
        )(near(losses), both)
        weight = lax.all_to_all(weight, OBL, 0, 0, tiled=True)
        soft, stat = call(
            heads_kernel,
            (1,),
            [pl.BlockSpec((n_obl, mr, 128), lambda i: (0, 0, scn_dev // 128))],
            [whole((8, mandates)), whole((8, mandates))],
            [row8, row8],
            name="heads",
        )(weight)
        gblock = min(512, half)

        def gradient_of(own):
            return call(
                functools.partial(gradient_kernel, own),
                (half // gblock,),
                [VMEM, VMEM],
                pl.BlockSpec((gblock, mandates), lambda i: (i, 0)),
                sds((half, mandates), f32),
                flops=2 * half * scn_dev * mandates,
                nbytes=half * scn_dev * 2,
                name="gradient",
            )(prob, weight)

        swap = [(0, 1), (1, 0)]
        sent = lax.ppermute(gradient_of(False), "c", swap)
        soft_other = lax.ppermute(soft, "c", swap)
        kept = gradient_of(True)
        gshape = sds((po, mandates), bf16)
        hops = {k: [(i, (i + k) % n_x) for i in range(n_x)] for k in range(1, n_x)}
        order = sorted(hops, key=lambda k: -min(k, n_x - k))
        slots = call(
            pair_kernel,
            (1,),
            [VMEM, VMEM, whole((8, mandates)), whole((8, mandates))],
            [VMEM] * n_x,
            [gshape] * n_x,
            nbytes=half * mandates * 10,
            name="pair",
        )(kept, sent, soft, soft_other)
        slots = list(slots)
        for k in order:
            slots[k] = lax.ppermute(slots[k], "x", hops[k])
        pay, short = call(
            functools.partial(whole_kernel, tail_scale),
            (1,),
            [whole((8, mandates))] + [VMEM] * n_x,
            [VMEM, whole((8, mandates))],
            [gshape, row8],
            nbytes=half * mandates * 4,
            name="whole",
        )(stat, *slots)
        results.append(short[0])
        slots = [pay] * n_x
        for k in order:
            slots[k] = lax.ppermute(pay, "x", hops[k])
        others = [lax.ppermute(slot, "c", swap) for slot in slots]
        last = iteration == STEPS - 1
        outs = call(
            functools.partial(update_kernel, n_x, last),
            (1,),
            [VMEM] * (2 * n_x + 2),
            [VMEM] + [VMEM] * (not last) + [VMEM],
            [near_shape((obl_dev, mandates), f32)]
            + [near_shape((mandates, obl_dev), bf16)] * (not last)
            + [sds((n_obl, 1, mandates), f32) if last else near_shape((mandates, 128), bf16)],
            nbytes=obl_dev * mandates * 14,
            name="update",
        )(*slots, *others, near(prev), lge)
        prev, expot, edge = outs[0], outs[-2], outs[-1]

    totals = lax.all_to_all(edge, OBL, 0, 0, tiled=True)
    positions = call(
        functools.partial(scale_kernel, obligors),
        (max(1, obl_dev // 512),),
        [VMEM, whole((n_obl, 1, mandates))],
        pl.BlockSpec((min(512, obl_dev), mandates), lambda i: (i, 0)),
        sds((obl_dev, mandates), f32),
        nbytes=obl_dev * mandates * 8,
        name="scale",
    )(near(prev), totals)
    return (positions, jnp.stack(results))


def solution(mesh):
    n_obl, n_scn = mesh.shape["obl"], mesh.shape["scn"]
    side = 1
    while side * side < n_obl:
        side *= 2
    fine = Mesh(mesh.devices.reshape(side, n_obl // side, n_scn // 2, 2), ("y", "z", "x", "c"))
    in_specs = (P(SCN, None), P(OBL, SCN), P(OBL, None), P(OBL), P(), P(OBL), P(OBL), P(), P(OBL, None))
    return jax.shard_map(on_device, mesh=fine, in_specs=in_specs, out_specs=(P(OBL, None), P()), check_vma=False)
```

```python
import functools

import jax
import jax.numpy as jnp
from jax import lax
from jax.experimental import pallas as pl
from jax.experimental.pallas import tpu as pltpu
from jax.sharding import Mesh
from jax.sharding import PartitionSpec as P

STEPS = 2
OBL = ("y", "z")
SCN = ("x", "c")
PLANE = ("y", "z", "c")
IDIO_SCALE = 0.8
LEVEL = 0.99
QUANTILE = 2.326
SMOOTH = 0.5
EPSILON = 1e-06
STEP_RATE = 8.0
HEAD = 8
SPAN = 127.0
INTERPRET = False

f32 = jnp.float32
bf16 = jnp.bfloat16


def call(kernel, grid, in_specs, out_specs, out_shape, scratch=(), prefetch=0, flops=0, nbytes=0, name=None):
    spec = pltpu.PrefetchScalarGridSpec(
        num_scalar_prefetch=prefetch, grid=grid, in_specs=in_specs, out_specs=out_specs, scratch_shapes=list(scratch)
    )
    return pl.pallas_call(
        kernel,
        grid_spec=spec,
        out_shape=out_shape,
        compiler_params=pltpu.CompilerParams(vmem_limit_bytes=24 * 1024 * 1024),
        cost_estimate=pl.CostEstimate(flops=int(flops), bytes_accessed=int(nbytes), transcendentals=0),
        interpret=INTERPRET,
        name=name,
    )


def split3(value):
    a = value.astype(bf16)
    rest = value - a.astype(f32)
    b = rest.astype(bf16)
    c = (rest - b.astype(f32)).astype(bf16)
    return [a.astype(f32), b.astype(f32), c.astype(f32)]


def join3(head, at):
    return head[at : at + 1] + head[at + 1 : at + 2] + head[at + 2 : at + 3]


def encode(values, extra):
    low = jnp.min(values, axis=0, keepdims=True)
    high = jnp.max(values, axis=0, keepdims=True)
    span = jnp.maximum(jnp.maximum(high - low, jnp.abs(low) * (1.0 / 64.0)), 1e-30)
    base = low.astype(bf16).astype(f32)
    span = (span * 1.02).astype(bf16).astype(f32)
    code = jnp.exp((values - base) * (SPAN / span) - 0.5 * SPAN).astype(bf16)
    rows = [base, span]
    for row in extra:
        rows += split3(row)
    if len(rows) < HEAD:
        rows.append(jnp.zeros((HEAD - len(rows), values.shape[1]), f32))
    return code, jnp.concatenate(rows, axis=0).astype(bf16)


def decode(code, head):
    base, span = head[0:1], head[1:2]
    return (base + 0.5 * span) + jnp.log(code.astype(f32)) * (span * (1.0 / SPAN))


def edge_of(total, reach):
    span = jnp.maximum(2.02 * reach, 1e-30).astype(bf16).astype(f32)
    rows = [span] + split3(total)
    rows.append(jnp.zeros((128 - len(rows), total.shape[1]), f32))
    return jnp.transpose(jnp.concatenate(rows, axis=0)).astype(bf16)


def put_codes(doubled, edge_ref, pay_ref, at):
    parts, rows = pay_ref.shape[:2]
    span = edge_ref[:, 0:1].astype(f32)
    code = jnp.exp(doubled * (SPAN / span) - 0.5 * SPAN).astype(bf16)
    pay_ref[:, :, at] = code.reshape(parts, rows, -1)

    @pl.when(pl.program_id(0) == 0)
    def _():
        pay_ref[:, :, pay_ref.shape[2] - 128 :] = edge_ref[...].reshape(parts, rows, 128)


def setup_kernel(hold_ref, lgd_ref, sector_ref, rating_ref, allowed_ref, load_ref, weighted_ref, lge_ref, aug_ref, expot_ref, edge_ref, sums_ref):
    rows = sector_ref.shape[1]
    sectors = allowed_ref.shape[0]
    here = pl.ds(pl.multiple_of(pl.program_id(0) * rows, rows), rows)
    allowed = allowed_ref[...].astype(f32)
    hot = (lax.broadcasted_iota(jnp.int32, (sectors, rows), 0) == sector_ref[...]).astype(f32)
    lgd = lgd_ref[...]
    parts = jnp.concatenate([hot * part for part in split3(lgd)], axis=0)
    dims = (((0,), (0,)), ((), ()))
    elig = lax.dot_general(hot.astype(bf16), allowed.astype(bf16), dims, preferred_element_type=f32)
    thrice = jnp.concatenate([allowed] * 3, axis=0)
    lge = lax.dot_general(parts.astype(bf16), thrice.astype(bf16), dims, preferred_element_type=f32)
    hold = hold_ref[...]
    weighted = elig * hold
    weighted_ref[here] = weighted
    lge_ref[here] = lge
    expo = (lge * hold).astype(bf16).astype(f32)
    expot_ref[:, here] = jnp.transpose(expo).astype(bf16)
    lane = lax.broadcasted_iota(jnp.int32, (128, rows), 0)
    rated = ((lane % 16 == rating_ref[...]) & (lane < 48)).astype(f32)
    aug_ref[here] = jnp.concatenate([load_ref[...], jnp.transpose(rated).astype(bf16)], axis=1)

    @pl.when(pl.program_id(0) == 0)
    def _():
        sums_ref[...] = jnp.zeros_like(sums_ref)

    sums_ref[0:1] += jnp.sum(weighted, axis=0, keepdims=True)
    sums_ref[1:2] += jnp.sum(expo, axis=0, keepdims=True)

    @pl.when(pl.program_id(0) == pl.num_programs(0) - 1)
    def _():
        edge_ref[...] = edge_of(sums_ref[0:1], sums_ref[1:2])


def first_losses_kernel(load_ref, fac_ref, bar_ref, idio_ref, expot_ref, edge_ref, p_ref, pay_ref):
    wide = fac_ref.shape[0]
    cols = pl.ds(pl.multiple_of(pl.program_id(0) * wide, wide), wide)
    block = min(256, load_ref.shape[0])
    fac = jnp.concatenate([fac_ref[...], jnp.broadcast_to(bar_ref[...], (wide, 128))], axis=1)
    for i in range(load_ref.shape[0] // block):
        sl = slice(i * block, (i + 1) * block)
        latent = lax.dot_general(load_ref[sl], fac, (((1,), (1,)), ((), ())), preferred_element_type=f32)
        p_ref[sl, cols] = (jnp.tanh(latent + IDIO_SCALE * idio_ref[sl].astype(f32)) + 1.0).astype(bf16)
    put_codes(jnp.dot(expot_ref[...], p_ref[:, cols], preferred_element_type=f32), edge_ref, pay_ref, cols)


def losses_kernel(wide, p_ref, expot_ref, edge_ref, pay_ref):
    cols = pl.ds(pl.multiple_of(pl.program_id(0) * wide, wide), wide)
    put_codes(jnp.dot(expot_ref[...], p_ref[:, cols], preferred_element_type=f32), edge_ref, pay_ref, cols)


def mid_kernel(pay_ref, out_ref, part_ref):
    fewer = out_ref.shape[0]
    count = pay_ref.shape[0] // fewer
    wide = part_ref.shape[2]
    piece = min(1024, wide)
    lane = lax.broadcasted_iota(jnp.int32, (pay_ref.shape[1], 128), 1)
    for q in range(fewer):
        edges = [pay_ref[k * fewer + q, :, wide:].astype(f32) for k in range(count)]
        spans = [edge[:, 0:1] for edge in edges]
        offset = 0.5 * sum(spans)
        factors = [span * (1.0 / SPAN) for span in spans]
        low, high = jnp.inf, -jnp.inf
        for at in range(0, wide, piece):
            codes = [pay_ref[k * fewer + q, :, at : at + piece].astype(f32) for k in range(count)]
            part = sum(jnp.log(code) * factor for code, factor in zip(codes, factors)) + offset
            part_ref[q, :, at : at + piece] = part
            low = jnp.minimum(low, jnp.min(part, axis=1, keepdims=True))
            high = jnp.maximum(high, jnp.max(part, axis=1, keepdims=True))
        span = jnp.maximum(jnp.maximum(high - low, jnp.abs(low) * (1.0 / 64.0)), 1e-30)
        base = low.astype(bf16).astype(f32)
        span = (span * 1.02).astype(bf16).astype(f32)
        for at in range(0, wide, piece):
            part = part_ref[q, :, at : at + piece]
            out_ref[q, :, at : at + piece] = jnp.exp((part - base) * (SPAN / span) - 0.5 * SPAN).astype(bf16)
        total = sum(edge[:, 1:2] + edge[:, 2:3] + edge[:, 3:4] for edge in edges)
        edge = jnp.zeros(lane.shape, f32)
        for at, value in enumerate([base, span] + split3(total)):
            edge = jnp.where(lane == at, value, edge)
        out_ref[q, :, wide:] = edge.astype(bf16)


def sum_kernel(pay_ref, losses_ref, both_ref):
    count = pay_ref.shape[0]
    wide = losses_ref.shape[1]
    edges = [pay_ref[k, :, wide:].astype(f32) for k in range(count)]
    spans = [edge[:, 1:2] for edge in edges]
    offset = sum(edge[:, 0:1] for edge in edges) + 0.5 * sum(spans)
    scale = 0.5 / sum(edge[:, 2:3] + edge[:, 3:4] + edge[:, 4:5] for edge in edges)
    factors = [span * (1.0 / SPAN) for span in spans]
    piece = min(1024, wide)
    total = 0.0
    for at in range(0, wide, piece):
        part = sum(jnp.log(pay_ref[k, :, at : at + piece].astype(f32)) * factors[k] for k in range(count))
        part = (part + offset) * scale
        losses_ref[:, at : at + piece] = part
        total += jnp.sum(part, axis=1, keepdims=True)
    mean = total * (1.0 / wide)
    second = jnp.sum(jnp.square(losses_ref[...] - mean), axis=1, keepdims=True)
    lane = lax.broadcasted_iota(jnp.int32, both_ref.shape[1:], 1)
    both = jnp.where(lane == 0, mean, jnp.where(lane == 1, second, 0.0))
    for k in range(both_ref.shape[0]):
        both_ref[k] = both


def tail_kernel(tail_scale, scenarios, losses_ref, both_ref, pay_ref):
    groups = both_ref.shape[0]
    wide = losses_ref.shape[1]
    means = [both_ref[k, :, 0:1] for k in range(groups)]
    center = sum(means) * (1.0 / groups)
    spread = sum(both_ref[k, :, 1:2] for k in range(groups)) * (1.0 / scenarios)
    spread += sum(jnp.square(each - center) for each in means) * (1.0 / groups)
    deviation = jnp.sqrt(spread + EPSILON)
    thresh = center + QUANTILE * deviation
    width = SMOOTH * deviation
    narrow = 1.0 / width
    piece = min(1024, wide)
    soft = 0.0
    for at in range(0, wide, piece):
        scaled = (losses_ref[:, at : at + piece] - thresh) * narrow
        small = jnp.exp(-jnp.abs(scaled))
        grown = 1.0 + small
        half = 0.5 * tail_scale
        weight = (jnp.where(scaled >= 0.0, half, half * small) / grown).astype(bf16)
        soft += jnp.sum(jnp.maximum(scaled, 0.0) + jnp.log(grown), axis=1, keepdims=True)
        for k in range(pay_ref.shape[0]):
            pay_ref[k, :, at : at + piece] = weight
    lane = lax.broadcasted_iota(jnp.int32, (pay_ref.shape[1], 128), 1)
    edge = jnp.zeros(lane.shape, f32)
    for at, part in enumerate(split3(soft) + split3(thresh) + split3(width)):
        edge = jnp.where(lane == at, part, edge)
    for k in range(pay_ref.shape[0]):
        pay_ref[k, :, wide:] = edge.astype(bf16)


def heads_kernel(edge_ref, soft_ref, stat_ref):
    rows = jnp.transpose(edge_ref[...].reshape(-1, 128).astype(f32))
    soft_ref[...] = jnp.broadcast_to(join3(rows, 0), soft_ref.shape)
    stat_ref[...] = jnp.zeros_like(stat_ref)
    stat_ref[0:1] = join3(rows, 3)
    stat_ref[1:2] = join3(rows, 6)


def gradient_kernel(own, p_ref, weight_ref, out_ref):
    rows = out_ref.shape[0]
    core = lax.axis_index("c")
    half = core if own else 1 - core
    at = (half * pl.num_programs(0) + pl.program_id(0)) * rows
    weight = weight_ref[:, :, 0 : p_ref.shape[1]].reshape(out_ref.shape[1], -1)
    out_ref[...] = lax.dot_general(
        p_ref[pl.ds(pl.multiple_of(at, rows), rows)],
        weight,
        (((1,), (1,)), ((), ())),
        preferred_element_type=f32,
    )


def pair_kernel(own_ref, other_ref, soft_ref, soft_other_ref, *pay_refs):
    count = len(pay_refs)
    rows = pay_refs[0].shape[0] - HEAD
    soft = soft_ref[0:1] + soft_other_ref[0:1]
    for k, pay_ref in enumerate(pay_refs):
        at = pl.multiple_of(lax.rem(lax.axis_index("x") + k, count) * rows, rows)
        code, head = encode(own_ref[pl.ds(at, rows)] + other_ref[pl.ds(at, rows)], [soft])
        pay_ref[0:rows] = code
        pay_ref[rows : rows + HEAD] = head


def whole_kernel(tail_scale, stat_ref, *refs):
    pay_refs, out_ref, short_ref = refs[:-2], refs[-2], refs[-1]
    rows = out_ref.shape[0] - HEAD
    total = jnp.zeros((rows, out_ref.shape[1]), f32)
    soft = jnp.zeros((1, out_ref.shape[1]), f32)
    for pay_ref in pay_refs:
        head = pay_ref[rows : rows + HEAD].astype(f32)
        total += decode(pay_ref[0:rows], head)
        soft += join3(head, 2)
    code, head = encode(total, [])
    out_ref[0:rows] = code
    out_ref[rows : rows + HEAD] = head
    short_ref[...] = jnp.broadcast_to(stat_ref[0:1] + stat_ref[1:2] * (soft * tail_scale), short_ref.shape)


def update_kernel(count, last, *refs):
    own_refs, other_refs = refs[:count], refs[count : 2 * count]
    prev_ref, lge_ref, unnorm_ref = refs[2 * count : 2 * count + 3]
    rows = own_refs[0].shape[0] - HEAD
    core = lax.axis_index("c")
    total = jnp.zeros((1, prev_ref.shape[1]), f32)
    reach = jnp.zeros((1, prev_ref.shape[1]), f32)
    for half, pay_refs in ((core, own_refs), (1 - core, other_refs)):
        for k, pay_ref in enumerate(pay_refs):
            at = (half * count + lax.rem(lax.axis_index("x") + (count - k), count)) * rows
            here = pl.ds(pl.multiple_of(at, rows), rows)
            gradient = decode(pay_ref[0:rows], pay_ref[rows : rows + HEAD].astype(f32))
            lge = lge_ref[here]
            unnorm = prev_ref[here] * jnp.exp(lge * (-STEP_RATE * gradient))
            unnorm_ref[here] = unnorm
            total += jnp.sum(unnorm, axis=0, keepdims=True)
            if not last:
                expo = (unnorm * lge).astype(bf16).astype(f32)
                refs[-2][:, here] = jnp.transpose(expo).astype(bf16)
                reach += jnp.sum(expo, axis=0, keepdims=True)
    if last:
        refs[-1][...] = jnp.broadcast_to(total[None], refs[-1].shape)
    else:
        refs[-1][...] = edge_of(total, reach)


def scale_kernel(obligors, unnorm_ref, totals_ref, out_ref):
    rows = out_ref.shape[0]
    here = pl.ds(pl.multiple_of(pl.program_id(0) * rows, rows), rows)
    total = sum(totals_ref[k] for k in range(totals_ref.shape[0]))
    out_ref[...] = unnorm_ref[here] * (obligors / total)


VMEM = pl.BlockSpec(memory_space=pltpu.VMEM)


def near(array):
    return array if INTERPRET else pltpu.with_memory_space_constraint(array, pltpu.VMEM)


def far(array):
    return array if INTERPRET else pltpu.with_memory_space_constraint(array, pltpu.HBM)


def near_shape(shape, dtype):
    return jax.ShapeDtypeStruct(shape, dtype) if INTERPRET else pltpu.VMEM(shape, dtype)


def whole(shape):
    return pl.BlockSpec(shape, lambda *_: (0,) * len(shape))


def groups_of(side, n_x):
    span = range(side)
    plane = lambda y, z, c: (y * side + z) * 2 + c
    along_y = lambda c: [[plane(y, z, c) for y in span] for z in span]
    along_z = lambda c: [[plane(y, z, c) for z in span] for y in span]
    place = lambda y, z, x, c: ((y * side + z) * n_x + x) * 2 + c
    same = [
        [place(a, b, x, 0) for x in range(n_x)] + [place(b, a, x, 1) for x in range(n_x)] for a in span for b in span
    ]
    return along_y(0) + along_z(1), along_z(0) + along_y(1), same


def rounded(value):
    return lax.reduce_precision(value, 8, 7)


def on_device(factors, idiosyncratic, loadings, rating, barrier, loss_given, sector, allowed, holdings):
    sds = jax.ShapeDtypeStruct
    n_obl, n_x, n_c = lax.axis_size(OBL), lax.axis_size("x"), lax.axis_size("c")
    side = lax.axis_size("y")
    first, second, same = groups_of(side, n_x)
    obl_dev, scn_dev = idiosyncratic.shape
    mandates = holdings.shape[1]
    obligors = obl_dev * n_obl
    scenarios = scn_dev * n_x * n_c
    tail_scale = 1.0 / ((1.0 - LEVEL) * scenarios)
    ro = obl_dev // (n_x * n_c)
    po = ro + HEAD
    mr = mandates // n_obl
    half = obl_dev // n_c
    row8 = sds((8, mandates), f32)
    ratings = barrier.shape[0]
    bar_a = rounded(barrier)
    bar_b = rounded(barrier - bar_a)
    bar_c = barrier - bar_a - bar_b
    bars = -jnp.concatenate([bar_a, bar_b, bar_c])
    bars = jnp.pad(bars, (0, 128 - 3 * ratings)).astype(bf16)[None, :]
    fdim = factors.shape[1]

    sb = min(512, obl_dev)
    line = pl.BlockSpec((1, sb), lambda i: (0, i))
    prev, lge, aug, expot, edge = call(
        setup_kernel,
        (obl_dev // sb,),
        [
            pl.BlockSpec((sb, mandates), lambda i: (i, 0)),
            line,
            line,
            line,
            whole(allowed.shape[::-1]),
            pl.BlockSpec((sb, fdim), lambda i: (i, 0)),
        ],
        [VMEM] * 5,
        [
            near_shape((obl_dev, mandates), f32),
            near_shape((obl_dev, mandates), f32),
            near_shape((obl_dev, fdim + 128), bf16),
            near_shape((mandates, obl_dev), bf16),
            near_shape((mandates, 128), bf16),
        ],
        scratch=[pltpu.VMEM((8, mandates), f32)],
        nbytes=obl_dev * mandates * 12,
        name="setup",
    )(far(holdings), far(loss_given[None, :]), far(sector[None, :]), far(rating[None, :]), allowed.T, far(loadings))
    lge = near(lge)

    results = []
    prob = None
    for iteration in range(STEPS):
        pay_shape = sds((n_obl, mr, scn_dev + 128), bf16)
        wide = min(512, scn_dev)
        if iteration == 0:
            prob, pay = call(
                first_losses_kernel,
                (scn_dev // wide,),
                [
                    VMEM,
                    pl.BlockSpec((wide, fdim), lambda i: (i, 0)),
                    whole((1, 128)),
                    pl.BlockSpec((obl_dev, wide), lambda i: (0, i)),
                    VMEM,
                    VMEM,
                ],
                [VMEM, VMEM],
                [near_shape((obl_dev, scn_dev), bf16), pay_shape],
                flops=4 * obl_dev * scn_dev * mandates,
                nbytes=obl_dev * scn_dev * 4,
                name="first_losses",
            )(near(aug), factors, bars, idiosyncratic, near(expot), near(edge))
            prob = near(prob)
        else:
            pay = call(
                functools.partial(losses_kernel, wide),
                (scn_dev // wide,),
                [VMEM, VMEM, VMEM],
                VMEM,
                pay_shape,
                flops=2 * obl_dev * scn_dev * mandates,
                nbytes=obl_dev * scn_dev * 2,
                name="losses",
            )(prob, near(expot), near(edge))
        pay = lax.all_to_all(pay, PLANE, 0, 0, axis_index_groups=first, tiled=True)
        few = sds((side, mr, scn_dev + 128), bf16)
        pay = call(
            mid_kernel,
            (1,),
            [VMEM],
            VMEM,
            few,
            scratch=[pltpu.VMEM((side, mr, scn_dev), f32)],
            nbytes=mandates * scn_dev * 2,
            name="mid",
        )(pay)
        pay = lax.all_to_all(pay, PLANE, 0, 0, axis_index_groups=second, tiled=True)
        n_scn = n_x * n_c
        losses, both = call(
            sum_kernel,
            (1,),
            [VMEM],
            [VMEM, VMEM],
            [near_shape((mr, scn_dev), f32), sds((n_scn, mr, 128), f32)],
            nbytes=mandates * scn_dev * 2,
            name="sum",
        )(pay)
        both = lax.all_to_all(both, OBL + SCN, 0, 0, axis_index_groups=same, tiled=True)
        weight = call(
            functools.partial(tail_kernel, tail_scale, scenarios),
            (1,),
            [VMEM, VMEM],
            VMEM,
            few,
            nbytes=mandates * scn_dev * 2,
            name="tail",
        )(near(losses), both)
        weight = lax.all_to_all(weight, PLANE, 0, 0, axis_index_groups=second, tiled=True)
        weight = jnp.broadcast_to(weight[None], (side, *weight.shape)).reshape(pay_shape.shape)
        weight = lax.all_to_all(weight, PLANE, 0, 0, axis_index_groups=first, tiled=True)
        soft, stat = call(
            heads_kernel,
            (1,),
            [pl.BlockSpec((n_obl, mr, 128), lambda i: (0, 0, scn_dev // 128))],
            [whole((8, mandates)), whole((8, mandates))],
            [row8, row8],
            name="heads",
        )(weight)
        gblock = min(512, half)

        def gradient_of(own):
            return call(
                functools.partial(gradient_kernel, own),
                (half // gblock,),
                [VMEM, VMEM],
                pl.BlockSpec((gblock, mandates), lambda i: (i, 0)),
                sds((half, mandates), f32),
                flops=2 * half * scn_dev * mandates,
                nbytes=half * scn_dev * 2,
                name="gradient",
            )(prob, weight)

        swap = [(0, 1), (1, 0)]
        sent = lax.ppermute(gradient_of(False), "c", swap)
        soft_other = lax.ppermute(soft, "c", swap)
        kept = gradient_of(True)
        gshape = sds((po, mandates), bf16)
        hops = {k: [(i, (i + k) % n_x) for i in range(n_x)] for k in range(1, n_x)}
        order = sorted(hops, key=lambda k: -min(k, n_x - k))
        slots = call(
            pair_kernel,
            (1,),
            [VMEM, VMEM, whole((8, mandates)), whole((8, mandates))],
            [VMEM] * n_x,
            [gshape] * n_x,
            nbytes=half * mandates * 10,
            name="pair",
        )(kept, sent, soft, soft_other)
        slots = list(slots)
        for k in order:
            slots[k] = lax.ppermute(slots[k], "x", hops[k])
        pay, short = call(
            functools.partial(whole_kernel, tail_scale),
            (1,),
            [whole((8, mandates))] + [VMEM] * n_x,
            [VMEM, whole((8, mandates))],
            [gshape, row8],
            nbytes=half * mandates * 4,
            name="whole",
        )(stat, *slots)
        results.append(short[0])
        slots = [pay] * n_x
        for k in order:
            slots[k] = lax.ppermute(pay, "x", hops[k])
        others = [lax.ppermute(slot, "c", swap) for slot in slots]
        last = iteration == STEPS - 1
        outs = call(
            functools.partial(update_kernel, n_x, last),
            (1,),
            [VMEM] * (2 * n_x + 2),
            [VMEM] + [VMEM] * (not last) + [VMEM],
            [near_shape((obl_dev, mandates), f32)]
            + [near_shape((mandates, obl_dev), bf16)] * (not last)
            + [sds((n_obl, 1, mandates), f32) if last else near_shape((mandates, 128), bf16)],
            nbytes=obl_dev * mandates * 14,
            name="update",
        )(*slots, *others, near(prev), lge)
        prev, expot, edge = outs[0], outs[-2], outs[-1]

    totals = lax.all_to_all(edge, OBL, 0, 0, tiled=True)
    positions = call(
        functools.partial(scale_kernel, obligors),
        (max(1, obl_dev // 512),),
        [VMEM, whole((n_obl, 1, mandates))],
        pl.BlockSpec((min(512, obl_dev), mandates), lambda i: (i, 0)),
        sds((obl_dev, mandates), f32),
        nbytes=obl_dev * mandates * 8,
        name="scale",
    )(near(prev), totals)
    return (positions, jnp.stack(results))


def solution(mesh):
    n_obl, n_scn = mesh.shape["obl"], mesh.shape["scn"]
    side = 1
    while side * side < n_obl:
        side *= 2
    fine = Mesh(mesh.devices.reshape(side, n_obl // side, n_scn // 2, 2), ("y", "z", "x", "c"))
    in_specs = (P(SCN, None), P(OBL, SCN), P(OBL, None), P(OBL), P(), P(OBL), P(OBL), P(), P(OBL, None))
    return jax.shard_map(on_device, mesh=fine, in_specs=in_specs, out_specs=(P(OBL, None), P()), check_vma=False)
```

```python
import functools

import jax
import jax.numpy as jnp
from jax import lax
from jax.experimental import pallas as pl
from jax.experimental.pallas import tpu as pltpu
from jax.sharding import Mesh
from jax.sharding import PartitionSpec as P

STEPS = 2
OBL = ("y", "z")
SCN = ("x", "c")
PLANE = ("y", "z", "c")
IDIO_SCALE = 0.8
LEVEL = 0.99
QUANTILE = 2.326
SMOOTH = 0.5
EPSILON = 1e-06
STEP_RATE = 8.0
HEAD = 8
SPAN = 127.0
INTERPRET = False

f32 = jnp.float32
bf16 = jnp.bfloat16


def call(kernel, grid, in_specs, out_specs, out_shape, scratch=(), prefetch=0, flops=0, nbytes=0, name=None):
    spec = pltpu.PrefetchScalarGridSpec(
        num_scalar_prefetch=prefetch, grid=grid, in_specs=in_specs, out_specs=out_specs, scratch_shapes=list(scratch)
    )
    return pl.pallas_call(
        kernel,
        grid_spec=spec,
        out_shape=out_shape,
        compiler_params=pltpu.CompilerParams(vmem_limit_bytes=24 * 1024 * 1024),
        cost_estimate=pl.CostEstimate(flops=int(flops), bytes_accessed=int(nbytes), transcendentals=0),
        interpret=INTERPRET,
        name=name,
    )


def split3(value):
    a = value.astype(bf16)
    rest = value - a.astype(f32)
    b = rest.astype(bf16)
    c = (rest - b.astype(f32)).astype(bf16)
    return [a.astype(f32), b.astype(f32), c.astype(f32)]


def join3(head, at):
    return head[at : at + 1] + head[at + 1 : at + 2] + head[at + 2 : at + 3]


def encode(values, extra):
    low = jnp.min(values, axis=0, keepdims=True)
    high = jnp.max(values, axis=0, keepdims=True)
    span = jnp.maximum(jnp.maximum(high - low, jnp.abs(low) * (1.0 / 64.0)), 1e-30)
    base = low.astype(bf16).astype(f32)
    span = (span * 1.02).astype(bf16).astype(f32)
    code = jnp.exp((values - base) * (SPAN / span) - 0.5 * SPAN).astype(bf16)
    rows = [base, span]
    for row in extra:
        rows += split3(row)
    if len(rows) < HEAD:
        rows.append(jnp.zeros((HEAD - len(rows), values.shape[1]), f32))
    return code, jnp.concatenate(rows, axis=0).astype(bf16)


def decode(code, head):
    base, span = head[0:1], head[1:2]
    return (base + 0.5 * span) + jnp.log(code.astype(f32)) * (span * (1.0 / SPAN))


def edge_of(total, reach):
    span = jnp.maximum(2.02 * reach, 1e-30).astype(bf16).astype(f32)
    rows = [span] + split3(total)
    rows.append(jnp.zeros((128 - len(rows), total.shape[1]), f32))
    return jnp.transpose(jnp.concatenate(rows, axis=0)).astype(bf16)


def spot():
    y, z, core = lax.axis_index("y"), lax.axis_index("z"), lax.axis_index("c")
    return jnp.where(core == 0, y, z), jnp.where(core == 0, z, y)


def put_rotated(ref, cols, value, side):
    rows = value.shape[0] // side
    for block in range(side):
        at = pl.multiple_of(lax.rem(block + side - spot()[0], side) * rows, rows)
        ref[pl.ds(at, rows), cols] = value[block * rows : (block + 1) * rows]


def put_codes(doubled, edge_ref, pay_refs, at):
    parts, rows, wide = pay_refs[0].shape
    span = edge_ref[:, 0:1].astype(f32)
    code = jnp.exp(doubled * (SPAN / span) - 0.5 * SPAN).astype(bf16)
    for k, pay_ref in enumerate(pay_refs):
        part = slice(k * parts * rows, (k + 1) * parts * rows)
        pay_ref[:, :, at] = code[part].reshape(parts, rows, -1)

    @pl.when(pl.program_id(0) == 0)
    def _():
        for k, pay_ref in enumerate(pay_refs):
            part = slice(k * parts * rows, (k + 1) * parts * rows)
            pay_ref[:, :, wide - 128 :] = edge_ref[part].reshape(parts, rows, 128)


def setup_kernel(side, hold_ref, lgd_ref, sector_ref, rating_ref, allowed_ref, load_ref, weighted_ref, lge_ref, aug_ref, expot_ref, edge_ref, sums_ref):
    rows = sector_ref.shape[1]
    sectors = allowed_ref.shape[0]
    here = pl.ds(pl.multiple_of(pl.program_id(0) * rows, rows), rows)
    allowed = allowed_ref[...].astype(f32)
    hot = (lax.broadcasted_iota(jnp.int32, (sectors, rows), 0) == sector_ref[...]).astype(f32)
    lgd = lgd_ref[...]
    parts = jnp.concatenate([hot * part for part in split3(lgd)], axis=0)
    dims = (((0,), (0,)), ((), ()))
    elig = lax.dot_general(hot.astype(bf16), allowed.astype(bf16), dims, preferred_element_type=f32)
    thrice = jnp.concatenate([allowed] * 3, axis=0)
    lge = lax.dot_general(parts.astype(bf16), thrice.astype(bf16), dims, preferred_element_type=f32)
    hold = hold_ref[...]
    weighted = elig * hold
    weighted_ref[here] = weighted
    lge_ref[here] = lge
    expo = (lge * hold).astype(bf16).astype(f32)
    put_rotated(expot_ref, here, jnp.transpose(expo).astype(bf16), side)
    lane = lax.broadcasted_iota(jnp.int32, (128, rows), 0)
    rated = ((lane % 16 == rating_ref[...]) & (lane < 48)).astype(f32)
    aug_ref[here] = jnp.concatenate([load_ref[...], jnp.transpose(rated).astype(bf16)], axis=1)

    @pl.when(pl.program_id(0) == 0)
    def _():
        sums_ref[...] = jnp.zeros_like(sums_ref)

    sums_ref[0:1] += jnp.sum(weighted, axis=0, keepdims=True)
    sums_ref[1:2] += jnp.sum(expo, axis=0, keepdims=True)

    @pl.when(pl.program_id(0) == pl.num_programs(0) - 1)
    def _():
        put_rotated(edge_ref, slice(None), edge_of(sums_ref[0:1], sums_ref[1:2]), side)


def first_losses_kernel(load_ref, fac_ref, bar_ref, idio_ref, expot_ref, edge_ref, p_ref, *pay_refs):
    wide = fac_ref.shape[0]
    cols = pl.ds(pl.multiple_of(pl.program_id(0) * wide, wide), wide)
    block = min(256, load_ref.shape[0])
    fac = jnp.concatenate([fac_ref[...], jnp.broadcast_to(bar_ref[...], (wide, 128))], axis=1)
    for i in range(load_ref.shape[0] // block):
        sl = slice(i * block, (i + 1) * block)
        latent = lax.dot_general(load_ref[sl], fac, (((1,), (1,)), ((), ())), preferred_element_type=f32)
        p_ref[sl, cols] = (jnp.tanh(latent + IDIO_SCALE * idio_ref[sl].astype(f32)) + 1.0).astype(bf16)
    put_codes(jnp.dot(expot_ref[...], p_ref[:, cols], preferred_element_type=f32), edge_ref, pay_refs, cols)


def losses_kernel(wide, p_ref, expot_ref, edge_ref, *pay_refs):
    cols = pl.ds(pl.multiple_of(pl.program_id(0) * wide, wide), wide)
    put_codes(jnp.dot(expot_ref[...], p_ref[:, cols], preferred_element_type=f32), edge_ref, pay_refs, cols)


def mid_kernel(*refs):
    part_ref = refs[-1]
    count = len(refs) // 2
    pay_refs, out_refs = refs[:count], refs[count:-1]
    wide = part_ref.shape[1]
    piece = min(1024, wide)
    lane = lax.broadcasted_iota(jnp.int32, (part_ref.shape[0], 128), 1)
    for k, out_ref in enumerate(out_refs):
        row = lax.rem(spot()[1] + k, count)
        edges = [pay_ref[row, :, wide:].astype(f32) for pay_ref in pay_refs]
        spans = [edge[:, 0:1] for edge in edges]
        offset = 0.5 * sum(spans)
        factors = [span * (1.0 / SPAN) for span in spans]
        low, high = jnp.inf, -jnp.inf
        for at in range(0, wide, piece):
            codes = [pay_ref[row, :, at : at + piece].astype(f32) for pay_ref in pay_refs]
            part = sum(jnp.log(code) * factor for code, factor in zip(codes, factors)) + offset
            part_ref[:, at : at + piece] = part
            low = jnp.minimum(low, jnp.min(part, axis=1, keepdims=True))
            high = jnp.maximum(high, jnp.max(part, axis=1, keepdims=True))
        span = jnp.maximum(jnp.maximum(high - low, jnp.abs(low) * (1.0 / 64.0)), 1e-30)
        base = low.astype(bf16).astype(f32)
        span = (span * 1.02).astype(bf16).astype(f32)
        for at in range(0, wide, piece):
            part = part_ref[:, at : at + piece]
            out_ref[:, at : at + piece] = jnp.exp((part - base) * (SPAN / span) - 0.5 * SPAN).astype(bf16)
        total = sum(edge[:, 1:2] + edge[:, 2:3] + edge[:, 3:4] for edge in edges)
        edge = jnp.zeros(lane.shape, f32)
        for at, value in enumerate([base, span] + split3(total)):
            edge = jnp.where(lane == at, value, edge)
        out_ref[:, wide:] = edge.astype(bf16)


def sum_kernel(*refs):
    pay_refs, losses_ref, both_ref = refs[:-2], refs[-2], refs[-1]
    wide = losses_ref.shape[1]
    edges = [pay_ref[:, wide:].astype(f32) for pay_ref in pay_refs]
    spans = [edge[:, 1:2] for edge in edges]
    offset = sum(edge[:, 0:1] for edge in edges) + 0.5 * sum(spans)
    scale = 0.5 / sum(edge[:, 2:3] + edge[:, 3:4] + edge[:, 4:5] for edge in edges)
    factors = [span * (1.0 / SPAN) for span in spans]
    piece = min(1024, wide)
    total = 0.0
    for at in range(0, wide, piece):
        codes = [pay_ref[:, at : at + piece].astype(f32) for pay_ref in pay_refs]
        part = sum(jnp.log(code) * factor for code, factor in zip(codes, factors))
        part = (part + offset) * scale
        losses_ref[:, at : at + piece] = part
        total += jnp.sum(part, axis=1, keepdims=True)
    mean = total * (1.0 / wide)
    second = jnp.sum(jnp.square(losses_ref[...] - mean), axis=1, keepdims=True)
    lane = lax.broadcasted_iota(jnp.int32, both_ref.shape[1:], 1)
    both = jnp.where(lane == 0, mean, jnp.where(lane == 1, second, 0.0))
    for k in range(both_ref.shape[0]):
        both_ref[k] = both


def tail_kernel(tail_scale, scenarios, losses_ref, both_ref, pay_ref):
    groups = both_ref.shape[0]
    wide = losses_ref.shape[1]
    means = [both_ref[k, :, 0:1] for k in range(groups)]
    center = sum(means) * (1.0 / groups)
    spread = sum(both_ref[k, :, 1:2] for k in range(groups)) * (1.0 / scenarios)
    spread += sum(jnp.square(each - center) for each in means) * (1.0 / groups)
    deviation = jnp.sqrt(spread + EPSILON)
    thresh = center + QUANTILE * deviation
    width = SMOOTH * deviation
    narrow = 1.0 / width
    piece = min(1024, wide)
    soft = 0.0
    for at in range(0, wide, piece):
        scaled = (losses_ref[:, at : at + piece] - thresh) * narrow
        small = jnp.exp(-jnp.abs(scaled))
        grown = 1.0 + small
        half = 0.5 * tail_scale
        weight = (jnp.where(scaled >= 0.0, half, half * small) / grown).astype(bf16)
        soft += jnp.sum(jnp.maximum(scaled, 0.0) + jnp.log(grown), axis=1, keepdims=True)
        pay_ref[:, at : at + piece] = weight
    lane = lax.broadcasted_iota(jnp.int32, (pay_ref.shape[0], 128), 1)
    edge = jnp.zeros(lane.shape, f32)
    for at, part in enumerate(split3(soft) + split3(thresh) + split3(width)):
        edge = jnp.where(lane == at, part, edge)
    pay_ref[:, wide:] = edge.astype(bf16)


def join_kernel(*refs):
    count = len(refs) - 1
    for k in range(count):
        refs[-1][lax.rem(spot()[1] + (count - k), count)] = refs[k][...]


def spread_kernel(*refs):
    pay_refs, (weight_ref, soft_ref, stat_ref, head_ref) = refs[:-4], refs[-4:]
    count = len(pay_refs)
    wide = weight_ref.shape[1]
    rows = weight_ref.shape[0] // count
    for k, pay_ref in enumerate(pay_refs):
        at = pl.multiple_of(lax.rem(spot()[0] + (count - k), count) * rows, rows)
        weight_ref[pl.ds(at, rows)] = pay_ref[:, :, 0:wide].reshape(rows, wide)
        head_ref[pl.ds(at, rows)] = pay_ref[:, :, wide:].reshape(rows, 128).astype(f32)
    heads = jnp.transpose(head_ref[...])
    soft_ref[...] = jnp.broadcast_to(join3(heads, 0), soft_ref.shape)
    stat_ref[...] = jnp.zeros_like(stat_ref)
    stat_ref[0:1] = join3(heads, 3)
    stat_ref[1:2] = join3(heads, 6)


def gradient_kernel(own, p_ref, weight_ref, out_ref):
    rows = out_ref.shape[0]
    core = lax.axis_index("c")
    half = core if own else 1 - core
    at = (half * pl.num_programs(0) + pl.program_id(0)) * rows
    out_ref[...] = lax.dot_general(
        p_ref[pl.ds(pl.multiple_of(at, rows), rows)],
        weight_ref[...],
        (((1,), (1,)), ((), ())),
        preferred_element_type=f32,
    )


def pair_kernel(own_ref, other_ref, soft_ref, soft_other_ref, *pay_refs):
    count = len(pay_refs)
    rows = pay_refs[0].shape[0] - HEAD
    soft = soft_ref[0:1] + soft_other_ref[0:1]
    for k, pay_ref in enumerate(pay_refs):
        at = pl.multiple_of(lax.rem(lax.axis_index("x") + k, count) * rows, rows)
        code, head = encode(own_ref[pl.ds(at, rows)] + other_ref[pl.ds(at, rows)], [soft])
        pay_ref[0:rows] = code
        pay_ref[rows : rows + HEAD] = head


def whole_kernel(tail_scale, stat_ref, *refs):
    pay_refs, out_ref, short_ref = refs[:-2], refs[-2], refs[-1]
    rows = out_ref.shape[0] - HEAD
    total = jnp.zeros((rows, out_ref.shape[1]), f32)
    soft = jnp.zeros((1, out_ref.shape[1]), f32)
    for pay_ref in pay_refs:
        head = pay_ref[rows : rows + HEAD].astype(f32)
        total += decode(pay_ref[0:rows], head)
        soft += join3(head, 2)
    code, head = encode(total, [])
    out_ref[0:rows] = code
    out_ref[rows : rows + HEAD] = head
    short_ref[...] = jnp.broadcast_to(stat_ref[0:1] + stat_ref[1:2] * (soft * tail_scale), short_ref.shape)


def update_kernel(count, last, side, *refs):
    own_refs, other_refs = refs[:count], refs[count : 2 * count]
    prev_ref, lge_ref, unnorm_ref = refs[2 * count : 2 * count + 3]
    rows = own_refs[0].shape[0] - HEAD
    core = lax.axis_index("c")
    total = jnp.zeros((1, prev_ref.shape[1]), f32)
    reach = jnp.zeros((1, prev_ref.shape[1]), f32)
    for half, pay_refs in ((core, own_refs), (1 - core, other_refs)):
        for k, pay_ref in enumerate(pay_refs):
            at = (half * count + lax.rem(lax.axis_index("x") + (count - k), count)) * rows
            here = pl.ds(pl.multiple_of(at, rows), rows)
            gradient = decode(pay_ref[0:rows], pay_ref[rows : rows + HEAD].astype(f32))
            lge = lge_ref[here]
            unnorm = prev_ref[here] * jnp.exp(lge * (-STEP_RATE * gradient))
            unnorm_ref[here] = unnorm
            total += jnp.sum(unnorm, axis=0, keepdims=True)
            if not last:
                expo = (unnorm * lge).astype(bf16).astype(f32)
                put_rotated(refs[-2], here, jnp.transpose(expo).astype(bf16), side)
                reach += jnp.sum(expo, axis=0, keepdims=True)
    if last:
        refs[-1][...] = jnp.broadcast_to(total[None], refs[-1].shape)
    else:
        put_rotated(refs[-1], slice(None), edge_of(total, reach), side)


def scale_kernel(obligors, unnorm_ref, totals_ref, out_ref):
    rows = out_ref.shape[0]
    here = pl.ds(pl.multiple_of(pl.program_id(0) * rows, rows), rows)
    total = sum(totals_ref[k] for k in range(totals_ref.shape[0]))
    out_ref[...] = unnorm_ref[here] * (obligors / total)


VMEM = pl.BlockSpec(memory_space=pltpu.VMEM)


def near(array):
    return array if INTERPRET else pltpu.with_memory_space_constraint(array, pltpu.VMEM)


def far(array):
    return array if INTERPRET else pltpu.with_memory_space_constraint(array, pltpu.HBM)


def near_shape(shape, dtype):
    return jax.ShapeDtypeStruct(shape, dtype) if INTERPRET else pltpu.VMEM(shape, dtype)


def whole(shape):
    return pl.BlockSpec(shape, lambda *_: (0,) * len(shape))


def groups_of(side, n_x):
    span = range(side)
    plane = lambda y, z, c: (y * side + z) * 2 + c
    along_y = lambda c: [[plane(y, z, c) for y in span] for z in span]
    along_z = lambda c: [[plane(y, z, c) for z in span] for y in span]
    place = lambda y, z, x, c: ((y * side + z) * n_x + x) * 2 + c
    same = [
        [place(a, b, x, 0) for x in range(n_x)] + [place(b, a, x, 1) for x in range(n_x)] for a in span for b in span
    ]
    return along_y(0) + along_z(1), along_z(0) + along_y(1), same


def exchanged(slots, groups):
    count = len(slots)
    out = list(slots)
    for k in sorted(range(1, count), key=lambda k: -min(k, count - k)):
        out[k] = lax.ppermute(
            slots[k], PLANE, [(group[i], group[(i + k) % count]) for group in groups for i in range(count)]
        )
    return out


def rounded(value):
    return lax.reduce_precision(value, 8, 7)


def on_device(factors, idiosyncratic, loadings, rating, barrier, loss_given, sector, allowed, holdings):
    sds = jax.ShapeDtypeStruct
    n_obl, n_x, n_c = lax.axis_size(OBL), lax.axis_size("x"), lax.axis_size("c")
    side = lax.axis_size("y")
    first, second, same = groups_of(side, n_x)
    obl_dev, scn_dev = idiosyncratic.shape
    mandates = holdings.shape[1]
    obligors = obl_dev * n_obl
    scenarios = scn_dev * n_x * n_c
    tail_scale = 1.0 / ((1.0 - LEVEL) * scenarios)
    ro = obl_dev // (n_x * n_c)
    po = ro + HEAD
    mr = mandates // n_obl
    half = obl_dev // n_c
    row8 = sds((8, mandates), f32)
    ratings = barrier.shape[0]
    bar_a = rounded(barrier)
    bar_b = rounded(barrier - bar_a)
    bar_c = barrier - bar_a - bar_b
    bars = -jnp.concatenate([bar_a, bar_b, bar_c])
    bars = jnp.pad(bars, (0, 128 - 3 * ratings)).astype(bf16)[None, :]
    fdim = factors.shape[1]

    sb = min(512, obl_dev)
    line = pl.BlockSpec((1, sb), lambda i: (0, i))
    prev, lge, aug, expot, edge = call(
        functools.partial(setup_kernel, side),
        (obl_dev // sb,),
        [
            pl.BlockSpec((sb, mandates), lambda i: (i, 0)),
            line,
            line,
            line,
            whole(allowed.shape[::-1]),
            pl.BlockSpec((sb, fdim), lambda i: (i, 0)),
        ],
        [VMEM] * 5,
        [
            near_shape((obl_dev, mandates), f32),
            near_shape((obl_dev, mandates), f32),
            near_shape((obl_dev, fdim + 128), bf16),
            near_shape((mandates, obl_dev), bf16),
            near_shape((mandates, 128), bf16),
        ],
        scratch=[pltpu.VMEM((8, mandates), f32)],
        nbytes=obl_dev * mandates * 12,
        name="setup",
    )(far(holdings), far(loss_given[None, :]), far(sector[None, :]), far(rating[None, :]), allowed.T, far(loadings))
    lge = near(lge)

    results = []
    prob = None
    for iteration in range(STEPS):
        quarter = sds((side, mr, scn_dev + 128), bf16)
        few = sds((mr, scn_dev + 128), bf16)
        wide = min(512, scn_dev)
        if iteration == 0:
            prob, *pays = call(
                first_losses_kernel,
                (scn_dev // wide,),
                [
                    VMEM,
                    pl.BlockSpec((wide, fdim), lambda i: (i, 0)),
                    whole((1, 128)),
                    pl.BlockSpec((obl_dev, wide), lambda i: (0, i)),
                    VMEM,
                    VMEM,
                ],
                [VMEM] * (1 + side),
                [near_shape((obl_dev, scn_dev), bf16)] + [quarter] * side,
                flops=4 * obl_dev * scn_dev * mandates,
                nbytes=obl_dev * scn_dev * 4,
                name="first_losses",
            )(near(aug), factors, bars, idiosyncratic, near(expot), near(edge))
            prob = near(prob)
        else:
            pays = call(
                functools.partial(losses_kernel, wide),
                (scn_dev // wide,),
                [VMEM, VMEM, VMEM],
                [VMEM] * side,
                [quarter] * side,
                flops=2 * obl_dev * scn_dev * mandates,
                nbytes=obl_dev * scn_dev * 2,
                name="losses",
            )(prob, near(expot), near(edge))
        pays = exchanged(pays, first)
        pays = call(
            mid_kernel,
            (1,),
            [VMEM] * side,
            [VMEM] * side,
            [few] * side,
            scratch=[pltpu.VMEM((mr, scn_dev), f32)],
            nbytes=mandates * scn_dev * 2,
            name="mid",
        )(*pays)
        pays = exchanged(pays, second)
        n_scn = n_x * n_c
        losses, both = call(
            sum_kernel,
            (1,),
            [VMEM] * side,
            [VMEM, VMEM],
            [near_shape((mr, scn_dev), f32), sds((n_scn, mr, 128), f32)],
            nbytes=mandates * scn_dev * 2,
            name="sum",
        )(*pays)
        both = lax.all_to_all(both, OBL + SCN, 0, 0, axis_index_groups=same, tiled=True)
        weight = call(
            functools.partial(tail_kernel, tail_scale, scenarios),
            (1,),
            [VMEM, VMEM],
            VMEM,
            few,
            nbytes=mandates * scn_dev * 2,
            name="tail",
        )(near(losses), both)
        weight = call(
            join_kernel,
            (1,),
            [VMEM] * side,
            VMEM,
            quarter,
            nbytes=scn_dev * mandates,
            name="join",
        )(*exchanged([weight] * side, second))
        weight, soft, stat = call(
            spread_kernel,
            (1,),
            [VMEM] * side,
            [VMEM, whole((8, mandates)), whole((8, mandates))],
            [near_shape((mandates, scn_dev), bf16), row8, row8],
            scratch=[pltpu.VMEM((mandates, 128), f32)],
            nbytes=scn_dev * mandates * 4,
            name="spread",
        )(*exchanged([weight] * side, first))
        weight = near(weight)
        gblock = min(512, half)

        def gradient_of(own):
            return call(
                functools.partial(gradient_kernel, own),
                (half // gblock,),
                [VMEM, VMEM],
                pl.BlockSpec((gblock, mandates), lambda i: (i, 0)),
                sds((half, mandates), f32),
                flops=2 * half * scn_dev * mandates,
                nbytes=half * scn_dev * 2,
                name="gradient",
            )(prob, weight)

        swap = [(0, 1), (1, 0)]
        sent = lax.ppermute(gradient_of(False), "c", swap)
        soft_other = lax.ppermute(soft, "c", swap)
        kept = gradient_of(True)
        gshape = sds((po, mandates), bf16)
        hops = {k: [(i, (i + k) % n_x) for i in range(n_x)] for k in range(1, n_x)}
        order = sorted(hops, key=lambda k: -min(k, n_x - k))
        slots = call(
            pair_kernel,
            (1,),
            [VMEM, VMEM, whole((8, mandates)), whole((8, mandates))],
            [VMEM] * n_x,
            [gshape] * n_x,
            nbytes=half * mandates * 10,
            name="pair",
        )(kept, sent, soft, soft_other)
        slots = list(slots)
        for k in order:
            slots[k] = lax.ppermute(slots[k], "x", hops[k])
        pay, short = call(
            functools.partial(whole_kernel, tail_scale),
            (1,),
            [whole((8, mandates))] + [VMEM] * n_x,
            [VMEM, whole((8, mandates))],
            [gshape, row8],
            nbytes=half * mandates * 4,
            name="whole",
        )(stat, *slots)
        results.append(short[0])
        slots = [pay] * n_x
        for k in order:
            slots[k] = lax.ppermute(pay, "x", hops[k])
        others = [lax.ppermute(slot, "c", swap) for slot in slots]
        last = iteration == STEPS - 1
        outs = call(
            functools.partial(update_kernel, n_x, last, side),
            (1,),
            [VMEM] * (2 * n_x + 2),
            [VMEM] + [VMEM] * (not last) + [VMEM],
            [near_shape((obl_dev, mandates), f32)]
            + [near_shape((mandates, obl_dev), bf16)] * (not last)
            + [sds((n_obl, 1, mandates), f32) if last else near_shape((mandates, 128), bf16)],
            nbytes=obl_dev * mandates * 14,
            name="update",
        )(*slots, *others, near(prev), lge)
        prev, expot, edge = outs[0], outs[-2], outs[-1]

    totals = lax.all_to_all(edge, OBL, 0, 0, tiled=True)
    positions = call(
        functools.partial(scale_kernel, obligors),
        (max(1, obl_dev // 512),),
        [VMEM, whole((n_obl, 1, mandates))],
        pl.BlockSpec((min(512, obl_dev), mandates), lambda i: (i, 0)),
        sds((obl_dev, mandates), f32),
        nbytes=obl_dev * mandates * 8,
        name="scale",
    )(near(prev), totals)
    return (positions, jnp.stack(results))


def solution(mesh):
    n_obl, n_scn = mesh.shape["obl"], mesh.shape["scn"]
    side = 1
    while side * side < n_obl:
        side *= 2
    fine = Mesh(mesh.devices.reshape(side, n_obl // side, n_scn // 2, 2), ("y", "z", "x", "c"))
    in_specs = (P(SCN, None), P(OBL, SCN), P(OBL, None), P(OBL), P(), P(OBL), P(OBL), P(), P(OBL, None))
    return jax.shard_map(on_device, mesh=fine, in_specs=in_specs, out_specs=(P(OBL, None), P()), check_vma=False)
```

```python
import functools

import jax
import jax.numpy as jnp
from jax import lax
from jax.experimental import pallas as pl
from jax.experimental.pallas import tpu as pltpu
from jax.sharding import Mesh
from jax.sharding import PartitionSpec as P

STEPS = 2
OBL = ("y", "z")
SCN = ("x", "c")
PLANE = ("y", "z", "c")
IDIO_SCALE = 0.8
LEVEL = 0.99
QUANTILE = 2.326
SMOOTH = 0.5
EPSILON = 1e-06
STEP_RATE = 8.0
HEAD = 8
SPAN = 127.0
INTERPRET = False

f32 = jnp.float32
bf16 = jnp.bfloat16


def call(kernel, grid, in_specs, out_specs, out_shape, scratch=(), prefetch=0, flops=0, nbytes=0, name=None):
    spec = pltpu.PrefetchScalarGridSpec(
        num_scalar_prefetch=prefetch, grid=grid, in_specs=in_specs, out_specs=out_specs, scratch_shapes=list(scratch)
    )
    return pl.pallas_call(
        kernel,
        grid_spec=spec,
        out_shape=out_shape,
        compiler_params=pltpu.CompilerParams(vmem_limit_bytes=24 * 1024 * 1024),
        cost_estimate=pl.CostEstimate(flops=int(flops), bytes_accessed=int(nbytes), transcendentals=0),
        interpret=INTERPRET,
        name=name,
    )


def split3(value):
    a = value.astype(bf16)
    rest = value - a.astype(f32)
    b = rest.astype(bf16)
    c = (rest - b.astype(f32)).astype(bf16)
    return [a.astype(f32), b.astype(f32), c.astype(f32)]


def join3(head, at):
    return head[at : at + 1] + head[at + 1 : at + 2] + head[at + 2 : at + 3]


def encode(values, extra):
    low = jnp.min(values, axis=0, keepdims=True)
    high = jnp.max(values, axis=0, keepdims=True)
    span = jnp.maximum(jnp.maximum(high - low, jnp.abs(low) * (1.0 / 64.0)), 1e-30)
    base = low.astype(bf16).astype(f32)
    span = (span * 1.02).astype(bf16).astype(f32)
    code = jnp.exp((values - base) * (SPAN / span) - 0.5 * SPAN).astype(bf16)
    rows = [base, span]
    for row in extra:
        rows += split3(row)
    if len(rows) < HEAD:
        rows.append(jnp.zeros((HEAD - len(rows), values.shape[1]), f32))
    return code, jnp.concatenate(rows, axis=0).astype(bf16)


def decode(code, head):
    base, span = head[0:1], head[1:2]
    return (base + 0.5 * span) + jnp.log(code.astype(f32)) * (span * (1.0 / SPAN))


def edge_of(total, reach):
    span = jnp.maximum(2.02 * reach, 1e-30).astype(bf16).astype(f32)
    rows = [span] + split3(total)
    rows.append(jnp.zeros((128 - len(rows), total.shape[1]), f32))
    return jnp.transpose(jnp.concatenate(rows, axis=0)).astype(bf16)


def spot():
    y, z, core = lax.axis_index("y"), lax.axis_index("z"), lax.axis_index("c")
    return jnp.where(core == 0, y, z), jnp.where(core == 0, z, y)


def put_rotated(ref, cols, value, side):
    rows = value.shape[0] // side
    for block in range(side):
        at = pl.multiple_of(lax.rem(block + side - spot()[0], side) * rows, rows)
        ref[pl.ds(at, rows), cols] = value[block * rows : (block + 1) * rows]


def put_codes(doubled, edge_ref, pay_refs, at):
    parts, rows, wide = pay_refs[0].shape
    span = edge_ref[:, 0:1].astype(f32)
    code = jnp.exp(doubled * (SPAN / span) - 0.5 * SPAN).astype(bf16)
    for k, pay_ref in enumerate(pay_refs):
        part = slice(k * parts * rows, (k + 1) * parts * rows)
        pay_ref[:, :, at] = code[part].reshape(parts, rows, -1)

    if wide % 256 == 0:
        return

    @pl.when(pl.program_id(0) == 0)
    def _():
        for k, pay_ref in enumerate(pay_refs):
            part = slice(k * parts * rows, (k + 1) * parts * rows)
            pay_ref[:, :, wide - 128 :] = edge_ref[part].reshape(parts, rows, 128)


def setup_kernel(side, hold_ref, lgd_ref, sector_ref, rating_ref, allowed_ref, load_ref, weighted_ref, lge_ref, aug_ref, expot_ref, edge_ref, sums_ref):
    rows = sector_ref.shape[1]
    sectors = allowed_ref.shape[0]
    here = pl.ds(pl.multiple_of(pl.program_id(0) * rows, rows), rows)
    allowed = allowed_ref[...].astype(f32)
    hot = (lax.broadcasted_iota(jnp.int32, (sectors, rows), 0) == sector_ref[...]).astype(f32)
    lgd = lgd_ref[...]
    parts = jnp.concatenate([hot * part for part in split3(lgd)], axis=0)
    dims = (((0,), (0,)), ((), ()))
    elig = lax.dot_general(hot.astype(bf16), allowed.astype(bf16), dims, preferred_element_type=f32)
    thrice = jnp.concatenate([allowed] * 3, axis=0)
    lge = lax.dot_general(parts.astype(bf16), thrice.astype(bf16), dims, preferred_element_type=f32)
    hold = hold_ref[...]
    weighted = elig * hold
    weighted_ref[here] = weighted
    lge_ref[here] = lge
    expo = (lge * hold).astype(bf16).astype(f32)
    put_rotated(expot_ref, here, jnp.transpose(expo).astype(bf16), side)
    lane = lax.broadcasted_iota(jnp.int32, (128, rows), 0)
    rated = ((lane % 16 == rating_ref[...]) & (lane < 48)).astype(f32)
    aug_ref[here] = jnp.concatenate([load_ref[...], jnp.transpose(rated).astype(bf16)], axis=1)

    @pl.when(pl.program_id(0) == 0)
    def _():
        sums_ref[...] = jnp.zeros_like(sums_ref)

    sums_ref[0:1] += jnp.sum(weighted, axis=0, keepdims=True)
    sums_ref[1:2] += jnp.sum(expo, axis=0, keepdims=True)

    @pl.when(pl.program_id(0) == pl.num_programs(0) - 1)
    def _():
        put_rotated(edge_ref, slice(None), edge_of(sums_ref[0:1], sums_ref[1:2]), side)


def first_losses_kernel(load_ref, fac_ref, bar_ref, idio_ref, expot_ref, edge_ref, p_ref, *pay_refs):
    wide = fac_ref.shape[0]
    cols = pl.ds(pl.multiple_of(pl.program_id(0) * wide, wide), wide)
    block = min(256, load_ref.shape[0])
    fac = jnp.concatenate([fac_ref[...], jnp.broadcast_to(bar_ref[...], (wide, 128))], axis=1)
    for i in range(load_ref.shape[0] // block):
        sl = slice(i * block, (i + 1) * block)
        latent = lax.dot_general(load_ref[sl], fac, (((1,), (1,)), ((), ())), preferred_element_type=f32)
        p_ref[sl, cols] = (jnp.tanh(latent + IDIO_SCALE * idio_ref[sl].astype(f32)) + 1.0).astype(bf16)
    put_codes(jnp.dot(expot_ref[...], p_ref[:, cols], preferred_element_type=f32), edge_ref, pay_refs, cols)


def losses_kernel(wide, p_ref, expot_ref, edge_ref, *pay_refs):
    cols = pl.ds(pl.multiple_of(pl.program_id(0) * wide, wide), wide)
    put_codes(jnp.dot(expot_ref[...], p_ref[:, cols], preferred_element_type=f32), edge_ref, pay_refs, cols)


def mid_kernel(*refs):
    part_ref = refs[-1]
    count = len(refs) // 3
    early_refs, pay_refs, out_refs = refs[:count], refs[count : 2 * count], refs[2 * count : -1]
    wide = part_ref.shape[1]
    begin = wide // 2
    piece = min(1024, begin)
    lane = lax.broadcasted_iota(jnp.int32, (part_ref.shape[0], 128), 1)
    for k, out_ref in enumerate(out_refs):
        row = lax.rem(spot()[1] + k, count)
        edges = [pay_ref[row, :, begin:].astype(f32) for pay_ref in pay_refs]
        spans = [edge[:, 0:1] for edge in edges]
        offset = 0.5 * sum(spans)
        factors = [span * (1.0 / SPAN) for span in spans]
        ends = (jnp.full((part_ref.shape[0], 1), jnp.inf, f32), jnp.full((part_ref.shape[0], 1), -jnp.inf, f32))
        for shift, sources in ((0, early_refs), (begin, pay_refs)):

            def add(i, ends, shift=shift, sources=sources):
                here = pl.ds(pl.multiple_of(i * piece, piece), piece)
                codes = [ref[row, :, here].astype(f32) for ref in sources]
                part = sum(jnp.log(code) * factor for code, factor in zip(codes, factors)) + offset
                part_ref[:, pl.ds(pl.multiple_of(shift + i * piece, piece), piece)] = part
                low = jnp.minimum(ends[0], jnp.min(part, axis=1, keepdims=True))
                return low, jnp.maximum(ends[1], jnp.max(part, axis=1, keepdims=True))

            ends = lax.fori_loop(0, begin // piece, add, ends)
        low, high = ends
        span = jnp.maximum(jnp.maximum(high - low, jnp.abs(low) * (1.0 / 64.0)), 1e-30)
        base = low.astype(bf16).astype(f32)
        span = (span * 1.02).astype(bf16).astype(f32)

        def code(i, carry, base=base, span=span, out_ref=out_ref):
            here = pl.ds(pl.multiple_of(i * piece, piece), piece)
            out_ref[:, here] = jnp.exp((part_ref[:, here] - base) * (SPAN / span) - 0.5 * SPAN).astype(bf16)
            return carry

        lax.fori_loop(0, wide // piece, code, 0)
        total = sum(edge[:, 1:2] + edge[:, 2:3] + edge[:, 3:4] for edge in edges)
        edge = jnp.zeros(lane.shape, f32)
        for at, value in enumerate([base, span] + split3(total)):
            edge = jnp.where(lane == at, value, edge)
        out_ref[:, wide:] = edge.astype(bf16)


def sum_kernel(*refs):
    pay_refs, losses_ref, both_ref = refs[:-2], refs[-2], refs[-1]
    wide = losses_ref.shape[1]
    edges = [pay_ref[:, wide:].astype(f32) for pay_ref in pay_refs]
    spans = [edge[:, 1:2] for edge in edges]
    offset = sum(edge[:, 0:1] for edge in edges) + 0.5 * sum(spans)
    scale = 0.5 / sum(edge[:, 2:3] + edge[:, 3:4] + edge[:, 4:5] for edge in edges)
    factors = [span * (1.0 / SPAN) for span in spans]
    piece = min(1024, wide)
    total = 0.0
    for at in range(0, wide, piece):
        codes = [pay_ref[:, at : at + piece].astype(f32) for pay_ref in pay_refs]
        part = sum(jnp.log(code) * factor for code, factor in zip(codes, factors))
        part = (part + offset) * scale
        losses_ref[:, at : at + piece] = part
        total += jnp.sum(part, axis=1, keepdims=True)
    mean = total * (1.0 / wide)
    second = jnp.sum(jnp.square(losses_ref[...] - mean), axis=1, keepdims=True)
    lane = lax.broadcasted_iota(jnp.int32, both_ref.shape[1:], 1)
    both = jnp.where(lane == 0, mean, jnp.where(lane == 1, second, 0.0))
    for k in range(both_ref.shape[0]):
        both_ref[k] = both


def tail_kernel(tail_scale, scenarios, losses_ref, both_ref, pay_ref):
    groups = both_ref.shape[0]
    wide = losses_ref.shape[1]
    means = [both_ref[k, :, 0:1] for k in range(groups)]
    center = sum(means) * (1.0 / groups)
    spread = sum(both_ref[k, :, 1:2] for k in range(groups)) * (1.0 / scenarios)
    spread += sum(jnp.square(each - center) for each in means) * (1.0 / groups)
    deviation = jnp.sqrt(spread + EPSILON)
    thresh = center + QUANTILE * deviation
    width = SMOOTH * deviation
    narrow = 1.0 / width
    piece = min(1024, wide)
    soft = 0.0
    for at in range(0, wide, piece):
        scaled = (losses_ref[:, at : at + piece] - thresh) * narrow
        small = jnp.exp(-jnp.abs(scaled))
        grown = 1.0 + small
        half = 0.5 * tail_scale
        weight = (jnp.where(scaled >= 0.0, half, half * small) / grown).astype(bf16)
        soft += jnp.sum(jnp.maximum(scaled, 0.0) + jnp.log(grown), axis=1, keepdims=True)
        pay_ref[:, at : at + piece] = weight
    lane = lax.broadcasted_iota(jnp.int32, (pay_ref.shape[0], 128), 1)
    edge = jnp.zeros(lane.shape, f32)
    for at, part in enumerate(split3(soft) + split3(thresh) + split3(width)):
        edge = jnp.where(lane == at, part, edge)
    pay_ref[:, wide:] = edge.astype(bf16)


def join_kernel(*refs):
    count = len(refs) - 2
    early_ref, late_ref = refs[-2:]
    begin = early_ref.shape[2]
    for k in range(count):
        at = lax.rem(spot()[1] + (count - k), count)
        early_ref[at] = refs[k][:, 0:begin]
        late_ref[at] = refs[k][:, begin:]


def early_spread_kernel(*refs):
    count = len(refs) - 1
    rows = refs[-1].shape[0] // count
    for k in range(count):
        at = pl.multiple_of(lax.rem(spot()[0] + (count - k), count) * rows, rows)
        refs[-1][pl.ds(at, rows)] = refs[k][...].reshape(rows, -1)


def spread_kernel(*refs):
    pay_refs, (weight_ref, soft_ref, stat_ref, head_ref) = refs[:-4], refs[-4:]
    count = len(pay_refs)
    wide = weight_ref.shape[1]
    rows = weight_ref.shape[0] // count
    for k, pay_ref in enumerate(pay_refs):
        at = pl.multiple_of(lax.rem(spot()[0] + (count - k), count) * rows, rows)
        weight_ref[pl.ds(at, rows)] = pay_ref[:, :, 0:wide].reshape(rows, wide)
        head_ref[pl.ds(at, rows)] = pay_ref[:, :, wide:].reshape(rows, 128).astype(f32)
    heads = jnp.transpose(head_ref[...])
    soft_ref[...] = jnp.broadcast_to(join3(heads, 0), soft_ref.shape)
    stat_ref[...] = jnp.zeros_like(stat_ref)
    stat_ref[0:1] = join3(heads, 3)
    stat_ref[1:2] = join3(heads, 6)


def gradient_kernel(own, p_ref, weight_ref, *refs):
    out_ref = refs[-1]
    rows = out_ref.shape[0]
    core = lax.axis_index("c")
    half = core if own else 1 - core
    at = (half * pl.num_programs(0) + pl.program_id(0)) * rows
    part = lax.dot_general(
        p_ref[pl.ds(pl.multiple_of(at, rows), rows)],
        weight_ref[...],
        (((1,), (1,)), ((), ())),
        preferred_element_type=f32,
    )
    out_ref[...] = part if len(refs) == 1 else part + refs[0][...]


def pair_kernel(own_ref, other_ref, soft_ref, soft_other_ref, *pay_refs):
    count = len(pay_refs)
    rows = pay_refs[0].shape[0] - HEAD
    soft = soft_ref[0:1] + soft_other_ref[0:1]
    for k, pay_ref in enumerate(pay_refs):
        at = pl.multiple_of(lax.rem(lax.axis_index("x") + k, count) * rows, rows)
        code, head = encode(own_ref[pl.ds(at, rows)] + other_ref[pl.ds(at, rows)], [soft])
        pay_ref[0:rows] = code
        pay_ref[rows : rows + HEAD] = head


def whole_kernel(tail_scale, stat_ref, *refs):
    pay_refs, out_ref, short_ref = refs[:-2], refs[-2], refs[-1]
    rows = out_ref.shape[0] - HEAD
    total = jnp.zeros((rows, out_ref.shape[1]), f32)
    soft = jnp.zeros((1, out_ref.shape[1]), f32)
    for pay_ref in pay_refs:
        head = pay_ref[rows : rows + HEAD].astype(f32)
        total += decode(pay_ref[0:rows], head)
        soft += join3(head, 2)
    code, head = encode(total, [])
    out_ref[0:rows] = code
    out_ref[rows : rows + HEAD] = head
    short_ref[...] = jnp.broadcast_to(stat_ref[0:1] + stat_ref[1:2] * (soft * tail_scale), short_ref.shape)


def update_kernel(count, last, side, *refs):
    own_refs, other_refs = refs[:count], refs[count : 2 * count]
    prev_ref, lge_ref, unnorm_ref = refs[2 * count : 2 * count + 3]
    rows = own_refs[0].shape[0] - HEAD
    core = lax.axis_index("c")
    total = jnp.zeros((1, prev_ref.shape[1]), f32)
    reach = jnp.zeros((1, prev_ref.shape[1]), f32)
    for half, pay_refs in ((core, own_refs), (1 - core, other_refs)):
        for k, pay_ref in enumerate(pay_refs):
            at = (half * count + lax.rem(lax.axis_index("x") + (count - k), count)) * rows
            here = pl.ds(pl.multiple_of(at, rows), rows)
            gradient = decode(pay_ref[0:rows], pay_ref[rows : rows + HEAD].astype(f32))
            lge = lge_ref[here]
            unnorm = prev_ref[here] * jnp.exp(lge * (-STEP_RATE * gradient))
            unnorm_ref[here] = unnorm
            total += jnp.sum(unnorm, axis=0, keepdims=True)
            if not last:
                expo = (unnorm * lge).astype(bf16).astype(f32)
                put_rotated(refs[-2], here, jnp.transpose(expo).astype(bf16), side)
                reach += jnp.sum(expo, axis=0, keepdims=True)
    if last:
        refs[-1][...] = jnp.broadcast_to(total[None], refs[-1].shape)
    else:
        put_rotated(refs[-1], slice(None), edge_of(total, reach), side)


def scale_kernel(obligors, unnorm_ref, totals_ref, out_ref):
    rows = out_ref.shape[0]
    here = pl.ds(pl.multiple_of(pl.program_id(0) * rows, rows), rows)
    total = sum(totals_ref[k] for k in range(totals_ref.shape[0]))
    out_ref[...] = unnorm_ref[here] * (obligors / total)


VMEM = pl.BlockSpec(memory_space=pltpu.VMEM)


def near(array):
    return array if INTERPRET else pltpu.with_memory_space_constraint(array, pltpu.VMEM)


def far(array):
    return array if INTERPRET else pltpu.with_memory_space_constraint(array, pltpu.HBM)


def near_shape(shape, dtype):
    return jax.ShapeDtypeStruct(shape, dtype) if INTERPRET else pltpu.VMEM(shape, dtype)


def whole(shape):
    return pl.BlockSpec(shape, lambda *_: (0,) * len(shape))


def groups_of(side, n_x):
    span = range(side)
    plane = lambda y, z, c: (y * side + z) * 2 + c
    along_y = lambda c: [[plane(y, z, c) for y in span] for z in span]
    along_z = lambda c: [[plane(y, z, c) for z in span] for y in span]
    place = lambda y, z, x, c: ((y * side + z) * n_x + x) * 2 + c
    same = [
        [place(a, b, x, 0) for x in range(n_x)] + [place(b, a, x, 1) for x in range(n_x)] for a in span for b in span
    ]
    return along_y(0) + along_z(1), along_z(0) + along_y(1), same


def exchanged(slots, groups):
    count = len(slots)
    out = list(slots)
    for k in sorted(range(1, count), key=lambda k: -min(k, count - k)):
        out[k] = lax.ppermute(
            slots[k], PLANE, [(group[i], group[(i + k) % count]) for group in groups for i in range(count)]
        )
    return out


def rounded(value):
    return lax.reduce_precision(value, 8, 7)


def on_device(factors, idiosyncratic, loadings, rating, barrier, loss_given, sector, allowed, holdings):
    sds = jax.ShapeDtypeStruct
    n_obl, n_x, n_c = lax.axis_size(OBL), lax.axis_size("x"), lax.axis_size("c")
    side = lax.axis_size("y")
    first, second, same = groups_of(side, n_x)
    obl_dev, scn_dev = idiosyncratic.shape
    mandates = holdings.shape[1]
    obligors = obl_dev * n_obl
    scenarios = scn_dev * n_x * n_c
    tail_scale = 1.0 / ((1.0 - LEVEL) * scenarios)
    ro = obl_dev // (n_x * n_c)
    po = ro + HEAD
    mr = mandates // n_obl
    half = obl_dev // n_c
    row8 = sds((8, mandates), f32)
    ratings = barrier.shape[0]
    bar_a = rounded(barrier)
    bar_b = rounded(barrier - bar_a)
    bar_c = barrier - bar_a - bar_b
    bars = -jnp.concatenate([bar_a, bar_b, bar_c])
    bars = jnp.pad(bars, (0, 128 - 3 * ratings)).astype(bf16)[None, :]
    fdim = factors.shape[1]

    sb = min(512, obl_dev)
    line = pl.BlockSpec((1, sb), lambda i: (0, i))
    prev, lge, aug, expot, edge = call(
        functools.partial(setup_kernel, side),
        (obl_dev // sb,),
        [
            pl.BlockSpec((sb, mandates), lambda i: (i, 0)),
            line,
            line,
            line,
            whole(allowed.shape[::-1]),
            pl.BlockSpec((sb, fdim), lambda i: (i, 0)),
        ],
        [VMEM] * 5,
        [
            near_shape((obl_dev, mandates), f32),
            near_shape((obl_dev, mandates), f32),
            near_shape((obl_dev, fdim + 128), bf16),
            near_shape((mandates, obl_dev), bf16),
            near_shape((mandates, 128), bf16),
        ],
        scratch=[pltpu.VMEM((8, mandates), f32)],
        nbytes=obl_dev * mandates * 12,
        name="setup",
    )(far(holdings), far(loss_given[None, :]), far(sector[None, :]), far(rating[None, :]), allowed.T, far(loadings))
    lge = near(lge)

    results = []
    probs = []
    for iteration in range(STEPS):
        part = scn_dev // 2
        early = sds((side, mr, part), bf16)
        late = sds((side, mr, part + 128), bf16)
        few = sds((mr, scn_dev + 128), bf16)
        wide = min(512, part)
        steps = part // wide
        probs = [] if iteration == 0 else probs
        arrived = []
        for which, shape in enumerate((early, late)):
            if iteration == 0:
                prob, *pays = call(
                    first_losses_kernel,
                    (steps,),
                    [
                        VMEM,
                        pl.BlockSpec((wide, fdim), lambda i, w=which: (w * steps + i, 0)),
                        whole((1, 128)),
                        pl.BlockSpec((obl_dev, wide), lambda i, w=which: (0, w * steps + i)),
                        VMEM,
                        VMEM,
                    ],
                    [VMEM] * (1 + side),
                    [near_shape((obl_dev, part), bf16)] + [shape] * side,
                    flops=4 * obl_dev * part * mandates,
                    nbytes=obl_dev * part * 4,
                    name="first_losses",
                )(near(aug), factors, bars, far(idiosyncratic), near(expot), near(edge))
                probs.append(near(prob))
            else:
                pays = call(
                    functools.partial(losses_kernel, wide),
                    (steps,),
                    [VMEM, VMEM, VMEM],
                    [VMEM] * side,
                    [shape] * side,
                    flops=2 * obl_dev * part * mandates,
                    nbytes=obl_dev * part * 2,
                    name="losses",
                )(probs[which], near(expot), near(edge))
            arrived += exchanged(pays, first)
        pays = call(
            mid_kernel,
            (1,),
            [VMEM] * (2 * side),
            [VMEM] * side,
            [few] * side,
            scratch=[pltpu.VMEM((mr, scn_dev), f32)],
            nbytes=mandates * scn_dev * 2,
            name="mid",
        )(*arrived)
        pays = exchanged(pays, second)
        n_scn = n_x * n_c
        losses, both = call(
            sum_kernel,
            (1,),
            [VMEM] * side,
            [VMEM, VMEM],
            [near_shape((mr, scn_dev), f32), sds((n_scn, mr, 128), f32)],
            nbytes=mandates * scn_dev * 2,
            name="sum",
        )(*pays)
        both = lax.all_to_all(both, OBL + SCN, 0, 0, axis_index_groups=same, tiled=True)
        weight = call(
            functools.partial(tail_kernel, tail_scale, scenarios),
            (1,),
            [VMEM, VMEM],
            VMEM,
            few,
            nbytes=mandates * scn_dev * 2,
            name="tail",
        )(near(losses), both)
        weights = call(
            join_kernel,
            (1,),
            [VMEM] * side,
            [VMEM] * 2,
            [early, late],
            nbytes=scn_dev * mandates,
            name="join",
        )(*exchanged([weight] * side, second))
        weights = [exchanged([weight] * side, first) for weight in weights]
        early_weight = call(
            early_spread_kernel,
            (1,),
            [VMEM] * side,
            VMEM,
            near_shape((mandates, part), bf16),
            nbytes=part * mandates * 4,
            name="early_spread",
        )(*weights[0])
        late_weight, soft, stat = call(
            spread_kernel,
            (1,),
            [VMEM] * side,
            [VMEM, whole((8, mandates)), whole((8, mandates))],
            [near_shape((mandates, part), bf16), row8, row8],
            scratch=[pltpu.VMEM((mandates, 128), f32)],
            nbytes=part * mandates * 4,
            name="spread",
        )(*weights[1])
        weights = [near(early_weight), near(late_weight)]
        gblock = min(256, half)

        def gradient_of(own, which, *before):
            return call(
                functools.partial(gradient_kernel, own),
                (half // gblock,),
                [VMEM, VMEM] + [pl.BlockSpec((gblock, mandates), lambda i: (i, 0))] * len(before),
                pl.BlockSpec((gblock, mandates), lambda i: (i, 0)),
                sds((half, mandates), f32),
                flops=2 * half * part * mandates,
                nbytes=half * part * 2,
                name="gradient",
            )(probs[which], weights[which], *before)

        swap = [(0, 1), (1, 0)]
        sent, kept = gradient_of(False, 0), gradient_of(True, 0)
        sent = lax.ppermute(gradient_of(False, 1, sent), "c", swap)
        soft_other = lax.ppermute(soft, "c", swap)
        kept = gradient_of(True, 1, kept)
        gshape = sds((po, mandates), bf16)
        hops = {k: [(i, (i + k) % n_x) for i in range(n_x)] for k in range(1, n_x)}
        order = sorted(hops, key=lambda k: -min(k, n_x - k))
        slots = call(
            pair_kernel,
            (1,),
            [VMEM, VMEM, whole((8, mandates)), whole((8, mandates))],
            [VMEM] * n_x,
            [gshape] * n_x,
            nbytes=half * mandates * 10,
            name="pair",
        )(kept, sent, soft, soft_other)
        slots = list(slots)
        for k in order:
            slots[k] = lax.ppermute(slots[k], "x", hops[k])
        pay, short = call(
            functools.partial(whole_kernel, tail_scale),
            (1,),
            [whole((8, mandates))] + [VMEM] * n_x,
            [VMEM, whole((8, mandates))],
            [gshape, row8],
            nbytes=half * mandates * 4,
            name="whole",
        )(stat, *slots)
        results.append(short[0])
        slots = [pay] * n_x
        for k in order:
            slots[k] = lax.ppermute(pay, "x", hops[k])
        others = [lax.ppermute(slot, "c", swap) for slot in slots]
        last = iteration == STEPS - 1
        outs = call(
            functools.partial(update_kernel, n_x, last, side),
            (1,),
            [VMEM] * (2 * n_x + 2),
            [VMEM] + [VMEM] * (not last) + [VMEM],
            [near_shape((obl_dev, mandates), f32)]
            + [near_shape((mandates, obl_dev), bf16)] * (not last)
            + [sds((n_obl, 1, mandates), f32) if last else near_shape((mandates, 128), bf16)],
            nbytes=obl_dev * mandates * 14,
            name="update",
        )(*slots, *others, near(prev), lge)
        prev, expot, edge = outs[0], outs[-2], outs[-1]

    totals = lax.all_to_all(edge, OBL, 0, 0, tiled=True)
    positions = call(
        functools.partial(scale_kernel, obligors),
        (max(1, obl_dev // 512),),
        [VMEM, whole((n_obl, 1, mandates))],
        pl.BlockSpec((min(512, obl_dev), mandates), lambda i: (i, 0)),
        sds((obl_dev, mandates), f32),
        nbytes=obl_dev * mandates * 8,
        name="scale",
    )(near(prev), totals)
    return (positions, jnp.stack(results))


def solution(mesh):
    n_obl, n_scn = mesh.shape["obl"], mesh.shape["scn"]
    side = 1
    while side * side < n_obl:
        side *= 2
    fine = Mesh(mesh.devices.reshape(side, n_obl // side, n_scn // 2, 2), ("y", "z", "x", "c"))
    in_specs = (P(SCN, None), P(OBL, SCN), P(OBL, None), P(OBL), P(), P(OBL), P(OBL), P(), P(OBL, None))
    return jax.shard_map(on_device, mesh=fine, in_specs=in_specs, out_specs=(P(OBL, None), P()), check_vma=False)
```

```python
import functools

import jax
import jax.numpy as jnp
from jax import lax
from jax.experimental import pallas as pl
from jax.experimental.pallas import tpu as pltpu
from jax.sharding import Mesh
from jax.sharding import PartitionSpec as P

STEPS = 2
OBL = ("y", "z")
SCN = ("x", "c")
PLANE = ("y", "z", "c")
IDIO_SCALE = 0.8
LEVEL = 0.99
QUANTILE = 2.326
SMOOTH = 0.5
EPSILON = 1e-06
STEP_RATE = 8.0
HEAD = 8
SPAN = 127.0
INTERPRET = False

f32 = jnp.float32
bf16 = jnp.bfloat16


def call(kernel, grid, in_specs, out_specs, out_shape, scratch=(), prefetch=0, flops=0, nbytes=0, name=None):
    spec = pltpu.PrefetchScalarGridSpec(
        num_scalar_prefetch=prefetch, grid=grid, in_specs=in_specs, out_specs=out_specs, scratch_shapes=list(scratch)
    )
    return pl.pallas_call(
        kernel,
        grid_spec=spec,
        out_shape=out_shape,
        compiler_params=pltpu.CompilerParams(vmem_limit_bytes=24 * 1024 * 1024),
        cost_estimate=pl.CostEstimate(flops=int(flops), bytes_accessed=int(nbytes), transcendentals=0),
        interpret=INTERPRET,
        name=name,
    )


def split3(value):
    a = value.astype(bf16)
    rest = value - a.astype(f32)
    b = rest.astype(bf16)
    c = (rest - b.astype(f32)).astype(bf16)
    return [a.astype(f32), b.astype(f32), c.astype(f32)]


def join3(head, at):
    return head[at : at + 1] + head[at + 1 : at + 2] + head[at + 2 : at + 3]


def encode(values, extra):
    low = jnp.min(values, axis=0, keepdims=True)
    high = jnp.max(values, axis=0, keepdims=True)
    span = jnp.maximum(jnp.maximum(high - low, jnp.abs(low) * (1.0 / 64.0)), 1e-30)
    base = low.astype(bf16).astype(f32)
    span = (span * 1.02).astype(bf16).astype(f32)
    code = jnp.exp((values - base) * (SPAN / span) - 0.5 * SPAN).astype(bf16)
    rows = [base, span]
    for row in extra:
        rows += split3(row)
    if len(rows) < HEAD:
        rows.append(jnp.zeros((HEAD - len(rows), values.shape[1]), f32))
    return code, jnp.concatenate(rows, axis=0).astype(bf16)


def decode(code, head):
    base, span = head[0:1], head[1:2]
    return (base + 0.5 * span) + jnp.log(code.astype(f32)) * (span * (1.0 / SPAN))


def edge_of(total, reach):
    span = jnp.maximum(2.02 * reach, 1e-30).astype(bf16).astype(f32)
    rows = [span] + split3(total)
    rows.append(jnp.zeros((128 - len(rows), total.shape[1]), f32))
    return jnp.transpose(jnp.concatenate(rows, axis=0)).astype(bf16)


def spot():
    y, z, core = lax.axis_index("y"), lax.axis_index("z"), lax.axis_index("c")
    return jnp.where(core == 0, y, z), jnp.where(core == 0, z, y)


def put_rotated(ref, cols, value, side):
    rows = value.shape[0] // (side * side)
    first = lax.axis_index("c") == 0
    for y in range(side):
        for z in range(side):
            on = lax.rem(jnp.where(first, y, z) + side - spot()[0], side)
            at = pl.multiple_of((on * side + jnp.where(first, z, y)) * rows, rows)
            part = (y * side + z) * rows
            ref[pl.ds(at, rows), cols] = value[part : part + rows]


def put_codes(doubled, edge_ref, pay_refs, at):
    parts, rows, wide = pay_refs[0].shape
    span = edge_ref[:, 0:1].astype(f32)
    code = jnp.exp(doubled * (SPAN / span) - 0.5 * SPAN).astype(bf16)
    for k, pay_ref in enumerate(pay_refs):
        part = slice(k * parts * rows, (k + 1) * parts * rows)
        pay_ref[:, :, at] = code[part].reshape(parts, rows, -1)

    if wide % 256 == 0:
        return

    @pl.when(pl.program_id(0) == 0)
    def _():
        for k, pay_ref in enumerate(pay_refs):
            part = slice(k * parts * rows, (k + 1) * parts * rows)
            pay_ref[:, :, wide - 128 :] = edge_ref[part].reshape(parts, rows, 128)


def setup_kernel(side, hold_ref, lgd_ref, sector_ref, rating_ref, allowed_ref, load_ref, weighted_ref, lge_ref, aug_ref, expot_ref, edge_ref, sums_ref):
    rows = sector_ref.shape[1]
    sectors = allowed_ref.shape[0]
    here = pl.ds(pl.multiple_of(pl.program_id(0) * rows, rows), rows)
    allowed = allowed_ref[...].astype(f32)
    hot = (lax.broadcasted_iota(jnp.int32, (sectors, rows), 0) == sector_ref[...]).astype(f32)
    lgd = lgd_ref[...]
    parts = jnp.concatenate([hot * part for part in split3(lgd)], axis=0)
    dims = (((0,), (0,)), ((), ()))
    elig = lax.dot_general(hot.astype(bf16), allowed.astype(bf16), dims, preferred_element_type=f32)
    thrice = jnp.concatenate([allowed] * 3, axis=0)
    lge = lax.dot_general(parts.astype(bf16), thrice.astype(bf16), dims, preferred_element_type=f32)
    hold = hold_ref[...]
    weighted = elig * hold
    weighted_ref[here] = weighted
    lge_ref[here] = lge
    expo = (lge * hold).astype(bf16).astype(f32)
    put_rotated(expot_ref, here, jnp.transpose(expo).astype(bf16), side)
    lane = lax.broadcasted_iota(jnp.int32, (128, rows), 0)
    rated = ((lane % 16 == rating_ref[...]) & (lane < 48)).astype(f32)
    aug_ref[here] = jnp.concatenate([load_ref[...], jnp.transpose(rated).astype(bf16)], axis=1)

    @pl.when(pl.program_id(0) == 0)
    def _():
        sums_ref[...] = jnp.zeros_like(sums_ref)

    sums_ref[0:1] += jnp.sum(weighted, axis=0, keepdims=True)
    sums_ref[1:2] += jnp.sum(expo, axis=0, keepdims=True)

    @pl.when(pl.program_id(0) == pl.num_programs(0) - 1)
    def _():
        put_rotated(edge_ref, slice(None), edge_of(sums_ref[0:1], sums_ref[1:2]), side)


def first_losses_kernel(load_ref, fac_ref, bar_ref, idio_ref, expot_ref, edge_ref, p_ref, *pay_refs):
    wide = fac_ref.shape[0]
    cols = pl.ds(pl.multiple_of(pl.program_id(0) * wide, wide), wide)
    block = min(256, load_ref.shape[0])
    fac = jnp.concatenate([fac_ref[...], jnp.broadcast_to(bar_ref[...], (wide, 128))], axis=1)
    for i in range(load_ref.shape[0] // block):
        sl = slice(i * block, (i + 1) * block)
        latent = lax.dot_general(load_ref[sl], fac, (((1,), (1,)), ((), ())), preferred_element_type=f32)
        p_ref[sl, cols] = (jnp.tanh(latent + IDIO_SCALE * idio_ref[sl].astype(f32)) + 1.0).astype(bf16)
    put_codes(jnp.dot(expot_ref[...], p_ref[:, cols], preferred_element_type=f32), edge_ref, pay_refs, cols)


def losses_kernel(wide, begin, p_ref, expot_ref, edge_ref, *pay_refs):
    at = pl.multiple_of(pl.program_id(0) * wide, wide)
    prob = p_ref[:, pl.ds(begin + at, wide)]
    put_codes(jnp.dot(expot_ref[...], prob, preferred_element_type=f32), edge_ref, pay_refs, pl.ds(at, wide))


def mid_kernel(pieces, *refs):
    part_ref = refs[-1]
    count = len(refs) // (pieces + 1)
    pay_refs = [refs[k * count : (k + 1) * count] for k in range(pieces)]
    out_refs = refs[pieces * count : -1]
    wide = part_ref.shape[1]
    begin = wide // pieces
    piece = min(1024, begin)
    lane = lax.broadcasted_iota(jnp.int32, (part_ref.shape[0], 128), 1)
    for k, out_ref in enumerate(out_refs):
        row = lax.rem(spot()[1] + k, count)
        edges = [pay_ref[row, :, begin:].astype(f32) for pay_ref in pay_refs[-1]]
        spans = [edge[:, 0:1] for edge in edges]
        offset = 0.5 * sum(spans)
        factors = [span * (1.0 / SPAN) for span in spans]
        low, high = jnp.inf, -jnp.inf
        for at in range(0, wide, piece):
            here = slice(at % begin, at % begin + piece)
            codes = [pay_ref[row, :, here].astype(f32) for pay_ref in pay_refs[at // begin]]
            part = sum(jnp.log(code) * factor for code, factor in zip(codes, factors)) + offset
            part_ref[:, at : at + piece] = part
            low = jnp.minimum(low, jnp.min(part, axis=1, keepdims=True))
            high = jnp.maximum(high, jnp.max(part, axis=1, keepdims=True))
        span = jnp.maximum(jnp.maximum(high - low, jnp.abs(low) * (1.0 / 64.0)), 1e-30)
        base = low.astype(bf16).astype(f32)
        span = (span * 1.02).astype(bf16).astype(f32)
        for at in range(0, wide, piece):
            part = part_ref[:, at : at + piece]
            out_ref[:, at : at + piece] = jnp.exp((part - base) * (SPAN / span) - 0.5 * SPAN).astype(bf16)
        total = sum(edge[:, 1:2] + edge[:, 2:3] + edge[:, 3:4] for edge in edges)
        edge = jnp.zeros(lane.shape, f32)
        for at, value in enumerate([base, span] + split3(total)):
            edge = jnp.where(lane == at, value, edge)
        out_ref[:, wide:] = edge.astype(bf16)


def sum_kernel(*refs):
    pay_refs, losses_ref, both_ref = refs[:-2], refs[-2], refs[-1]
    wide = losses_ref.shape[1]
    edges = [pay_ref[:, wide:].astype(f32) for pay_ref in pay_refs]
    spans = [edge[:, 1:2] for edge in edges]
    offset = sum(edge[:, 0:1] for edge in edges) + 0.5 * sum(spans)
    scale = 0.5 / sum(edge[:, 2:3] + edge[:, 3:4] + edge[:, 4:5] for edge in edges)
    factors = [span * (1.0 / SPAN) for span in spans]
    piece = min(1024, wide)
    total = 0.0
    for at in range(0, wide, piece):
        codes = [pay_ref[:, at : at + piece].astype(f32) for pay_ref in pay_refs]
        part = sum(jnp.log(code) * factor for code, factor in zip(codes, factors))
        part = (part + offset) * scale
        losses_ref[:, at : at + piece] = part
        total += jnp.sum(part, axis=1, keepdims=True)
    mean = total * (1.0 / wide)
    second = jnp.sum(jnp.square(losses_ref[...] - mean), axis=1, keepdims=True)
    lane = lax.broadcasted_iota(jnp.int32, both_ref.shape[1:], 1)
    both = jnp.where(lane == 0, mean, jnp.where(lane == 1, second, 0.0))
    for k in range(both_ref.shape[0]):
        both_ref[k] = both


def tail_kernel(tail_scale, scenarios, losses_ref, both_ref, pay_ref):
    groups = both_ref.shape[0]
    wide = losses_ref.shape[1]
    means = [both_ref[k, :, 0:1] for k in range(groups)]
    center = sum(means) * (1.0 / groups)
    spread = sum(both_ref[k, :, 1:2] for k in range(groups)) * (1.0 / scenarios)
    spread += sum(jnp.square(each - center) for each in means) * (1.0 / groups)
    deviation = jnp.sqrt(spread + EPSILON)
    thresh = center + QUANTILE * deviation
    width = SMOOTH * deviation
    narrow = 1.0 / width
    piece = min(1024, wide)
    soft = 0.0
    for at in range(0, wide, piece):
        scaled = (losses_ref[:, at : at + piece] - thresh) * narrow
        small = jnp.exp(-jnp.abs(scaled))
        grown = 1.0 + small
        half = 0.5 * tail_scale
        weight = (jnp.where(scaled >= 0.0, half, half * small) / grown).astype(bf16)
        soft += jnp.sum(jnp.maximum(scaled, 0.0) + jnp.log(grown), axis=1, keepdims=True)
        pay_ref[:, at : at + piece] = weight
    lane = lax.broadcasted_iota(jnp.int32, (pay_ref.shape[0], 128), 1)
    edge = jnp.zeros(lane.shape, f32)
    for at, part in enumerate(split3(soft) + split3(thresh) + split3(width)):
        edge = jnp.where(lane == at, part, edge)
    pay_ref[:, wide:] = edge.astype(bf16)


def join_kernel(*refs):
    count = len(refs) - 1
    for k in range(count):
        refs[-1][lax.rem(spot()[1] + (count - k), count)] = refs[k][...]


def spread_kernel(*refs):
    pay_refs, (weight_ref, soft_ref, stat_ref, head_ref) = refs[:-4], refs[-4:]
    count = len(pay_refs)
    wide = weight_ref.shape[1]
    rows = weight_ref.shape[0] // (count * count)
    for k, pay_ref in enumerate(pay_refs):
        place = lax.rem(spot()[0] + (count - k), count)
        for j in range(count):
            owner = jnp.where(lax.axis_index("c") == 0, place * count + j, j * count + place)
            at = pl.multiple_of(owner * rows, rows)
            weight_ref[pl.ds(at, rows)] = pay_ref[j, :, 0:wide]
            head_ref[pl.ds(at, rows)] = pay_ref[j, :, wide:].astype(f32)
    heads = jnp.transpose(head_ref[...])
    soft_ref[...] = jnp.broadcast_to(join3(heads, 0), soft_ref.shape)
    stat_ref[...] = jnp.zeros_like(stat_ref)
    stat_ref[0:1] = join3(heads, 3)
    stat_ref[1:2] = join3(heads, 6)


def gradient_kernel(own, p_ref, weight_ref, out_ref):
    rows = out_ref.shape[0]
    core = lax.axis_index("c")
    half = core if own else 1 - core
    at = (half * pl.num_programs(0) + pl.program_id(0)) * rows
    out_ref[...] = lax.dot_general(
        p_ref[pl.ds(pl.multiple_of(at, rows), rows)],
        weight_ref[...],
        (((1,), (1,)), ((), ())),
        preferred_element_type=f32,
    )


def pair_kernel(own_ref, other_ref, soft_ref, soft_other_ref, *pay_refs):
    count = len(pay_refs)
    rows = pay_refs[0].shape[0] - HEAD
    soft = soft_ref[0:1] + soft_other_ref[0:1]
    for k, pay_ref in enumerate(pay_refs):
        at = pl.multiple_of(lax.rem(lax.axis_index("x") + k, count) * rows, rows)
        code, head = encode(own_ref[pl.ds(at, rows)] + other_ref[pl.ds(at, rows)], [soft])
        pay_ref[0:rows] = code
        pay_ref[rows : rows + HEAD] = head


def whole_kernel(tail_scale, stat_ref, *refs):
    pay_refs, out_ref, short_ref = refs[:-2], refs[-2], refs[-1]
    rows = out_ref.shape[0] - HEAD
    total = jnp.zeros((rows, out_ref.shape[1]), f32)
    soft = jnp.zeros((1, out_ref.shape[1]), f32)
    for pay_ref in pay_refs:
        head = pay_ref[rows : rows + HEAD].astype(f32)
        total += decode(pay_ref[0:rows], head)
        soft += join3(head, 2)
    code, head = encode(total, [])
    out_ref[0:rows] = code
    out_ref[rows : rows + HEAD] = head
    short_ref[...] = jnp.broadcast_to(stat_ref[0:1] + stat_ref[1:2] * (soft * tail_scale), short_ref.shape)


def update_kernel(count, last, side, *refs):
    own_refs, other_refs = refs[:count], refs[count : 2 * count]
    prev_ref, lge_ref, unnorm_ref = refs[2 * count : 2 * count + 3]
    rows = own_refs[0].shape[0] - HEAD
    core = lax.axis_index("c")
    total = jnp.zeros((1, prev_ref.shape[1]), f32)
    reach = jnp.zeros((1, prev_ref.shape[1]), f32)
    for half, pay_refs in ((core, own_refs), (1 - core, other_refs)):
        for k, pay_ref in enumerate(pay_refs):
            at = (half * count + lax.rem(lax.axis_index("x") + (count - k), count)) * rows
            here = pl.ds(pl.multiple_of(at, rows), rows)
            gradient = decode(pay_ref[0:rows], pay_ref[rows : rows + HEAD].astype(f32))
            lge = lge_ref[here]
            unnorm = prev_ref[here] * jnp.exp(lge * (-STEP_RATE * gradient))
            unnorm_ref[here] = unnorm
            total += jnp.sum(unnorm, axis=0, keepdims=True)
            if not last:
                expo = (unnorm * lge).astype(bf16).astype(f32)
                put_rotated(refs[-2], here, jnp.transpose(expo).astype(bf16), side)
                reach += jnp.sum(expo, axis=0, keepdims=True)
    if last:
        refs[-1][...] = jnp.broadcast_to(total[None], refs[-1].shape)
    else:
        put_rotated(refs[-1], slice(None), edge_of(total, reach), side)


def scale_kernel(obligors, unnorm_ref, totals_ref, out_ref):
    rows = out_ref.shape[0]
    here = pl.ds(pl.multiple_of(pl.program_id(0) * rows, rows), rows)
    total = sum(totals_ref[k] for k in range(totals_ref.shape[0]))
    out_ref[...] = unnorm_ref[here] * (obligors / total)


VMEM = pl.BlockSpec(memory_space=pltpu.VMEM)


def near(array):
    return array if INTERPRET else pltpu.with_memory_space_constraint(array, pltpu.VMEM)


def far(array):
    return array if INTERPRET else pltpu.with_memory_space_constraint(array, pltpu.HBM)


def near_shape(shape, dtype):
    return jax.ShapeDtypeStruct(shape, dtype) if INTERPRET else pltpu.VMEM(shape, dtype)


def whole(shape):
    return pl.BlockSpec(shape, lambda *_: (0,) * len(shape))


def groups_of(side):
    span = range(side)
    plane = lambda y, z, c: (y * side + z) * 2 + c
    along_y = lambda c: [[plane(y, z, c) for y in span] for z in span]
    along_z = lambda c: [[plane(y, z, c) for z in span] for y in span]
    return along_y(0) + along_z(1), along_z(0) + along_y(1)


def exchanged(slots, groups):
    count = len(slots)
    out = list(slots)
    for k in sorted(range(1, count), key=lambda k: -min(k, count - k)):
        out[k] = lax.ppermute(
            slots[k], PLANE, [(group[i], group[(i + k) % count]) for group in groups for i in range(count)]
        )
    return out


def rounded(value):
    return lax.reduce_precision(value, 8, 7)


def on_device(factors, idiosyncratic, loadings, rating, barrier, loss_given, sector, allowed, holdings):
    sds = jax.ShapeDtypeStruct
    n_obl, n_x, n_c = lax.axis_size(OBL), lax.axis_size("x"), lax.axis_size("c")
    side = lax.axis_size("y")
    first, second = groups_of(side)
    obl_dev, scn_dev = idiosyncratic.shape
    mandates = holdings.shape[1]
    obligors = obl_dev * n_obl
    scenarios = scn_dev * n_x * n_c
    tail_scale = 1.0 / ((1.0 - LEVEL) * scenarios)
    ro = obl_dev // (n_x * n_c)
    po = ro + HEAD
    mr = mandates // n_obl
    half = obl_dev // n_c
    row8 = sds((8, mandates), f32)
    ratings = barrier.shape[0]
    bar_a = rounded(barrier)
    bar_b = rounded(barrier - bar_a)
    bar_c = barrier - bar_a - bar_b
    bars = -jnp.concatenate([bar_a, bar_b, bar_c])
    bars = jnp.pad(bars, (0, 128 - 3 * ratings)).astype(bf16)[None, :]
    fdim = factors.shape[1]

    sb = min(512, obl_dev)
    line = pl.BlockSpec((1, sb), lambda i: (0, i))
    prev, lge, aug, expot, edge = call(
        functools.partial(setup_kernel, side),
        (obl_dev // sb,),
        [
            pl.BlockSpec((sb, mandates), lambda i: (i, 0)),
            line,
            line,
            line,
            whole(allowed.shape[::-1]),
            pl.BlockSpec((sb, fdim), lambda i: (i, 0)),
        ],
        [VMEM] * 5,
        [
            near_shape((obl_dev, mandates), f32),
            near_shape((obl_dev, mandates), f32),
            near_shape((obl_dev, fdim + 128), bf16),
            near_shape((mandates, obl_dev), bf16),
            near_shape((mandates, 128), bf16),
        ],
        scratch=[pltpu.VMEM((8, mandates), f32)],
        nbytes=obl_dev * mandates * 12,
        name="setup",
    )(far(holdings), far(loss_given[None, :]), far(sector[None, :]), far(rating[None, :]), allowed.T, far(loadings))
    lge = near(lge)

    results = []
    prob = None
    for iteration in range(STEPS):
        quarter = sds((side, mr, scn_dev + 128), bf16)
        few = sds((mr, scn_dev + 128), bf16)
        wide = min(512, scn_dev)
        if iteration == 0:
            prob, *pays = call(
                first_losses_kernel,
                (scn_dev // wide,),
                [
                    VMEM,
                    pl.BlockSpec((wide, fdim), lambda i: (i, 0)),
                    whole((1, 128)),
                    pl.BlockSpec((obl_dev, wide), lambda i: (0, i)),
                    VMEM,
                    VMEM,
                ],
                [VMEM] * (1 + side),
                [near_shape((obl_dev, scn_dev), bf16)] + [quarter] * side,
                flops=4 * obl_dev * scn_dev * mandates,
                nbytes=obl_dev * scn_dev * 4,
                name="first_losses",
            )(near(aug), factors, bars, idiosyncratic, near(expot), near(edge))
            prob = near(prob)
            arrived = exchanged(pays, first)
        else:
            part = scn_dev // 2
            narrow = min(512, part)
            arrived = []
            for begin, edges in ((0, 0), (part, 128)):
                pays = call(
                    functools.partial(losses_kernel, narrow, begin),
                    (part // narrow,),
                    [VMEM, VMEM, VMEM],
                    [VMEM] * side,
                    [sds((side, mr, part + edges), bf16)] * side,
                    flops=2 * obl_dev * part * mandates,
                    nbytes=obl_dev * part * 2,
                    name="losses",
                )(prob, near(expot), near(edge))
                arrived += exchanged(pays, first)
        pays = call(
            functools.partial(mid_kernel, len(arrived) // side),
            (1,),
            [VMEM] * len(arrived),
            [VMEM] * side,
            [few] * side,
            scratch=[pltpu.VMEM((mr, scn_dev), f32)],
            nbytes=mandates * scn_dev * 2,
            name="mid",
        )(*arrived)
        pays = exchanged(pays, second)
        n_scn = n_x * n_c
        losses, both = call(
            sum_kernel,
            (1,),
            [VMEM] * side,
            [VMEM, VMEM],
            [near_shape((mr, scn_dev), f32), sds((n_scn, mr, 128), f32)],
            nbytes=mandates * scn_dev * 2,
            name="sum",
        )(*pays)
        both = lax.all_to_all(both, SCN, 0, 0, tiled=True)
        weight = call(
            functools.partial(tail_kernel, tail_scale, scenarios),
            (1,),
            [VMEM, VMEM],
            VMEM,
            few,
            nbytes=mandates * scn_dev * 2,
            name="tail",
        )(near(losses), both)
        weight = call(
            join_kernel,
            (1,),
            [VMEM] * side,
            VMEM,
            quarter,
            nbytes=scn_dev * mandates,
            name="join",
        )(*exchanged([weight] * side, second))
        weight, soft, stat = call(
            spread_kernel,
            (1,),
            [VMEM] * side,
            [VMEM, whole((8, mandates)), whole((8, mandates))],
            [near_shape((mandates, scn_dev), bf16), row8, row8],
            scratch=[pltpu.VMEM((mandates, 128), f32)],
            nbytes=scn_dev * mandates * 4,
            name="spread",
        )(*exchanged([weight] * side, first))
        weight = near(weight)
        gblock = min(512, half)

        def gradient_of(own):
            return call(
                functools.partial(gradient_kernel, own),
                (half // gblock,),
                [VMEM, VMEM],
                pl.BlockSpec((gblock, mandates), lambda i: (i, 0)),
                sds((half, mandates), f32),
                flops=2 * half * scn_dev * mandates,
                nbytes=half * scn_dev * 2,
                name="gradient",
            )(prob, weight)

        swap = [(0, 1), (1, 0)]
        sent = lax.ppermute(gradient_of(False), "c", swap)
        soft_other = lax.ppermute(soft, "c", swap)
        kept = gradient_of(True)
        gshape = sds((po, mandates), bf16)
        hops = {k: [(i, (i + k) % n_x) for i in range(n_x)] for k in range(1, n_x)}
        order = sorted(hops, key=lambda k: -min(k, n_x - k))
        slots = call(
            pair_kernel,
            (1,),
            [VMEM, VMEM, whole((8, mandates)), whole((8, mandates))],
            [VMEM] * n_x,
            [gshape] * n_x,
            nbytes=half * mandates * 10,
            name="pair",
        )(kept, sent, soft, soft_other)
        slots = list(slots)
        for k in order:
            slots[k] = lax.ppermute(slots[k], "x", hops[k])
        pay, short = call(
            functools.partial(whole_kernel, tail_scale),
            (1,),
            [whole((8, mandates))] + [VMEM] * n_x,
            [VMEM, whole((8, mandates))],
            [gshape, row8],
            nbytes=half * mandates * 4,
            name="whole",
        )(stat, *slots)
        results.append(short[0])
        slots = [pay] * n_x
        for k in order:
            slots[k] = lax.ppermute(pay, "x", hops[k])
        others = [lax.ppermute(slot, "c", swap) for slot in slots]
        last = iteration == STEPS - 1
        outs = call(
            functools.partial(update_kernel, n_x, last, side),
            (1,),
            [VMEM] * (2 * n_x + 2),
            [VMEM] + [VMEM] * (not last) + [VMEM],
            [near_shape((obl_dev, mandates), f32)]
            + [near_shape((mandates, obl_dev), bf16)] * (not last)
            + [sds((n_obl, 1, mandates), f32) if last else near_shape((mandates, 128), bf16)],
            nbytes=obl_dev * mandates * 14,
            name="update",
        )(*slots, *others, near(prev), lge)
        prev, expot, edge = outs[0], outs[-2], outs[-1]

    totals = lax.all_to_all(edge, OBL, 0, 0, tiled=True)
    positions = call(
        functools.partial(scale_kernel, obligors),
        (max(1, obl_dev // 512),),
        [VMEM, whole((n_obl, 1, mandates))],
        pl.BlockSpec((min(512, obl_dev), mandates), lambda i: (i, 0)),
        sds((obl_dev, mandates), f32),
        nbytes=obl_dev * mandates * 8,
        name="scale",
    )(near(prev), totals)
    return (positions, jnp.stack(results))


def solution(mesh):
    n_obl, n_scn = mesh.shape["obl"], mesh.shape["scn"]
    side = 1
    while side * side < n_obl:
        side *= 2
    fine = Mesh(mesh.devices.reshape(side, n_obl // side, n_scn // 2, 2), ("y", "z", "x", "c"))
    in_specs = (P(SCN, None), P(OBL, SCN), P(OBL, None), P(OBL), P(), P(OBL), P(OBL), P(), P(OBL, None))
    return jax.shard_map(on_device, mesh=fine, in_specs=in_specs, out_specs=(P(OBL, None), P()), check_vma=False)
```

```python
import functools

import jax
import jax.numpy as jnp
from jax import lax
from jax.experimental import pallas as pl
from jax.experimental.pallas import tpu as pltpu
from jax.sharding import Mesh
from jax.sharding import PartitionSpec as P

STEPS = 2
OBL = ("y", "z")
SCN = ("x", "c")
PLANE = ("y", "z", "c")
IDIO_SCALE = 0.8
LEVEL = 0.99
QUANTILE = 2.326
SMOOTH = 0.5
EPSILON = 1e-06
STEP_RATE = 8.0
HEAD = 8
SPAN = 127.0
INTERPRET = False

f32 = jnp.float32
bf16 = jnp.bfloat16


def call(kernel, grid, in_specs, out_specs, out_shape, scratch=(), prefetch=0, flops=0, nbytes=0, name=None):
    spec = pltpu.PrefetchScalarGridSpec(
        num_scalar_prefetch=prefetch, grid=grid, in_specs=in_specs, out_specs=out_specs, scratch_shapes=list(scratch)
    )
    return pl.pallas_call(
        kernel,
        grid_spec=spec,
        out_shape=out_shape,
        compiler_params=pltpu.CompilerParams(vmem_limit_bytes=24 * 1024 * 1024),
        cost_estimate=pl.CostEstimate(flops=int(flops), bytes_accessed=int(nbytes), transcendentals=0),
        interpret=INTERPRET,
        name=name,
    )


def split3(value):
    a = value.astype(bf16)
    rest = value - a.astype(f32)
    b = rest.astype(bf16)
    c = (rest - b.astype(f32)).astype(bf16)
    return [a.astype(f32), b.astype(f32), c.astype(f32)]


def join3(head, at):
    return head[at : at + 1] + head[at + 1 : at + 2] + head[at + 2 : at + 3]


def encode(values, extra):
    low = jnp.min(values, axis=0, keepdims=True)
    high = jnp.max(values, axis=0, keepdims=True)
    span = jnp.maximum(jnp.maximum(high - low, jnp.abs(low) * (1.0 / 64.0)), 1e-30)
    base = low.astype(bf16).astype(f32)
    span = (span * 1.02).astype(bf16).astype(f32)
    code = jnp.exp((values - base) * (SPAN / span) - 0.5 * SPAN).astype(bf16)
    rows = [base, span]
    for row in extra:
        rows += split3(row)
    if len(rows) < HEAD:
        rows.append(jnp.zeros((HEAD - len(rows), values.shape[1]), f32))
    return code, jnp.concatenate(rows, axis=0).astype(bf16)


def decode(code, head):
    base, span = head[0:1], head[1:2]
    return (base + 0.5 * span) + jnp.log(code.astype(f32)) * (span * (1.0 / SPAN))


def edge_of(total, reach):
    span = jnp.maximum(2.02 * reach, 1e-30).astype(bf16).astype(f32)
    rows = [span] + split3(total)
    rows.append(jnp.zeros((128 - len(rows), total.shape[1]), f32))
    return jnp.transpose(jnp.concatenate(rows, axis=0)).astype(bf16)


def spot():
    y, z, core = lax.axis_index("y"), lax.axis_index("z"), lax.axis_index("c")
    return jnp.where(core == 0, y, z), jnp.where(core == 0, z, y)


def put_rotated(ref, cols, value, side):
    rows = value.shape[0] // (side * side)
    first = lax.axis_index("c") == 0
    for y in range(side):
        for z in range(side):
            on = lax.rem(jnp.where(first, y, z) + side - spot()[0], side)
            at = pl.multiple_of((on * side + jnp.where(first, z, y)) * rows, rows)
            part = (y * side + z) * rows
            ref[pl.ds(at, rows), cols] = value[part : part + rows]


def put_codes(doubled, edge_ref, pay_refs, at):
    parts, rows, wide = pay_refs[0].shape
    span = edge_ref[:, 0:1].astype(f32)
    code = jnp.exp(doubled * (SPAN / span) - 0.5 * SPAN).astype(bf16)
    for k, pay_ref in enumerate(pay_refs):
        part = slice(k * parts * rows, (k + 1) * parts * rows)
        pay_ref[:, :, at] = code[part].reshape(parts, rows, -1)

    if wide % 256 == 0:
        return

    @pl.when(pl.program_id(0) == 0)
    def _():
        for k, pay_ref in enumerate(pay_refs):
            part = slice(k * parts * rows, (k + 1) * parts * rows)
            pay_ref[:, :, wide - 128 :] = edge_ref[part].reshape(parts, rows, 128)


def setup_kernel(side, hold_ref, lgd_ref, sector_ref, rating_ref, allowed_ref, load_ref, weighted_ref, lge_ref, aug_ref, expot_ref, edge_ref, sums_ref):
    rows = sector_ref.shape[1]
    sectors = allowed_ref.shape[0]
    here = pl.ds(pl.multiple_of(pl.program_id(0) * rows, rows), rows)
    allowed = allowed_ref[...].astype(f32)
    hot = (lax.broadcasted_iota(jnp.int32, (sectors, rows), 0) == sector_ref[...]).astype(f32)
    lgd = lgd_ref[...]
    parts = jnp.concatenate([hot * part for part in split3(lgd)], axis=0)
    dims = (((0,), (0,)), ((), ()))
    elig = lax.dot_general(hot.astype(bf16), allowed.astype(bf16), dims, preferred_element_type=f32)
    thrice = jnp.concatenate([allowed] * 3, axis=0)
    lge = lax.dot_general(parts.astype(bf16), thrice.astype(bf16), dims, preferred_element_type=f32)
    hold = hold_ref[...]
    weighted = elig * hold
    weighted_ref[here] = weighted
    lge_ref[here] = lge
    expo = (lge * hold).astype(bf16).astype(f32)
    put_rotated(expot_ref, here, jnp.transpose(expo).astype(bf16), side)
    lane = lax.broadcasted_iota(jnp.int32, (128, rows), 0)
    rated = ((lane % 16 == rating_ref[...]) & (lane < 48)).astype(f32)
    aug_ref[here] = jnp.concatenate([load_ref[...], jnp.transpose(rated).astype(bf16)], axis=1)

    @pl.when(pl.program_id(0) == 0)
    def _():
        sums_ref[...] = jnp.zeros_like(sums_ref)

    sums_ref[0:1] += jnp.sum(weighted, axis=0, keepdims=True)
    sums_ref[1:2] += jnp.sum(expo, axis=0, keepdims=True)

    @pl.when(pl.program_id(0) == pl.num_programs(0) - 1)
    def _():
        put_rotated(edge_ref, slice(None), edge_of(sums_ref[0:1], sums_ref[1:2]), side)


def first_losses_kernel(load_ref, fac_ref, bar_ref, idio_ref, expot_ref, edge_ref, p_ref, *pay_refs):
    wide = fac_ref.shape[0]
    cols = pl.ds(pl.multiple_of(pl.program_id(0) * wide, wide), wide)
    block = min(256, load_ref.shape[0])
    fac = jnp.concatenate([fac_ref[...], jnp.broadcast_to(bar_ref[...], (wide, 128))], axis=1)
    for i in range(load_ref.shape[0] // block):
        sl = slice(i * block, (i + 1) * block)
        latent = lax.dot_general(load_ref[sl], fac, (((1,), (1,)), ((), ())), preferred_element_type=f32)
        p_ref[sl, cols] = (jnp.tanh(latent + IDIO_SCALE * idio_ref[sl].astype(f32)) + 1.0).astype(bf16)
    put_codes(jnp.dot(expot_ref[...], p_ref[:, cols], preferred_element_type=f32), edge_ref, pay_refs, cols)


def losses_kernel(wide, begin, p_ref, expot_ref, edge_ref, *pay_refs):
    at = pl.multiple_of(pl.program_id(0) * wide, wide)
    prob = p_ref[:, pl.ds(begin + at, wide)]
    put_codes(jnp.dot(expot_ref[...], prob, preferred_element_type=f32), edge_ref, pay_refs, pl.ds(at, wide))


def mid_kernel(pieces, *refs):
    part_ref = refs[-1]
    count = len(refs) // (pieces + 1)
    pay_refs = [refs[k * count : (k + 1) * count] for k in range(pieces)]
    out_refs = refs[pieces * count : -1]
    wide = part_ref.shape[1]
    begin = wide // pieces
    piece = min(1024, begin)
    lane = lax.broadcasted_iota(jnp.int32, (part_ref.shape[0], 128), 1)
    for k, out_ref in enumerate(out_refs):
        row = lax.rem(spot()[1] + k, count)
        edges = [pay_ref[row, :, begin:].astype(f32) for pay_ref in pay_refs[-1]]
        spans = [edge[:, 0:1] for edge in edges]
        offset = 0.5 * sum(spans)
        factors = [span * (1.0 / SPAN) for span in spans]
        low, high = jnp.inf, -jnp.inf
        for at in range(0, wide, piece):
            here = slice(at % begin, at % begin + piece)
            codes = [pay_ref[row, :, here].astype(f32) for pay_ref in pay_refs[at // begin]]
            part = sum(jnp.log(code) * factor for code, factor in zip(codes, factors)) + offset
            part_ref[:, at : at + piece] = part
            low = jnp.minimum(low, jnp.min(part, axis=1, keepdims=True))
            high = jnp.maximum(high, jnp.max(part, axis=1, keepdims=True))
        span = jnp.maximum(jnp.maximum(high - low, jnp.abs(low) * (1.0 / 64.0)), 1e-30)
        base = low.astype(bf16).astype(f32)
        span = (span * 1.02).astype(bf16).astype(f32)
        for at in range(0, wide, piece):
            part = part_ref[:, at : at + piece]
            out_ref[:, at : at + piece] = jnp.exp((part - base) * (SPAN / span) - 0.5 * SPAN).astype(bf16)
        total = sum(edge[:, 1:2] + edge[:, 2:3] + edge[:, 3:4] for edge in edges)
        edge = jnp.zeros(lane.shape, f32)
        for at, value in enumerate([base, span] + split3(total)):
            edge = jnp.where(lane == at, value, edge)
        out_ref[:, wide:] = edge.astype(bf16)


def sum_kernel(*refs):
    pay_refs, losses_ref, both_ref = refs[:-2], refs[-2], refs[-1]
    wide = losses_ref.shape[1]
    edges = [pay_ref[:, wide:].astype(f32) for pay_ref in pay_refs]
    spans = [edge[:, 1:2] for edge in edges]
    offset = sum(edge[:, 0:1] for edge in edges) + 0.5 * sum(spans)
    scale = 0.5 / sum(edge[:, 2:3] + edge[:, 3:4] + edge[:, 4:5] for edge in edges)
    factors = [span * (1.0 / SPAN) for span in spans]
    piece = min(1024, wide)
    total = 0.0
    for at in range(0, wide, piece):
        codes = [pay_ref[:, at : at + piece].astype(f32) for pay_ref in pay_refs]
        part = sum(jnp.log(code) * factor for code, factor in zip(codes, factors))
        part = (part + offset) * scale
        losses_ref[:, at : at + piece] = part
        total += jnp.sum(part, axis=1, keepdims=True)
    mean = total * (1.0 / wide)
    second = jnp.sum(jnp.square(losses_ref[...] - mean), axis=1, keepdims=True)
    lane = lax.broadcasted_iota(jnp.int32, both_ref.shape[1:], 1)
    both = jnp.where(lane == 0, mean, jnp.where(lane == 1, second, 0.0))
    for k in range(both_ref.shape[0]):
        both_ref[k] = both


def tail_kernel(tail_scale, scenarios, losses_ref, both_ref, pay_ref):
    groups = both_ref.shape[0]
    wide = losses_ref.shape[1]
    means = [both_ref[k, :, 0:1] for k in range(groups)]
    center = sum(means) * (1.0 / groups)
    spread = sum(both_ref[k, :, 1:2] for k in range(groups)) * (1.0 / scenarios)
    spread += sum(jnp.square(each - center) for each in means) * (1.0 / groups)
    deviation = jnp.sqrt(spread + EPSILON)
    thresh = center + QUANTILE * deviation
    width = SMOOTH * deviation
    narrow = 1.0 / width
    piece = min(1024, wide)
    soft = 0.0
    for at in range(0, wide, piece):
        scaled = (losses_ref[:, at : at + piece] - thresh) * narrow
        small = jnp.exp(-jnp.abs(scaled))
        grown = 1.0 + small
        half = 0.5 * tail_scale
        weight = (jnp.where(scaled >= 0.0, half, half * small) / grown).astype(bf16)
        soft += jnp.sum(jnp.maximum(scaled, 0.0) + jnp.log(grown), axis=1, keepdims=True)
        pay_ref[:, at : at + piece] = weight
    lane = lax.broadcasted_iota(jnp.int32, (pay_ref.shape[0], 128), 1)
    edge = jnp.zeros(lane.shape, f32)
    for at, part in enumerate(split3(soft) + split3(thresh) + split3(width)):
        edge = jnp.where(lane == at, part, edge)
    pay_ref[:, wide:] = edge.astype(bf16)


def join_kernel(*refs):
    count = len(refs) - 1
    for k, ref in zip(farthest_last(count), refs):
        refs[-1][lax.rem(spot()[1] + (count - k), count)] = ref[...]


def spread_kernel(*refs):
    pay_refs, (weight_ref, soft_ref, stat_ref, head_ref) = refs[:-4], refs[-4:]
    count = len(pay_refs)
    wide = weight_ref.shape[1]
    rows = weight_ref.shape[0] // (count * count)
    for k, pay_ref in zip(farthest_last(count), pay_refs):
        place = lax.rem(spot()[0] + (count - k), count)
        for j in range(count):
            owner = jnp.where(lax.axis_index("c") == 0, place * count + j, j * count + place)
            at = pl.multiple_of(owner * rows, rows)
            weight_ref[pl.ds(at, rows)] = pay_ref[j, :, 0:wide]
            head_ref[pl.ds(at, rows)] = pay_ref[j, :, wide:].astype(f32)
    heads = jnp.transpose(head_ref[...])
    soft_ref[...] = jnp.broadcast_to(join3(heads, 0), soft_ref.shape)
    stat_ref[...] = jnp.zeros_like(stat_ref)
    stat_ref[0:1] = join3(heads, 3)
    stat_ref[1:2] = join3(heads, 6)


def gradient_kernel(own, p_ref, weight_ref, out_ref):
    rows = out_ref.shape[0]
    core = lax.axis_index("c")
    half = core if own else 1 - core
    at = (half * pl.num_programs(0) + pl.program_id(0)) * rows
    out_ref[...] = lax.dot_general(
        p_ref[pl.ds(pl.multiple_of(at, rows), rows)],
        weight_ref[...],
        (((1,), (1,)), ((), ())),
        preferred_element_type=f32,
    )


def pair_kernel(own_ref, other_ref, soft_ref, soft_other_ref, *pay_refs):
    count = len(pay_refs)
    rows = pay_refs[0].shape[0] - HEAD
    soft = soft_ref[0:1] + soft_other_ref[0:1]
    for k, pay_ref in enumerate(pay_refs):
        at = pl.multiple_of(lax.rem(lax.axis_index("x") + k, count) * rows, rows)
        code, head = encode(own_ref[pl.ds(at, rows)] + other_ref[pl.ds(at, rows)], [soft])
        pay_ref[0:rows] = code
        pay_ref[rows : rows + HEAD] = head


def whole_kernel(tail_scale, stat_ref, *refs):
    pay_refs, out_ref, short_ref = refs[:-2], refs[-2], refs[-1]
    rows = out_ref.shape[0] - HEAD
    total = jnp.zeros((rows, out_ref.shape[1]), f32)
    soft = jnp.zeros((1, out_ref.shape[1]), f32)
    for pay_ref in pay_refs:
        head = pay_ref[rows : rows + HEAD].astype(f32)
        total += decode(pay_ref[0:rows], head)
        soft += join3(head, 2)
    code, head = encode(total, [])
    out_ref[0:rows] = code
    out_ref[rows : rows + HEAD] = head
    short_ref[...] = jnp.broadcast_to(stat_ref[0:1] + stat_ref[1:2] * (soft * tail_scale), short_ref.shape)


def update_kernel(count, last, side, *refs):
    own_refs, other_refs = refs[:count], refs[count : 2 * count]
    prev_ref, lge_ref, unnorm_ref = refs[2 * count : 2 * count + 3]
    rows = own_refs[0].shape[0] - HEAD
    core = lax.axis_index("c")
    total = jnp.zeros((1, prev_ref.shape[1]), f32)
    reach = jnp.zeros((1, prev_ref.shape[1]), f32)
    for half, pay_refs in ((core, own_refs), (1 - core, other_refs)):
        for k, pay_ref in enumerate(pay_refs):
            at = (half * count + lax.rem(lax.axis_index("x") + (count - k), count)) * rows
            here = pl.ds(pl.multiple_of(at, rows), rows)
            gradient = decode(pay_ref[0:rows], pay_ref[rows : rows + HEAD].astype(f32))
            lge = lge_ref[here]
            unnorm = prev_ref[here] * jnp.exp(lge * (-STEP_RATE * gradient))
            unnorm_ref[here] = unnorm
            total += jnp.sum(unnorm, axis=0, keepdims=True)
            if not last:
                expo = (unnorm * lge).astype(bf16).astype(f32)
                put_rotated(refs[-2], here, jnp.transpose(expo).astype(bf16), side)
                reach += jnp.sum(expo, axis=0, keepdims=True)
    if last:
        refs[-1][...] = jnp.broadcast_to(total[None], refs[-1].shape)
    else:
        put_rotated(refs[-1], slice(None), edge_of(total, reach), side)


def scale_kernel(obligors, unnorm_ref, totals_ref, out_ref):
    rows = out_ref.shape[0]
    here = pl.ds(pl.multiple_of(pl.program_id(0) * rows, rows), rows)
    total = sum(totals_ref[k] for k in range(totals_ref.shape[0]))
    out_ref[...] = unnorm_ref[here] * (obligors / total)


VMEM = pl.BlockSpec(memory_space=pltpu.VMEM)


def near(array):
    return array if INTERPRET else pltpu.with_memory_space_constraint(array, pltpu.VMEM)


def far(array):
    return array if INTERPRET else pltpu.with_memory_space_constraint(array, pltpu.HBM)


def near_shape(shape, dtype):
    return jax.ShapeDtypeStruct(shape, dtype) if INTERPRET else pltpu.VMEM(shape, dtype)


def whole(shape):
    return pl.BlockSpec(shape, lambda *_: (0,) * len(shape))


def groups_of(side):
    span = range(side)
    plane = lambda y, z, c: (y * side + z) * 2 + c
    along_y = lambda c: [[plane(y, z, c) for y in span] for z in span]
    along_z = lambda c: [[plane(y, z, c) for z in span] for y in span]
    return along_y(0) + along_z(1), along_z(0) + along_y(1)


def farthest_last(count):
    return sorted(range(count), key=lambda k: min(k, count - k))


def exchanged(slots, groups):
    count = len(slots)
    out = list(slots)
    for k in sorted(range(1, count), key=lambda k: -min(k, count - k)):
        out[k] = lax.ppermute(
            slots[k], PLANE, [(group[i], group[(i + k) % count]) for group in groups for i in range(count)]
        )
    return out


def rounded(value):
    return lax.reduce_precision(value, 8, 7)


def on_device(factors, idiosyncratic, loadings, rating, barrier, loss_given, sector, allowed, holdings):
    sds = jax.ShapeDtypeStruct
    n_obl, n_x, n_c = lax.axis_size(OBL), lax.axis_size("x"), lax.axis_size("c")
    side = lax.axis_size("y")
    first, second = groups_of(side)
    obl_dev, scn_dev = idiosyncratic.shape
    mandates = holdings.shape[1]
    obligors = obl_dev * n_obl
    scenarios = scn_dev * n_x * n_c
    tail_scale = 1.0 / ((1.0 - LEVEL) * scenarios)
    ro = obl_dev // (n_x * n_c)
    po = ro + HEAD
    mr = mandates // n_obl
    half = obl_dev // n_c
    row8 = sds((8, mandates), f32)
    ratings = barrier.shape[0]
    bar_a = rounded(barrier)
    bar_b = rounded(barrier - bar_a)
    bar_c = barrier - bar_a - bar_b
    bars = -jnp.concatenate([bar_a, bar_b, bar_c])
    bars = jnp.pad(bars, (0, 128 - 3 * ratings)).astype(bf16)[None, :]
    fdim = factors.shape[1]

    sb = min(512, obl_dev)
    line = pl.BlockSpec((1, sb), lambda i: (0, i))
    prev, lge, aug, expot, edge = call(
        functools.partial(setup_kernel, side),
        (obl_dev // sb,),
        [
            pl.BlockSpec((sb, mandates), lambda i: (i, 0)),
            line,
            line,
            line,
            whole(allowed.shape[::-1]),
            pl.BlockSpec((sb, fdim), lambda i: (i, 0)),
        ],
        [VMEM] * 5,
        [
            near_shape((obl_dev, mandates), f32),
            near_shape((obl_dev, mandates), f32),
            near_shape((obl_dev, fdim + 128), bf16),
            near_shape((mandates, obl_dev), bf16),
            near_shape((mandates, 128), bf16),
        ],
        scratch=[pltpu.VMEM((8, mandates), f32)],
        nbytes=obl_dev * mandates * 12,
        name="setup",
    )(far(holdings), far(loss_given[None, :]), far(sector[None, :]), far(rating[None, :]), far(allowed.T), far(loadings))
    lge = near(lge)

    results = []
    prob = None
    for iteration in range(STEPS):
        quarter = sds((side, mr, scn_dev + 128), bf16)
        few = sds((mr, scn_dev + 128), bf16)
        wide = min(512, scn_dev)
        if iteration == 0:
            prob, *pays = call(
                first_losses_kernel,
                (scn_dev // wide,),
                [
                    VMEM,
                    pl.BlockSpec((wide, fdim), lambda i: (i, 0)),
                    whole((1, 128)),
                    pl.BlockSpec((obl_dev, wide), lambda i: (0, i)),
                    VMEM,
                    VMEM,
                ],
                [VMEM] * (1 + side),
                [near_shape((obl_dev, scn_dev), bf16)] + [quarter] * side,
                flops=4 * obl_dev * scn_dev * mandates,
                nbytes=obl_dev * scn_dev * 4,
                name="first_losses",
            )(near(aug), factors, bars, idiosyncratic, near(expot), near(edge))
            prob = near(prob)
            pays = exchanged(pays, first)
            arrived = pays[:1] + [pays[k] for k in farthest_last(side)[:0:-1]]
        else:
            part = scn_dev // 2
            narrow = min(512, part)
            arrived = []
            for begin, edges in ((0, 0), (part, 128)):
                pays = call(
                    functools.partial(losses_kernel, narrow, begin),
                    (part // narrow,),
                    [VMEM, VMEM, VMEM],
                    [VMEM] * side,
                    [sds((side, mr, part + edges), bf16)] * side,
                    flops=2 * obl_dev * part * mandates,
                    nbytes=obl_dev * part * 2,
                    name="losses",
                )(prob, near(expot), near(edge))
                pays = exchanged(pays, first)
                arrived += pays[:1] + [pays[k] for k in farthest_last(side)[:0:-1]]
        pays = call(
            functools.partial(mid_kernel, len(arrived) // side),
            (1,),
            [VMEM] * len(arrived),
            [VMEM] * side,
            [few] * side,
            scratch=[pltpu.VMEM((mr, scn_dev), f32)],
            nbytes=mandates * scn_dev * 2,
            name="mid",
        )(*arrived)
        pays = exchanged(pays, second)
        pays = pays[:1] + [pays[k] for k in farthest_last(side)[:0:-1]]
        n_scn = n_x * n_c
        losses, both = call(
            sum_kernel,
            (1,),
            [VMEM] * side,
            [VMEM, VMEM],
            [near_shape((mr, scn_dev), f32), sds((n_scn, mr, 128), f32)],
            nbytes=mandates * scn_dev * 2,
            name="sum",
        )(*pays)
        both = lax.all_to_all(both, SCN, 0, 0, tiled=True)
        weight = call(
            functools.partial(tail_kernel, tail_scale, scenarios),
            (1,),
            [VMEM, VMEM],
            VMEM,
            few,
            nbytes=mandates * scn_dev * 2,
            name="tail",
        )(near(losses), both)
        weight = call(
            join_kernel,
            (1,),
            [VMEM] * side,
            VMEM,
            quarter,
            nbytes=scn_dev * mandates,
            name="join",
        )(*(lambda out: [out[k] for k in farthest_last(side)])(exchanged([weight] * side, second)))
        weight, soft, stat = call(
            spread_kernel,
            (1,),
            [VMEM] * side,
            [VMEM, whole((8, mandates)), whole((8, mandates))],
            [near_shape((mandates, scn_dev), bf16), row8, row8],
            scratch=[pltpu.VMEM((mandates, 128), f32)],
            nbytes=scn_dev * mandates * 4,
            name="spread",
        )(*(lambda out: [out[k] for k in farthest_last(side)])(exchanged([weight] * side, first)))
        weight = near(weight)
        gblock = min(512, half)

        def gradient_of(own):
            return call(
                functools.partial(gradient_kernel, own),
                (half // gblock,),
                [VMEM, VMEM],
                pl.BlockSpec((gblock, mandates), lambda i: (i, 0)),
                sds((half, mandates), f32),
                flops=2 * half * scn_dev * mandates,
                nbytes=half * scn_dev * 2,
                name="gradient",
            )(prob, weight)

        swap = [(0, 1), (1, 0)]
        sent = lax.ppermute(gradient_of(False), "c", swap)
        soft_other = lax.ppermute(soft, "c", swap)
        kept = gradient_of(True)
        gshape = sds((po, mandates), bf16)
        hops = {k: [(i, (i + k) % n_x) for i in range(n_x)] for k in range(1, n_x)}
        order = sorted(hops, key=lambda k: -min(k, n_x - k))
        slots = call(
            pair_kernel,
            (1,),
            [VMEM, VMEM, whole((8, mandates)), whole((8, mandates))],
            [VMEM] * n_x,
            [gshape] * n_x,
            nbytes=half * mandates * 10,
            name="pair",
        )(kept, sent, soft, soft_other)
        slots = list(slots)
        for k in order:
            slots[k] = lax.ppermute(slots[k], "x", hops[k])
        pay, short = call(
            functools.partial(whole_kernel, tail_scale),
            (1,),
            [whole((8, mandates))] + [VMEM] * n_x,
            [VMEM, whole((8, mandates))],
            [gshape, row8],
            nbytes=half * mandates * 4,
            name="whole",
        )(stat, *slots)
        results.append(short[0])
        slots = [pay] * n_x
        for k in order:
            slots[k] = lax.ppermute(pay, "x", hops[k])
        others = [lax.ppermute(slot, "c", swap) for slot in slots]
        last = iteration == STEPS - 1
        outs = call(
            functools.partial(update_kernel, n_x, last, side),
            (1,),
            [VMEM] * (2 * n_x + 2),
            [VMEM] + [VMEM] * (not last) + [VMEM],
            [near_shape((obl_dev, mandates), f32)]
            + [near_shape((mandates, obl_dev), bf16)] * (not last)
            + [sds((n_obl, 1, mandates), f32) if last else near_shape((mandates, 128), bf16)],
            nbytes=obl_dev * mandates * 14,
            name="update",
        )(*slots, *others, near(prev), lge)
        prev, expot, edge = outs[0], outs[-2], outs[-1]

    totals = lax.all_to_all(edge, OBL, 0, 0, tiled=True)
    positions = call(
        functools.partial(scale_kernel, obligors),
        (max(1, obl_dev // 512),),
        [VMEM, whole((n_obl, 1, mandates))],
        pl.BlockSpec((min(512, obl_dev), mandates), lambda i: (i, 0)),
        sds((obl_dev, mandates), f32),
        nbytes=obl_dev * mandates * 8,
        name="scale",
    )(near(prev), totals)
    return (positions, jnp.stack(results))


def solution(mesh):
    n_obl, n_scn = mesh.shape["obl"], mesh.shape["scn"]
    side = 1
    while side * side < n_obl:
        side *= 2
    fine = Mesh(mesh.devices.reshape(side, n_obl // side, n_scn // 2, 2), ("y", "z", "x", "c"))
    in_specs = (P(SCN, None), P(OBL, SCN), P(OBL, None), P(OBL), P(), P(OBL), P(OBL), P(), P(OBL, None))
    return jax.shard_map(on_device, mesh=fine, in_specs=in_specs, out_specs=(P(OBL, None), P()), check_vma=False)
```
